32 devices in a mesh: dp: 32 (over z, y, x, core).
Axes of the slice: x: 2, y: 2, z: 4, core: 2. Of those that a mesh axis runs over, the one named last changes fastest.
Arguments:
- grad_rows: bfloat16 [32, 7520256], P('dp')
- master: float32 [7520256], P('dp')
- mom_first: float32 [7520256], P('dp')
- mom_second: float32 [7520256], P('dp')
- decay_mask: int32 [7520256], P('dp')
- learn_rate: float32 [1], replicated
Outputs:
- output 1: bfloat16 [7520256], replicated
- output 2: float32 [7520256], P('dp')
- output 3: float32 [7520256], P('dp')
- output 4: float32 [7520256], P('dp')
- output 5: float32 [1], replicated
All inputs are finite; a program needn't handle non-finite values.
Results may differ from the reference program's by a relative error of at most 0.001.
Values are sent between devices in bfloat16 or wider.
A program may use at most 1 GiB of HBM per device.

```python
import jax
import jax.numpy as jnp
from jax import lax

NUM_DEV = 32
MODEL_WIDTH = 640
MLP_HIDDEN = 1728
VOCAB_ROWS = 4000
PADDED = 7520256
ADAM_STEP = 10

BETA_FIRST = 0.9
BETA_SECOND = 0.95
ADAM_EPS = 1e-8
CLIP_EPS = 1e-6
WEIGHT_DECAY = 0.1


def decay_layout(mask_key):
    seg_lens = [VOCAB_ROWS * MODEL_WIDTH, MODEL_WIDTH * MODEL_WIDTH, MODEL_WIDTH * MODEL_WIDTH, MODEL_WIDTH * MODEL_WIDTH, MODEL_WIDTH * MODEL_WIDTH, MODEL_WIDTH * MLP_HIDDEN, MODEL_WIDTH * MLP_HIDDEN, MLP_HIDDEN * MODEL_WIDTH, MODEL_WIDTH, MODEL_WIDTH, MODEL_WIDTH, MODEL_WIDTH]
    seg_flags = [0, 1, 1, 1, 1, 1, 1, 1, 0, 0, 0, 0]
    tensor_order = jax.random.permutation(mask_key, len(seg_lens))
    lens_perm = jnp.array(seg_lens, dtype=jnp.int32)[tensor_order]
    flags_perm = jnp.concatenate([jnp.array(seg_flags, dtype=jnp.int32)[tensor_order], jnp.zeros((1,), jnp.int32)])
    seg_ends = jnp.cumsum(lens_perm)
    seg_pos = jnp.searchsorted(seg_ends, jnp.arange(PADDED, dtype=jnp.int32), side='right')
    return flags_perm[seg_pos]


def setup_inputs(seed: int = 0) -> dict:
    key_list = jax.random.split(jax.random.key(seed), 8)
    dev_scale = 2.0 ** jax.random.uniform(key_list[0], (NUM_DEV,), jnp.float32, -1.5, 1.5)
    norm_aim = jax.random.uniform(key_list[1], (), jnp.float32, 3.0, 8.0)
    grad_scale = norm_aim * NUM_DEV / jnp.sqrt(jnp.sum(dev_scale * dev_scale) * PADDED)
    row_keys = jax.random.split(key_list[2], NUM_DEV)

    def draw_row(row_args):
        row_key, row_scale = row_args
        row_vals = jax.random.normal(row_key, (PADDED,), jnp.float32) * (grad_scale * row_scale)
        return row_vals.astype(jnp.bfloat16)

    grad_rows = lax.map(draw_row, (row_keys, dev_scale))
    unit_scale = PADDED ** -0.5
    master = jax.random.normal(key_list[3], (PADDED,), jnp.float32)
    mom_first = 0.15 * unit_scale * jax.random.normal(key_list[4], (PADDED,), jnp.float32)
    mom_second = 0.05 * unit_scale * unit_scale * (0.5 + jax.random.uniform(key_list[5], (PADDED,), jnp.float32))
    decay_mask = decay_layout(key_list[6])
    learn_rate = jax.random.uniform(key_list[7], (1,), jnp.float32, 0.5, 1.0)
    return {'grad_rows': grad_rows, 'master': master, 'mom_first': mom_first, 'mom_second': mom_second, 'decay_mask': decay_mask, 'learn_rate': learn_rate}


def reference(grad_rows, master, mom_first, mom_second, decay_mask, learn_rate):
    grad_mean = jnp.sum(grad_rows, axis=0, dtype=jnp.float32) / NUM_DEV
    grad_norm = jnp.sqrt(jnp.sum(grad_mean * grad_mean))
    clip_coef = jnp.minimum(1.0, 1.0 / (grad_norm + CLIP_EPS))
    clipped = grad_mean * clip_coef
    new_first = BETA_FIRST * mom_first + (1.0 - BETA_FIRST) * clipped
    new_second = BETA_SECOND * mom_second + (1.0 - BETA_SECOND) * clipped * clipped
    step_dir = (new_first / (1.0 - BETA_FIRST ** ADAM_STEP)) / (jnp.sqrt(new_second / (1.0 - BETA_SECOND ** ADAM_STEP)) + ADAM_EPS)
    decay_flag = decay_mask.astype(jnp.float32)
    new_master = master - learn_rate[0] * (step_dir + WEIGHT_DECAY * decay_flag * master)
    params = new_master.astype(jnp.bfloat16)
    return params, new_master, new_first, new_second, grad_norm.reshape(1)
```

```python
import functools

import jax
import jax.numpy as jnp
from jax import lax
from jax.experimental import pallas as pl
from jax.experimental.pallas import tpu as pltpu
from jax.sharding import PartitionSpec as P

BETA_FIRST = 0.9
BETA_SECOND = 0.95
ADAM_EPS = 1e-8
CLIP_EPS = 1e-6
WEIGHT_DECAY = 0.1
ADAM_STEP = 10
LANES = 128
TILE = 16
STAGES = 3
MESH = pl.DeviceIdType.MESH
F32 = jnp.float32
BF16 = jnp.bfloat16


def over_tiles(count, group, body):
    whole = count // group
    size = group * TILE

    def step(i, carry):
        body(pl.multiple_of(i * size, size), size)
        return carry

    if whole:
        lax.fori_loop(0, whole, step, 0)
    if count % group:
        body(whole * size, (count % group) * TILE)


def kernel(rows, grad_hbm, w_hbm, m_hbm, v_hbm, d_hbm, lr_ref,
           out_hbm, nw_hbm, nm_hbm, nv_hbm, norm_ref,
           stage0, stage1, stage2, row, got1, kept, sent2, got2, got3, w, m, v, d, own, part1, part2,
           stage_sem, state_sem, s1, r1, s2, r2, s3, r3, ns1, nr1, ns2, nr2, gs1, gr1, gs2, gr2, gs3, gr3, gs4, gr4):
    stages = (stage0, stage1, stage2)
    tiles = -(-rows // TILE)
    tiles_c = (tiles - tiles // 2, tiles // 2)
    rows_c = (tiles_c[0] * TILE, tiles_c[1] * TILE)
    first_c = (0, rows_c[0])
    block = rows * LANES
    units = rows // 2
    unit_first = (0, rows_c[0] // 2)
    unit_len = (rows_c[0] // 2, units - rows_c[0] // 2)
    full = rows // TILE
    rest = rows - full * TILE

    me = lax.axis_index('dp')
    z = lax.div(me, 8)
    me8 = lax.rem(me, 8)
    y = lax.div(me8, 4)
    x = lax.rem(lax.div(me8, 2), 2)
    c = lax.rem(me8, 2)

    def flip(a, by):
        return 1 - a if by else a

    def in_plane(jy, jx, jc):
        return flip(y, jy) * 4 + flip(x, jx) * 2 + flip(c, jc)

    def peer(jy, jx, jc):
        return z * 8 + in_plane(jy, jx, jc)

    def z_ahead(g):
        return lax.rem(z + 1 + g, 4)

    def z_behind(g):
        return lax.rem(z + 3 - g, 4)

    plane = [(jy, jx, jc) for jy in (0, 1) for jx in (0, 1) for jc in (0, 1) if jy + jx + jc]

    def state_copy(i):
        return pltpu.make_async_copy((w_hbm, m_hbm, v_hbm, d_hbm)[i], (w, m, v, d)[i], state_sem.at[i])

    order = [(1, 1, 1), (1, 1, 0), (1, 0, 1), (1, 0, 0), (0, 1, 1), (0, 1, 0), (0, 0, 1), (0, 0, 0)]
    work = [(g, j) for g in range(4) for j in order]

    def block_of(g, j):
        return z_ahead(g) * 8 + in_plane(*j)

    def stage_copy(i):
        g, j = work[i]
        at = pl.multiple_of(block_of(g, j) * block, LANES)
        return pltpu.make_async_copy(grad_hbm.at[:, pl.ds(at, block)], stages[i % STAGES], stage_sem.at[i % STAGES])

    for i in range(STAGES):
        stage_copy(i).start()

    barrier = pltpu.get_barrier_semaphore()
    for j in plane:
        pl.semaphore_signal(barrier, inc=1, device_id=(peer(*j),), device_id_type=MESH)
    for g in range(3):
        pl.semaphore_signal(barrier, inc=1, device_id=(z_ahead(g) * 8 + me8,), device_id_type=MESH)

    def pack(i):
        g, j = work[i]
        k = block_of(g, j)
        source = stages[i % STAGES]
        stage_copy(i).wait()

        def body(at, size):
            lane = at * LANES
            if not isinstance(at, int):
                lane = pl.multiple_of(lane, TILE * LANES)
            val = source[:, pl.ds(lane, size * LANES)].astype(F32).reshape(size, LANES)
            row[k, pl.ds(at, size), :] = val.astype(BF16)

        over_tiles(full, 4, body)
        if rest:
            row[k, pl.ds(full * TILE, TILE), :] = jnp.zeros((TILE, LANES), BF16)
            body(full * TILE, rest)
        if i + STAGES < len(work):
            stage_copy(i + STAGES).start()

    def first_copy(col, g, j2, slot):
        near = 1 if slot else 0
        jc = 1 if slot != 1 else 0
        j = (j2, near, jc) if col == 0 else (near, j2, jc)
        to = peer(0, near, jc) if col == 0 else peer(near, 0, jc)
        return pltpu.make_async_remote_copy(
            src_ref=row.at[block_of(g, j), pl.ds(first_c[col], rows_c[col])],
            dst_ref=got1.at[col, g, j2, slot, pl.ds(0, rows_c[col])],
            send_sem=s1.at[col, g, j2, slot], recv_sem=r1.at[col, g, j2, slot],
            device_id=(to,), device_id_type=MESH)

    def second_copy(col, g):
        to = peer(1, 0, 0) if col == 0 else peer(0, 1, 0)
        return pltpu.make_async_remote_copy(
            src_ref=sent2.at[col, g, pl.ds(0, rows_c[col])], dst_ref=got2.at[col, g, pl.ds(0, rows_c[col])],
            send_sem=s2.at[col, g], recv_sem=r2.at[col, g], device_id=(to,), device_id_type=MESH)

    def third_copy(col, g):
        return pltpu.make_async_remote_copy(
            src_ref=kept.at[col, g, pl.ds(0, rows_c[col])], dst_ref=got3.at[col, g, pl.ds(0, rows_c[col])],
            send_sem=s3.at[col, g], recv_sem=r3.at[col, g],
            device_id=(z_ahead(g) * 8 + me8,), device_id_type=MESH)

    def send_first(g, j2):
        for slot in (1, 2, 0):
            for col in (0, 1):
                first_copy(col, g, j2, slot).start()

    def four_sum(col, g, j2, target):
        for slot in (0, 1, 2):
            first_copy(col, g, j2, slot).wait_recv()
        k = block_of(g, (j2, 0, 0) if col == 0 else (0, j2, 0))

        def body(at, size):
            near = pl.ds(at, size)
            mine = row[k, pl.ds(first_c[col] + at, size), :].astype(F32) + got1[col, g, j2, 0, near, :].astype(F32)
            other = got1[col, g, j2, 1, near, :].astype(F32) + got1[col, g, j2, 2, near, :].astype(F32)
            target[col, g, near, :] = mine + other

        over_tiles(tiles_c[col], 4, body)

    for i in range(8):
        pack(i)
        if i == 0:
            pl.semaphore_wait(barrier, 10)
        if i == 5:
            send_first(0, 1)
    send_first(0, 0)
    for i in range(4):
        state_copy(i).start()
    for i in range(8, 16):
        pack(i)

    for g in range(4):
        for col in (0, 1):
            four_sum(col, g, 1, sent2)
        for col in (0, 1):
            second_copy(col, g).start()
        if g < 3:
            send_first(g + 1, 1)
        for col in (0, 1):
            four_sum(col, g, 0, kept)
        if g < 3:
            send_first(g + 1, 0)
        if g < 2:
            for i in range(8 * (g + 2), 8 * (g + 3)):
                pack(i)
        for col in (0, 1):
            second_copy(col, g).wait_recv()

            if g < 3:
                def body(at, size):
                    kept[col, g, pl.ds(at, size), :] = kept[col, g, pl.ds(at, size), :] + got2[col, g, pl.ds(at, size), :]

                over_tiles(tiles_c[col], 4, body)
        if g < 3:
            for col in (0, 1):
                third_copy(col, g).start()

    for i in range(4):
        state_copy(i).wait()
    acc = jnp.zeros((8, LANES), F32)
    for col in (0, 1):
        for g in range(3):
            third_copy(col, g).wait_recv()

        def mean_of(at, size):
            near = pl.ds(at, size)
            total = (kept[col, 3, near, :] + got2[col, 3, near, :]) + (got3[col, 0, near, :] + got3[col, 1, near, :])
            total = (total + got3[col, 2, near, :]) * (1.0 / 32.0)
            kept[col, 3, near, :] = total
            return jnp.sum((total * total).reshape(size // 8, 8, LANES), axis=0)

        whole = tiles_c[col] // 4
        if whole:
            acc = lax.fori_loop(0, whole, lambda i, a: a + mean_of(pl.multiple_of(i * 64, 64), 64), acc)
        if tiles_c[col] % 4:
            acc = acc + mean_of(whole * 64, (tiles_c[col] % 4) * TILE)

    def norm_copy1(j):
        return pltpu.make_async_remote_copy(
            src_ref=part1.at[me8], dst_ref=part1.at[me8],
            send_sem=ns1.at[j], recv_sem=nr1.at[j], device_id=(peer(*plane[j]),), device_id_type=MESH)

    def norm_copy2(g):
        return pltpu.make_async_remote_copy(
            src_ref=part2.at[z], dst_ref=part2.at[z],
            send_sem=ns2.at[g], recv_sem=nr2.at[g], device_id=(z_ahead(g) * 8 + me8,), device_id_type=MESH)

    def landed(ref, at, send_sem, recv_sem):
        return pltpu.make_async_remote_copy(
            src_ref=ref.at[at], dst_ref=ref.at[at], send_sem=send_sem, recv_sem=recv_sem,
            device_id=(me,), device_id_type=MESH)

    part1[me8] = acc
    for j in range(7):
        norm_copy1(j).start()
    for j in range(7):
        landed(part1, in_plane(*plane[j]), ns1.at[j], nr1.at[j]).wait_recv()
    acc = part1[0]
    for j in range(1, 8):
        acc = acc + part1[j]
    part2[z] = acc
    for g in range(3):
        norm_copy2(g).start()
    for g in range(3):
        landed(part2, z_behind(g), ns2.at[g], nr2.at[g]).wait_recv()
    acc = (part2[0] + part2[1]) + (part2[2] + part2[3])
    norm = jnp.sqrt(jnp.full((1, LANES), jnp.sum(acc), F32))
    norm_ref[...] = norm
    coef = jnp.minimum(1.0, 1.0 / (norm + CLIP_EPS))
    lr = lr_ref[0]

    def update(col):
        def body(at, size):
            near = pl.ds(first_c[col] + at, size)
            h = kept[col, 3, pl.ds(at, size), :] * coef
            nm = BETA_FIRST * m[near, :] + (1.0 - BETA_FIRST) * h
            nv = BETA_SECOND * v[near, :] + (1.0 - BETA_SECOND) * h * h
            step = (nm * (1.0 / (1.0 - BETA_FIRST ** ADAM_STEP))) / (jnp.sqrt(nv * (1.0 / (1.0 - BETA_SECOND ** ADAM_STEP))) + ADAM_EPS)
            old = w[near, :]
            nw = old - lr * (step + WEIGHT_DECAY * d[near, :].astype(F32) * old)
            m[near, :] = nm
            v[near, :] = nv
            w[near, :] = nw
            unit = first_c[col] // 2 + (at // 2 if isinstance(at, int) else lax.div(at, 2))
            own[pl.ds(unit, size // 2)] = nw.astype(BF16).reshape(size // 2, 2, LANES)

        count = tiles_c[col] if col == 0 else tiles_c[col] - (1 if rest else 0)
        over_tiles(count, 2, body)
        if col == 1 and rest:
            body(count * TILE, rest)

    def place(zz, jy, jx, jc, col):
        k = zz * 8 + in_plane(jy, jx, jc)
        return out_hbm.at[pl.ds(k * units + unit_first[col], unit_len[col])]

    def zed(zi):
        return z if zi == 3 else z_behind(zi)

    def mine_or(zi, spot, col, first):
        return own.at[pl.ds(unit_first[col], unit_len[col])] if first else spot

    def gather1(col, g):
        spot = place(z, 0, 0, 0, col)
        return pltpu.make_async_remote_copy(
            src_ref=mine_or(3, spot, col, True), dst_ref=spot, send_sem=gs1.at[col, g], recv_sem=gr1.at[col, g],
            device_id=(z_ahead(g) * 8 + me8,), device_id_type=MESH)

    def gather2(col, zi):
        spot = place(zed(zi), 0, 0, 0, col)
        to = peer(1, 0, 0) if col == 0 else peer(0, 1, 0)
        return pltpu.make_async_remote_copy(
            src_ref=mine_or(zi, spot, col, zi == 3), dst_ref=spot, send_sem=gs2.at[col, zi], recv_sem=gr2.at[col, zi],
            device_id=(to,), device_id_type=MESH)

    def gather3(col, zi, j2):
        spot = place(zed(zi), j2, 0, 0, col) if col == 0 else place(zed(zi), 0, j2, 0, col)
        to = peer(0, 1, 0) if col == 0 else peer(1, 0, 0)
        return pltpu.make_async_remote_copy(
            src_ref=mine_or(zi, spot, col, zi == 3 and j2 == 0), dst_ref=spot,
            send_sem=gs3.at[col, zi, j2], recv_sem=gr3.at[col, zi, j2], device_id=(to,), device_id_type=MESH)

    def gather4(col, zi, j2, j3):
        spot = place(zed(zi), j2, j3, 0, col) if col == 0 else place(zed(zi), j3, j2, 0, col)
        return pltpu.make_async_remote_copy(
            src_ref=mine_or(zi, spot, col, zi == 3 and j2 == 0 and j3 == 0), dst_ref=spot,
            send_sem=gs4.at[col, zi, j2, j3], recv_sem=gr4.at[col, zi, j2, j3],
            device_id=(peer(0, 0, 1),), device_id_type=MESH)

    for col in (0, 1):
        update(col)
        gather1(col, 0).start()
        gather2(col, 3).start()
        gather3(col, 3, 0).start()
    for g in (1, 2):
        for col in (0, 1):
            gather1(col, g).start()
    results = [pltpu.make_async_copy((w, m, v)[i], (nw_hbm, nm_hbm, nv_hbm)[i], state_sem.at[i]) for i in range(3)]
    results.append(pltpu.make_async_copy(own, out_hbm.at[pl.ds(me * units, units)], state_sem.at[3]))
    for copy in results:
        copy.start()
    for col in (0, 1):
        gather4(col, 3, 0, 0).start()

    def landed1(col, g):
        return pltpu.make_async_remote_copy(
            src_ref=own.at[pl.ds(unit_first[col], unit_len[col])], dst_ref=place(z_behind(g), 0, 0, 0, col),
            send_sem=gs1.at[col, g], recv_sem=gr1.at[col, g], device_id=(me,), device_id_type=MESH)

    for zi in (3, 0, 1, 2):
        if zi < 3:
            for col in (0, 1):
                landed1(col, zi).wait_recv()
                gather2(col, zi).start()
                gather3(col, zi, 0).start()
                gather4(col, zi, 0, 0).start()
        for col in (0, 1):
            gather2(col, zi).wait_recv()
            gather3(col, zi, 1).start()
            gather4(col, zi, 1, 0).start()
    for zi in (3, 0, 1, 2):
        for j2 in (0, 1):
            for col in (0, 1):
                gather3(col, zi, j2).wait_recv()
                gather4(col, zi, j2, 1).start()

    for copy in results:
        copy.wait()
    for col in (0, 1):
        for zi in (3, 0, 1, 2):
            for j2 in (0, 1):
                for j3 in (0, 1):
                    gather4(col, zi, j2, j3).wait()
                gather3(col, zi, j2).wait_send()
            gather2(col, zi).wait_send()
        for g in range(3):
            gather1(col, g).wait_send()
            third_copy(col, g).wait_send()
        for g in range(4):
            second_copy(col, g).wait_send()
            for j2 in (0, 1):
                for slot in range(3):
                    first_copy(col, g, j2, slot).wait_send()
    for j in range(7):
        norm_copy1(j).wait_send()
    for g in range(3):
        norm_copy2(g).wait_send()


def solution(mesh):
    num_dev = mesh.shape['dp']

    def local_step(grad_row, master, mom_first, mom_second, decay_mask, learn_rate):
        shard_len = master.shape[0]
        rows = shard_len // LANES
        tiles = -(-rows // TILE)
        half = (tiles - tiles // 2) * TILE
        dma = pltpu.SemaphoreType.DMA
        any_spec = pl.BlockSpec(memory_space=pl.ANY)
        flat = (rows, LANES)
        state = jax.ShapeDtypeStruct(flat, F32)
        outs = pl.pallas_call(
            functools.partial(kernel, rows),
            out_shape=(jax.ShapeDtypeStruct((num_dev * rows // 2, 2, LANES), BF16), state, state, state,
                       jax.ShapeDtypeStruct((1, LANES), F32)),
            in_specs=[any_spec] * 5 + [pl.BlockSpec(memory_space=pltpu.SMEM)],
            out_specs=(any_spec, any_spec, any_spec, any_spec, pl.BlockSpec(memory_space=pltpu.VMEM)),
            scratch_shapes=[pltpu.VMEM((1, shard_len), BF16)] * STAGES + [
                pltpu.VMEM((num_dev, tiles * TILE, LANES), BF16),
                pltpu.VMEM((2, 4, 2, 3, half, LANES), BF16),
                pltpu.VMEM((2, 4, half, LANES), F32),
                pltpu.VMEM((2, 4, half, LANES), F32),
                pltpu.VMEM((2, 4, half, LANES), F32),
                pltpu.VMEM((2, 3, half, LANES), F32),
                pltpu.VMEM(flat, F32), pltpu.VMEM(flat, F32), pltpu.VMEM(flat, F32), pltpu.VMEM(flat, jnp.int32),
                pltpu.VMEM((rows // 2, 2, LANES), BF16),
                pltpu.VMEM((8, 8, LANES), F32), pltpu.VMEM((4, 8, LANES), F32),
                dma((STAGES,)), dma((4,)),
                dma((2, 4, 2, 3)), dma((2, 4, 2, 3)), dma((2, 4)), dma((2, 4)), dma((2, 3)), dma((2, 3)),
                dma((7,)), dma((7,)), dma((3,)), dma((3,)),
                dma((2, 3)), dma((2, 3)), dma((2, 4)), dma((2, 4)), dma((2, 4, 2)), dma((2, 4, 2)),
                dma((2, 4, 2, 2)), dma((2, 4, 2, 2)),
            ],
            compiler_params=pltpu.CompilerParams(
                collective_id=0, has_side_effects=True, vmem_limit_bytes=60 * 1024 * 1024),
        )(grad_row, master.reshape(flat), mom_first.reshape(flat), mom_second.reshape(flat), decay_mask.reshape(flat), learn_rate)
        params, new_master, new_first, new_second, norm = outs
        return (params.reshape(num_dev * shard_len), new_master.reshape(shard_len), new_first.reshape(shard_len),
                new_second.reshape(shard_len), norm[0, :1])

    return jax.shard_map(local_step, mesh=mesh, in_specs=(P('dp', None), P('dp'), P('dp'), P('dp'), P('dp'), P()),
                         out_specs=(P(), P('dp'), P('dp'), P('dp'), P()), check_vma=False)
```

```python
import functools

import jax
import jax.numpy as jnp
from jax import lax
from jax.experimental import pallas as pl
from jax.experimental.pallas import tpu as pltpu
from jax.sharding import PartitionSpec as P

BETA_FIRST = 0.9
BETA_SECOND = 0.95
ADAM_EPS = 1e-8
CLIP_EPS = 1e-6
WEIGHT_DECAY = 0.1
ADAM_STEP = 10
LANES = 128
TILE = 16
STAGES = 6
SHARE = 0.386
VMEM_LIMIT = 46 * 1024 * 1024
MESH = pl.DeviceIdType.MESH
F32 = jnp.float32
BF16 = jnp.bfloat16

HIGH, LOW, Y, X, CORE = range(5)
COLOURS = ((X, Y, LOW, HIGH), (Y, X, LOW, HIGH), (LOW, HIGH, X, Y))
GROUPS = ((1, 1), (0, 1), (1, 0), (0, 0))
HALF = ((1, 1), (1, 0), (0, 1), (0, 0))


def parts_of(rows):
    near = max(1, int((rows // TILE) * SHARE)) * TILE
    return (near, near, rows - 2 * near)


def padded(n):
    return -(-n // 8) * 8


def over_rows(rows, group, body):
    size = group * TILE
    whole = rows // size

    def step(i, carry):
        body(pl.multiple_of(i * size, size), size)
        return carry

    if whole:
        lax.fori_loop(0, whole, step, 0)
    at = whole * size
    if rows - at >= TILE:
        body(at, (rows - at) // TILE * TILE)
        at += (rows - at) // TILE * TILE
    if rows > at:
        body(at, rows - at)


def half_of(at):
    return at // 2 if isinstance(at, int) else lax.div(at, 2)


def kernel(rows, grad_hbm, w_hbm, m_hbm, v_hbm, d_hbm, lr_ref, full, w, m, v, norm_ref, *scratch):
    stages = scratch[:STAGES]
    scratch = scratch[STAGES:]
    got1, kept, sent2, got2, got3 = (scratch[3 * i:3 * i + 3] for i in range(5))
    (d, partial, stage_sem, state_sem, s1, r1, s2, r2, s3, r3, ns, nr,
     gs1, gr1, gs2, gr2, gs3, gr3, gs4, gr4) = scratch[15:]
    colours = range(3)
    part = parts_of(rows)
    first = (0, part[0], part[0] + part[1])
    units = rows // 2

    me = lax.axis_index('dp')
    bits = (lax.div(me, 16), lax.rem(lax.div(me, 8), 2), lax.rem(lax.div(me, 4), 2), lax.rem(lax.div(me, 2), 2),
            lax.rem(me, 2))

    def across(*flips):
        total = 0
        for bit in range(5):
            value = 1 - bits[bit] if bit in flips else bits[bit]
            total = total * 2 + value
        return total

    def pick(axes, values):
        return tuple(a for a, val in zip(axes, values) if val)

    def where(col, g, j2, j1, jc):
        d1, d2, d3, d4 = COLOURS[col]
        return pick((d1, d2, d3, d4, CORE), (j1, j2) + GROUPS[g] + (jc,))

    def piece(ref, k, col):
        return ref.at[pl.ds(k * units + first[col] // 2, part[col] // 2)]

    def send(src, dst, send_sem, recv_sem, flips):
        return pltpu.make_async_remote_copy(
            src_ref=src, dst_ref=dst, send_sem=send_sem, recv_sem=recv_sem,
            device_id=(across(*flips),), device_id_type=MESH)

    def state_copy(i):
        return pltpu.make_async_copy((w_hbm, m_hbm, v_hbm, d_hbm)[i], (w, m, v, d)[i], state_sem.at[i])

    work = [(g, j2, j1, jc, col) for g in range(4) for j2 in (1, 0) for j1, jc in HALF for col in colours]

    def stage_copy(i):
        g, j2, j1, jc, col = work[i]
        k = across(*where(col, g, j2, j1, jc))
        at = pl.multiple_of((k * rows + first[col]) * LANES, LANES)
        return pltpu.make_async_copy(grad_hbm.at[:, pl.ds(at, part[col] * LANES)],
                                     stages[i % STAGES].at[:, pl.ds(0, part[col] * LANES)], stage_sem.at[i % STAGES])

    def first_copy(col, g, j2, slot):
        j1 = 1 if slot else 0
        jc = 0 if slot == 1 else 1
        d1 = COLOURS[col][0]
        return send(piece(full, across(*where(col, g, j2, j1, jc)), col), got1[col].at[g, j2, slot],
                    s1.at[col, g, j2, slot], r1.at[col, g, j2, slot], pick((d1, CORE), (j1, jc)))

    def second_copy(col, g):
        return send(sent2[col].at[g], got2[col].at[g], s2.at[col, g], r2.at[col, g], (COLOURS[col][1],))

    def third_copy(col, g):
        return send(kept[col].at[g], got3[col].at[g], s3.at[col, g], r3.at[col, g], pick(COLOURS[col][2:], GROUPS[g]))

    def slot_of(j1, jc):
        return (2 if jc else 1) if j1 else 0

    def pack(i, start):
        g, j2, j1, jc, col = work[i]
        k = across(*where(col, g, j2, j1, jc))
        source = stages[i % STAGES]
        base = k * units + first[col] // 2
        stage_copy(i).wait()

        def body(at, size):
            lane = at * LANES
            if not isinstance(at, int):
                lane = pl.multiple_of(lane, TILE * LANES)
            val = source[:, pl.ds(lane, size * LANES)].astype(F32).reshape(size, LANES)
            full[pl.ds(base + half_of(at), size // 2)] = val.astype(BF16).reshape(size // 2, 2, LANES)

        over_rows(part[col], 4, body)
        if i + STAGES < len(work):
            stage_copy(i + STAGES).start()
        if start and (j1 or jc):
            first_copy(col, g, j2, slot_of(j1, jc)).start()

    def send_first(g, j2):
        for j1, jc in HALF[:3]:
            for col in colours:
                first_copy(col, g, j2, slot_of(j1, jc)).start()

    def four_sum(col, g, j2, target):
        for slot in (0, 1, 2):
            first_copy(col, g, j2, slot).wait_recv()
        base = across(*where(col, g, j2, 0, 0)) * units + first[col] // 2

        def body(at, size):
            near = pl.ds(half_of(at), size // 2)

            def wide(val):
                return val.reshape(size, LANES).astype(F32)

            mine = wide(full[pl.ds(base + half_of(at), size // 2)]) + wide(got1[col][g, j2, 0, near])
            other = wide(got1[col][g, j2, 1, near]) + wide(got1[col][g, j2, 2, near])
            target[g, pl.ds(at, size), :] = mine + other

        over_rows(part[col], 4, body)

    def plane_sum(col, g):
        def body(at, size):
            near = pl.ds(at, size)
            kept[col][g, near, :] = kept[col][g, near, :] + got2[col][g, near, :]

        over_rows(part[col], 4, body)

    everyone = [pick((HIGH, LOW, Y, X, CORE), [(n >> b) & 1 for b in (4, 3, 2, 1, 0)]) for n in range(1, 32)]

    for i in range(STAGES):
        stage_copy(i).start()
    barrier = pltpu.get_barrier_semaphore()
    for flips in everyone:
        pl.semaphore_signal(barrier, inc=1, device_id=(across(*flips),), device_id_type=MESH)
    size = len(work) // 4
    pack(0, False)
    pl.semaphore_wait(barrier, 31)
    first_copy(work[0][4], 0, 1, 2).start()
    for i in range(1, size):
        pack(i, True)
    for i in range(4):
        state_copy(i).start()
    for i in range(size, 2 * size):
        pack(i, False)

    for g in range(4):
        for col in colours:
            four_sum(col, g, 1, sent2[col])
        for col in colours:
            second_copy(col, g).start()
        if g < 3:
            send_first(g + 1, 1)
        for col in colours:
            four_sum(col, g, 0, kept[col])
        if g < 3:
            send_first(g + 1, 0)
        if g < 2:
            for i in range(size * (g + 2), size * (g + 3)):
                pack(i, False)
        for col in colours:
            second_copy(col, g).wait_recv()
            if g < 3:
                plane_sum(col, g)
        if g < 3:
            for col in colours:
                third_copy(col, g).start()

    for col in colours:
        for g in range(4):
            for j2 in (0, 1):
                for slot in range(3):
                    first_copy(col, g, j2, slot).wait_send()

    acc = jnp.zeros((8, LANES), F32)
    for col in colours:
        for g in range(3):
            third_copy(col, g).wait_recv()

        def mean_of(at, size):
            near = pl.ds(at, size)
            total = (kept[col][3, near, :] + got2[col][3, near, :]) + (got3[col][0, near, :] + got3[col][1, near, :])
            total = (total + got3[col][2, near, :]) * (1.0 / 32.0)
            kept[col][3, near, :] = total
            return total * total

        def fold(val):
            return jnp.sum(val.reshape(val.shape[0] // 8, 8, LANES), axis=0)

        whole = part[col] // 64
        if whole:
            acc = lax.fori_loop(0, whole, lambda i, a: a + fold(mean_of(pl.multiple_of(i * 64, 64), 64)), acc)
        at = whole * 64
        if part[col] - at >= 8:
            size = (part[col] - at) // 8 * 8
            acc = acc + fold(mean_of(at, size))
            at += size
        if part[col] > at:
            tail = mean_of(at, part[col] - at)
            acc = acc + jnp.concatenate([tail, jnp.zeros((8 - tail.shape[0], LANES), F32)], axis=0)

    partial[me] = acc

    def norm_copy(j, owner):
        return send(partial.at[owner], partial.at[owner], ns.at[j], nr.at[j], everyone[j])

    for j in range(31):
        norm_copy(j, me).start()
    for i in range(4):
        state_copy(i).wait()
    for j in range(31):
        norm_copy(j, across(*everyone[j])).wait_recv()
    norm = jnp.sqrt(jnp.full((1, LANES), jnp.sum(jnp.sum(partial[...], axis=0)), F32))
    norm_ref[...] = norm
    coef = jnp.minimum(1.0, 1.0 / (norm + CLIP_EPS))
    lr = lr_ref[0]

    def update(col):
        def body(at, size):
            near = pl.ds(first[col] + at, size)
            h = kept[col][3, pl.ds(at, size), :] * coef
            nm = BETA_FIRST * m[near, :] + (1.0 - BETA_FIRST) * h
            nv = BETA_SECOND * v[near, :] + (1.0 - BETA_SECOND) * h * h
            step = (nm * (1.0 / (1.0 - BETA_FIRST ** ADAM_STEP))) / (
                jnp.sqrt(nv * (1.0 / (1.0 - BETA_SECOND ** ADAM_STEP))) + ADAM_EPS)
            old = w[near, :]
            nw = old - lr * (step + WEIGHT_DECAY * d[near, :].astype(F32) * old)
            m[near, :] = nm
            v[near, :] = nv
            w[near, :] = nw
            full[pl.ds(me * units + first[col] // 2 + half_of(at), size // 2)] = nw.astype(BF16).reshape(
                size // 2, 2, LANES)

        over_rows(part[col], 2, body)

    def gather1(col, g):
        spot = piece(full, me, col)
        return send(spot, spot, gs1.at[col, g], gr1.at[col, g], pick(COLOURS[col][2:], GROUPS[g]))

    def gather1_in(col, g):
        spot = piece(full, across(*where(col, g, 0, 0, 0)), col)
        return send(spot, spot, gs1.at[col, g], gr1.at[col, g], pick(COLOURS[col][2:], GROUPS[g]))

    def gather2(col, g):
        spot = piece(full, across(*where(col, g, 0, 0, 0)), col)
        return send(spot, spot, gs2.at[col, g], gr2.at[col, g], (COLOURS[col][1],))

    def gather3(col, g, j2):
        spot = piece(full, across(*where(col, g, j2, 0, 0)), col)
        return send(spot, spot, gs3.at[col, g, j2], gr3.at[col, g, j2], (COLOURS[col][0],))

    def gather4(col, g, j2, j1):
        spot = piece(full, across(*where(col, g, j2, j1, 0)), col)
        return send(spot, spot, gs4.at[col, g, j2, j1], gr4.at[col, g, j2, j1], (CORE,))

    for col in (2, 0, 1):
        update(col)
        for g in (2, 1, 0):
            gather1(col, g).start()
        gather2(col, 3).start()
        gather3(col, 3, 0).start()
    for col in colours:
        gather4(col, 3, 0, 0).start()
    for g in (3, 2, 1, 0):
        if g < 3:
            for col in (2, 0, 1):
                gather1_in(col, g).wait_recv()
                gather2(col, g).start()
                gather3(col, g, 0).start()
                gather4(col, g, 0, 0).start()
        for col in (2, 0, 1):
            gather2(col, g).wait_recv()
            gather3(col, g, 1).start()
            gather4(col, g, 1, 0).start()
    for g in (3, 2, 1, 0):
        for j2 in (0, 1):
            for col in colours:
                gather3(col, g, j2).wait_recv()
                gather4(col, g, j2, 1).start()

    for col in colours:
        for g in (3, 2, 1, 0):
            for j2 in (0, 1):
                for j1 in (0, 1):
                    gather4(col, g, j2, j1).wait()
                gather3(col, g, j2).wait_send()
            gather2(col, g).wait_send()
            second_copy(col, g).wait_send()
        for g in range(3):
            gather1(col, g).wait_send()
            third_copy(col, g).wait_send()
    for j in range(31):
        norm_copy(j, me).wait_send()


def write_out(*refs):
    sem = refs[-1]
    count = len(refs) // 2
    copies = [pltpu.make_async_copy(refs[i], refs[count + i], sem.at[i]) for i in range(count)]
    for copy in copies:
        copy.start()
    for copy in copies:
        copy.wait()


def solution(mesh):
    num_dev = mesh.shape['dp']

    def local_step(grad_row, master, mom_first, mom_second, decay_mask, learn_rate):
        shard_len = master.shape[0]
        rows = shard_len // LANES
        part = parts_of(rows)
        dma = pltpu.SemaphoreType.DMA
        hbm = pl.BlockSpec(memory_space=pltpu.HBM)
        vmem = pl.BlockSpec(memory_space=pltpu.VMEM)
        flat = (rows, LANES)
        whole = (num_dev * rows // 2, 2, LANES)
        results = pl.pallas_call(
            functools.partial(kernel, rows),
            out_shape=(pltpu.VMEM(whole, BF16), pltpu.VMEM(flat, F32), pltpu.VMEM(flat, F32), pltpu.VMEM(flat, F32),
                       pltpu.VMEM((1, LANES), F32)),
            in_specs=[hbm] * 5 + [pl.BlockSpec(memory_space=pltpu.SMEM)],
            out_specs=(vmem,) * 5,
            scratch_shapes=[pltpu.VMEM((1, max(part) * LANES), BF16)] * STAGES
            + [pltpu.VMEM((4, 2, 3, n // 2, 2, LANES), BF16) for n in part]
            + [pltpu.VMEM((count, padded(n), LANES), F32) for count in (4, 4, 4, 3) for n in part]
            + [
                pltpu.VMEM(flat, jnp.int32), pltpu.VMEM((num_dev, 8, LANES), F32),
                dma((STAGES,)), dma((4,)),
                dma((3, 4, 2, 3)), dma((3, 4, 2, 3)), dma((3, 4)), dma((3, 4)), dma((3, 3)), dma((3, 3)),
                dma((num_dev - 1,)), dma((num_dev - 1,)),
                dma((3, 3)), dma((3, 3)), dma((3, 4)), dma((3, 4)), dma((3, 4, 2)), dma((3, 4, 2)),
                dma((3, 4, 2, 2)), dma((3, 4, 2, 2)),
            ],
            compiler_params=pltpu.CompilerParams(
                collective_id=0, has_side_effects=True, vmem_limit_bytes=VMEM_LIMIT),
        )(grad_row, master.reshape(flat), mom_first.reshape(flat), mom_second.reshape(flat), decay_mask.reshape(flat), learn_rate)
        state = jax.ShapeDtypeStruct(flat, F32)
        params, new_master, new_first, new_second, norm = pl.pallas_call(
            write_out,
            out_shape=(jax.ShapeDtypeStruct(whole, BF16), state, state, state, jax.ShapeDtypeStruct((1, LANES), F32)),
            in_specs=[vmem] * 5,
            out_specs=(hbm,) * 5,
            scratch_shapes=[dma((5,))],
            compiler_params=pltpu.CompilerParams(vmem_limit_bytes=1024 * 1024),
        )(*results)
        return (params.reshape(num_dev * shard_len), new_master.reshape(shard_len), new_first.reshape(shard_len),
                new_second.reshape(shard_len), norm[0, :1])

    return jax.shard_map(local_step, mesh=mesh, in_specs=(P('dp', None), P('dp'), P('dp'), P('dp'), P('dp'), P()),
                         out_specs=(P(), P('dp'), P('dp'), P('dp'), P()), check_vma=False)
```

```python
import functools

import jax
import jax.numpy as jnp
from jax import lax
from jax.experimental import pallas as pl
from jax.experimental.pallas import tpu as pltpu
from jax.sharding import PartitionSpec as P

BETA_FIRST = 0.9
BETA_SECOND = 0.95
ADAM_EPS = 1e-8
CLIP_EPS = 1e-6
WEIGHT_DECAY = 0.1
ADAM_STEP = 10
LANES = 128
TILE = 16
STAGES = 4
VMEM_LIMIT = 46 * 1024 * 1024
MESH = pl.DeviceIdType.MESH
F32 = jnp.float32
BF16 = jnp.bfloat16

HIGH, LOW, Y, X, CORE = range(5)
REDUCE = (
    ((X, Y, LOW, HIGH), ((1, 1), (1, 0), (0, 1), (0, 0))),
    ((Y, X, LOW, HIGH), ((1, 1), (1, 0), (0, 1), (0, 0))),
    ((LOW, HIGH, X, Y), ((1, 1), (1, 0), (0, 1), (0, 0))),
)
REDUCE_TILES = (47, 47, 20)
SPAN_OF = (0, 0, 1)
GATHER = (
    ((X, Y, LOW, HIGH), ((0, 1), (1, 0), (1, 1), (0, 0))),
    ((Y, X, LOW, HIGH), ((0, 1), (1, 0), (1, 1), (0, 0))),
    ((LOW, HIGH, X, Y), ((0, 1), (1, 0), (1, 1), (0, 0))),
)
GATHER_TILES = (48, 48, 18)
REDUCE_ORDER = (
    (0, 1, 0, 1, 1, 1), (1, 2, 0, 1, 2, -1), (0, 0, 0, 1, 1, 1), (1, 0, 0, 1, 2, -1), (1, 1, 0, 1, 2, -1),
    (0, 1, 0, 1, 1, 0), (1, 2, 0, 1, 1, -1), (0, 0, 0, 1, 1, 0), (1, 0, 0, 1, 1, -1), (1, 1, 0, 1, 1, -1),
    (0, 1, 0, 1, 0, 1), (1, 2, 0, 1, 0, -1), (0, 0, 0, 1, 0, 1), (1, 0, 0, 1, 0, -1), (1, 1, 0, 0, 2, -1),
    (0, 1, 0, 1, 0, 0), (0, 0, 0, 1, 0, 0), (1, 1, 0, 0, 1, -1), (0, 1, 0, 0, 1, 1), (1, 2, 0, 0, 2, -1),
    (0, 0, 0, 0, 1, 1), (1, 1, 0, 1, 0, -1), (1, 0, 0, 0, 2, -1), (0, 1, 0, 0, 1, 0), (1, 2, 0, 0, 1, -1),
    (0, 0, 0, 0, 1, 0), (1, 0, 0, 0, 1, -1), (0, 1, 0, 0, 0, 1), (1, 2, 0, 0, 0, -1), (0, 0, 0, 0, 0, 1),
    (1, 0, 0, 0, 0, -1), (1, 1, 0, 0, 0, -1), (0, 1, 0, 0, 0, 0), (0, 0, 0, 0, 0, 0), (0, 1, 1, 1, 1, 1),
    (1, 2, 1, 1, 2, -1), (0, 0, 1, 1, 1, 1), (0, 1, 1, 1, 1, 0), (1, 2, 1, 1, 1, -1), (0, 0, 1, 1, 1, 0),
    (0, 1, 1, 1, 0, 1), (1, 2, 1, 1, 0, -1), (0, 0, 1, 1, 0, 1), (0, 1, 1, 1, 0, 0), (0, 0, 1, 1, 0, 0), (2, 2, 0),
    (0, 1, 1, 0, 1, 1), (1, 2, 1, 0, 2, 0), (0, 0, 1, 0, 1, 1), (0, 1, 1, 0, 1, 0), (1, 2, 1, 0, 1, 0),
    (0, 0, 1, 0, 1, 0), (0, 1, 1, 0, 0, 1), (1, 2, 1, 0, 0, 0), (0, 0, 1, 0, 0, 1), (0, 1, 1, 0, 0, 0),
    (0, 0, 1, 0, 0, 0), (0, 1, 2, 1, 1, 1), (0, 0, 2, 1, 1, 1), (0, 1, 2, 1, 1, 0), (0, 0, 2, 1, 1, 0),
    (0, 1, 2, 1, 0, 1), (0, 0, 2, 1, 0, 1), (0, 1, 2, 1, 0, 0), (0, 0, 2, 1, 0, 0), (0, 1, 2, 0, 1, 1),
    (0, 0, 2, 0, 1, 1), (0, 1, 2, 0, 1, 0), (0, 0, 2, 0, 1, 0), (2, 0, 0), (2, 1, 0), (3, 2, 0), (1, 0, 1, 1, 2, 0),
    (1, 1, 1, 1, 2, 0), (0, 1, 2, 0, 0, 1), (1, 0, 1, 1, 1, 0), (1, 1, 1, 1, 1, 0), (1, 0, 1, 1, 0, 0),
    (1, 1, 1, 1, 0, 0), (1, 2, 2, 1, 2, 1), (1, 2, 2, 1, 1, 1), (1, 2, 2, 1, 0, 1), (0, 0, 2, 0, 0, 1),
    (0, 1, 2, 0, 0, 0), (0, 0, 2, 0, 0, 0), (0, 1, 3, 1, 1, 1), (0, 0, 3, 1, 1, 1), (0, 1, 3, 1, 1, 0),
    (0, 0, 3, 1, 1, 0), (0, 1, 3, 1, 0, 1), (0, 0, 3, 1, 0, 1), (0, 1, 3, 1, 0, 0), (0, 0, 3, 1, 0, 0),
    (0, 1, 3, 0, 1, 1), (0, 0, 3, 0, 1, 1), (0, 1, 3, 0, 1, 0), (0, 0, 3, 0, 1, 0), (0, 1, 3, 0, 0, 1),
    (0, 0, 3, 0, 0, 1), (0, 1, 3, 0, 0, 0), (0, 0, 3, 0, 0, 0), (2, 2, 1), (1, 2, 2, 0, 2, 2), (1, 2, 2, 0, 1, 2),
    (1, 2, 2, 0, 0, 2), (3, 0, 0), (3, 1, 0), (1, 0, 1, 0, 2, 1), (1, 1, 1, 0, 2, 1), (1, 0, 1, 0, 1, 1),
    (1, 1, 1, 0, 1, 1), (1, 0, 1, 0, 0, 1), (1, 1, 1, 0, 0, 1), (4, 2, 0), (3, 2, 1), (1, 2, 3, 1, 2, 3),
    (1, 2, 3, 1, 1, 3), (1, 2, 3, 1, 0, 3), (4, 1, 0), (4, 0, 0), (2, 2, 2), (1, 2, 3, 0, 2, 4), (1, 2, 3, 0, 1, 4),
    (1, 2, 3, 0, 0, 4), (4, 2, 1), (2, 0, 1), (2, 1, 1), (1, 0, 2, 1, 2, 2), (1, 1, 2, 1, 2, 2), (1, 0, 2, 1, 1, 2),
    (1, 1, 2, 1, 1, 2), (1, 0, 2, 1, 0, 2), (1, 1, 2, 1, 0, 2), (3, 2, 2), (2, 2, 3), (3, 0, 1), (1, 0, 2, 0, 2, 3),
    (1, 0, 2, 0, 1, 3), (1, 0, 2, 0, 0, 3), (3, 1, 1), (1, 1, 2, 0, 2, 3), (1, 1, 2, 0, 1, 3), (1, 1, 2, 0, 0, 3),
    (4, 1, 1), (4, 0, 1), (2, 0, 2), (2, 1, 2), (1, 0, 3, 1, 2, 4), (1, 1, 3, 1, 2, 4), (1, 0, 3, 1, 1, 4),
    (1, 1, 3, 1, 1, 4), (1, 0, 3, 1, 0, 4), (1, 1, 3, 1, 0, 4), (3, 0, 2), (3, 1, 2), (1, 0, 3, 0, 2, 5),
    (1, 1, 3, 0, 2, 5), (1, 0, 3, 0, 1, 5), (1, 1, 3, 0, 1, 5), (1, 0, 3, 0, 0, 5), (1, 1, 3, 0, 0, 5), (4, 2, 2),
    (4, 1, 2), (3, 2, 3), (4, 0, 2), (4, 2, 3), (2, 0, 3), (2, 1, 3), (3, 0, 3), (5, 2, 0), (3, 1, 3), (4, 1, 3),
    (4, 0, 3), (5, 1, 0), (5, 0, 0),
)
GATHER_ORDER = (
    (0, 0, 0, 0), (0, 1, 0, 0), (0, 2, 0, 0), (1, 0, 0, 0), (1, 1, 0, 0), (1, 2, 0, 0), (2, 0, 0, 0), (2, 1, 0, 0),
    (2, 2, 0, 0), (5, 0, 3, 0), (4, 0, 3, 0), (4, 1, 3, 0), (5, 1, 3, 0), (3, 0, 2, 0), (3, 2, 1, 0), (3, 2, 2, 0),
    (3, 0, 1, 0), (3, 2, 0, 0), (5, 0, 3, 1), (3, 0, 0, 0), (5, 1, 3, 1), (5, 0, 1, 0), (5, 0, 2, 0), (4, 0, 1, 0),
    (4, 0, 2, 0), (3, 1, 2, 0), (5, 0, 0, 0), (3, 1, 1, 0), (4, 0, 0, 0), (5, 1, 1, 0), (5, 0, 1, 1), (5, 0, 2, 1),
    (5, 1, 2, 0), (3, 1, 0, 0), (4, 2, 3, 0), (4, 1, 2, 0), (5, 2, 3, 0), (4, 2, 1, 0), (5, 1, 0, 0), (5, 2, 1, 0),
    (4, 1, 1, 0), (5, 1, 2, 1), (4, 2, 2, 0), (5, 2, 2, 0), (4, 1, 0, 0), (5, 0, 0, 1), (4, 2, 0, 0), (5, 1, 1, 1),
    (5, 2, 0, 0), (5, 2, 3, 1), (5, 2, 1, 1), (5, 1, 0, 1), (5, 2, 2, 1), (5, 2, 0, 1),
)
HALF = ((1, 1), (1, 0), (0, 1), (0, 0))


def parts_of(rows, tiles):
    full = rows // TILE
    part = [max(1, full * n // sum(tiles)) * TILE for n in tiles[:-1]]
    return part + [rows - sum(part)]


def padded(n, unit):
    return -(-n // unit) * unit


def over_rows(rows, group, body):
    size = group * TILE
    whole = rows // size

    def step(i, carry):
        body(pl.multiple_of(i * size, size), size)
        return carry

    if whole:
        lax.fori_loop(0, whole, step, 0)
    at = whole * size
    if rows - at >= TILE:
        body(at, (rows - at) // TILE * TILE)
        at += (rows - at) // TILE * TILE
    if rows > at:
        body(at, rows - at)


def half_of(at):
    return at // 2 if isinstance(at, int) else lax.div(at, 2)


def kernel(rows, grad_hbm, w_hbm, m_hbm, v_hbm, d_hbm, lr_ref, full, w, m, v, norm_ref, *scratch):
    count = len(REDUCE)
    stages = scratch[:STAGES]
    scratch = scratch[STAGES:]
    got1, kept, sent2, got2, got3 = (scratch[count * i:count * i + count] for i in range(5))
    (row, mean, d, partial, stage_sem, state_sem, s1, r1, s2, r2, s3, r3, ns, nr,
     gs1, gr1, gs2, gr2, gs3, gr3, gs4, gr4) = scratch[5 * count:]
    part = parts_of(rows, REDUCE_TILES)
    first = [sum(part[:i]) for i in range(count)]
    units = rows // 2
    gather_part = parts_of(rows, GATHER_TILES)
    gather_first = [sum(gather_part[:i]) for i in range(len(gather_part))]

    me = lax.axis_index('dp')
    bits = (lax.div(me, 16), lax.rem(lax.div(me, 8), 2), lax.rem(lax.div(me, 4), 2), lax.rem(lax.div(me, 2), 2),
            lax.rem(me, 2))

    def across(*flips):
        total = 0
        for bit in range(5):
            value = 1 - bits[bit] if bit in flips else bits[bit]
            total = total * 2 + value
        return total

    def pick(axes, values):
        return tuple(a for a, val in zip(axes, values) if val)

    def where(colour, g, j2, j1, jc):
        axes, groups = colour
        return pick(axes + (CORE,), (j1, j2) + groups[g] + (jc,))

    def send(src, dst, send_sem, recv_sem, flips):
        return pltpu.make_async_remote_copy(
            src_ref=src, dst_ref=dst, send_sem=send_sem, recv_sem=recv_sem,
            device_id=(across(*flips),), device_id_type=MESH)

    waited = set()

    def need(copy_of, *key):
        if (copy_of.__name__,) + key not in waited:
            waited.add((copy_of.__name__,) + key)
            copy_of(*key).wait_recv()

    def state_copy(i):
        return pltpu.make_async_copy((w_hbm, m_hbm, v_hbm, d_hbm)[i], (w, m, v, d)[i], state_sem.at[i])

    work = [task[1:] for task in REDUCE_ORDER if task[0] == 0]
    spans = []
    for lead in range(2):
        inside = [i for i in range(count) if SPAN_OF[i] == lead]
        spans.append((inside[0], first[inside[0]], sum(part[i] for i in inside)))

    def stage_copy(i):
        span, g, j2, j1, jc = work[i]
        c, begin, length = spans[span]
        k = across(*where(REDUCE[c], g, j2, j1, jc))
        at = pl.multiple_of((k * rows + begin) * LANES, LANES)
        return pltpu.make_async_copy(grad_hbm.at[:, pl.ds(at, length * LANES)],
                                     stages[i % STAGES].at[:, pl.ds(0, length * LANES)], stage_sem.at[i % STAGES])

    def first_copy(c, g, j2, slot):
        j1 = 1 if slot else 0
        jc = 0 if slot == 1 else 1
        k = across(*where(REDUCE[c], g, j2, j1, jc))
        return send(row.at[k, pl.ds(first[c], padded(part[c], TILE))], got1[c].at[g, j2, slot],
                    s1.at[c, g, j2, slot], r1.at[c, g, j2, slot], pick((REDUCE[c][0][0], CORE), (j1, jc)))

    def second_copy(c, g):
        return send(sent2[c].at[g], got2[c].at[g], s2.at[c, g], r2.at[c, g], (REDUCE[c][0][1],))

    def third_copy(c, g):
        return send(kept[c].at[g], got3[c].at[g], s3.at[c, g], r3.at[c, g], pick(REDUCE[c][0][2:], REDUCE[c][1][g]))

    def pack(i):
        span, g, j2, j1, jc = work[i]
        c, begin, length = spans[span]
        k = across(*where(REDUCE[c], g, j2, j1, jc))
        source = stages[i % STAGES]
        stage_copy(i).wait()

        def body(at, size):
            lane = at * LANES
            if not isinstance(at, int):
                lane = pl.multiple_of(lane, TILE * LANES)
            val = source[:, pl.ds(lane, size * LANES)].astype(F32).reshape(size, LANES)
            row[k, pl.ds(begin + at, size), :] = val.astype(BF16)

        over_rows(length, 4, body)
        if i + STAGES < len(work):
            stage_copy(i + STAGES).start()

    def four_sum(c, g, j2, target):
        for slot in (0, 1, 2):
            need(first_copy, c, g, j2, slot)
        k = across(*where(REDUCE[c], g, j2, 0, 0))

        def body(at, size):
            near = pl.ds(at, size)
            mine = row[k, pl.ds(first[c] + at, size), :].astype(F32) + got1[c][g, j2, 0, near, :].astype(F32)
            other = got1[c][g, j2, 1, near, :].astype(F32) + got1[c][g, j2, 2, near, :].astype(F32)
            target[g, near, :] = mine + other

        over_rows(part[c], 4, body)

    def plane_sum(c, g):
        need(second_copy, c, g)

        def body(at, size):
            near = pl.ds(at, size)
            kept[c][g, near, :] = kept[c][g, near, :] + got2[c][g, near, :]

        if g < 3:
            over_rows(part[c], 4, body)
            third_copy(c, g).start()

    def final(c, acc):
        for g in range(3):
            need(third_copy, c, g)

        def mean_of(at, size):
            near = pl.ds(at, size)
            total = (kept[c][3, near, :] + got2[c][3, near, :]) + (got3[c][0, near, :] + got3[c][1, near, :])
            total = (total + got3[c][2, near, :]) * (1.0 / 32.0)
            mean[pl.ds(first[c] + at, size), :] = total
            return total * total

        def fold(val):
            return jnp.sum(val.reshape(val.shape[0] // 8, 8, LANES), axis=0)

        whole = part[c] // 64
        if whole:
            acc = lax.fori_loop(0, whole, lambda i, a: a + fold(mean_of(pl.multiple_of(i * 64, 64), 64)), acc)
        at = whole * 64
        if part[c] - at >= 8:
            size = (part[c] - at) // 8 * 8
            acc = acc + fold(mean_of(at, size))
            at += size
        if part[c] > at:
            tail = mean_of(at, part[c] - at)
            acc = acc + jnp.concatenate([tail, jnp.zeros((8 - tail.shape[0], LANES), F32)], axis=0)
        return acc

    everyone = [pick((HIGH, LOW, Y, X, CORE), [(n >> b) & 1 for b in (4, 3, 2, 1, 0)]) for n in range(1, 32)]

    for i in range(STAGES):
        stage_copy(i).start()
    barrier = pltpu.get_barrier_semaphore()
    for flips in everyone:
        pl.semaphore_signal(barrier, inc=1, device_id=(across(*flips),), device_id_type=MESH)

    acc = jnp.zeros((8, LANES), F32)
    packed = 0
    entered = False
    for task in REDUCE_ORDER:
        kind, c, g = task[:3]
        if kind == 0:
            pack(packed)
            packed += 1
            if packed == len(work):
                for i in range(4):
                    state_copy(i).start()
        elif kind == 1:
            if not entered:
                pl.semaphore_wait(barrier, 31)
                entered = True
            j2, slot, h = task[3:]
            if h >= 0:
                for other in range(3):
                    need(first_copy, c, h // 2, 1 - h % 2, other)
            first_copy(c, g, j2, slot).start()
        elif kind == 2:
            four_sum(c, g, 1, sent2[c])
            second_copy(c, g).start()
        elif kind == 3:
            four_sum(c, g, 0, kept[c])
        elif kind == 4:
            plane_sum(c, g)
        else:
            acc = final(c, acc)

    partial[me] = acc

    def norm_copy(j, owner):
        return send(partial.at[owner], partial.at[owner], ns.at[j], nr.at[j], everyone[j])

    for j in range(31):
        norm_copy(j, me).start()
    for i in range(4):
        state_copy(i).wait()
    for j in range(31):
        norm_copy(j, across(*everyone[j])).wait_recv()
    norm = jnp.sqrt(jnp.full((1, LANES), jnp.sum(jnp.sum(partial[...], axis=0)), F32))
    norm_ref[...] = norm
    coef = jnp.minimum(1.0, 1.0 / (norm + CLIP_EPS))
    lr = lr_ref[0]

    def update(c):
        def body(at, size):
            near = pl.ds(gather_first[c] + at, size)
            h = mean[near, :] * coef
            nm = BETA_FIRST * m[near, :] + (1.0 - BETA_FIRST) * h
            nv = BETA_SECOND * v[near, :] + (1.0 - BETA_SECOND) * h * h
            step = (nm * (1.0 / (1.0 - BETA_FIRST ** ADAM_STEP))) / (
                jnp.sqrt(nv * (1.0 / (1.0 - BETA_SECOND ** ADAM_STEP))) + ADAM_EPS)
            old = w[near, :]
            nw = old - lr * (step + WEIGHT_DECAY * d[near, :].astype(F32) * old)
            m[near, :] = nm
            v[near, :] = nv
            w[near, :] = nw
            full[pl.ds(me * units + gather_first[c] // 2 + half_of(at), size // 2)] = nw.astype(BF16).reshape(
                size // 2, 2, LANES)

        over_rows(gather_part[c], 2, body)

    def piece(c, g, j2, j1):
        k = across(*where(GATHER[c], g, j2, j1, 0))
        return full.at[pl.ds(k * units + gather_first[c] // 2, gather_part[c] // 2)]

    def gather1(c, g):
        spot = piece(c, 3, 0, 0)
        return send(spot, spot, gs1.at[c, g], gr1.at[c, g], pick(GATHER[c][0][2:], GATHER[c][1][g]))

    def gather1_in(c, g):
        spot = piece(c, g, 0, 0)
        return send(spot, spot, gs1.at[c, g], gr1.at[c, g], pick(GATHER[c][0][2:], GATHER[c][1][g]))

    def gather2(c, g):
        spot = piece(c, g, 0, 0)
        return send(spot, spot, gs2.at[c, g], gr2.at[c, g], (GATHER[c][0][1],))

    def gather3(c, g, j2):
        spot = piece(c, g, j2, 0)
        return send(spot, spot, gs3.at[c, g, j2], gr3.at[c, g, j2], (GATHER[c][0][0],))

    def gather4(c, g, j2, j1):
        spot = piece(c, g, j2, j1)
        return send(spot, spot, gs4.at[c, g, j2, j1], gr4.at[c, g, j2, j1], (CORE,))

    for kind, c, g, j2 in GATHER_ORDER:
        if kind == 0:
            update(c)
        elif kind == 1:
            for group in (2, 1, 0):
                gather1(c, group).start()
            gather2(c, 3).start()
            gather3(c, 3, 0).start()
        elif kind == 2:
            gather4(c, 3, 0, 0).start()
        elif kind == 3:
            gather1_in(c, g).wait_recv()
            gather2(c, g).start()
            gather3(c, g, 0).start()
            gather4(c, g, 0, 0).start()
        elif kind == 4:
            gather2(c, g).wait_recv()
            gather3(c, g, 1).start()
            gather4(c, g, 1, 0).start()
        else:
            gather3(c, g, j2).wait_recv()
            gather4(c, g, j2, 1).start()

    for c in range(count):
        for g in range(4):
            for j2 in (0, 1):
                for slot in range(3):
                    first_copy(c, g, j2, slot).wait_send()
            second_copy(c, g).wait_send()
        for g in range(3):
            third_copy(c, g).wait_send()
    for j in range(31):
        norm_copy(j, me).wait_send()
    for c in range(len(GATHER)):
        for g in range(3):
            gather1(c, g).wait_send()
        for g in range(4):
            gather2(c, g).wait_send()
            for j2 in (0, 1):
                gather3(c, g, j2).wait_send()
                for j1 in (0, 1):
                    gather4(c, g, j2, j1).wait()


def write_out(*refs):
    sem = refs[-1]
    count = len(refs) // 2
    copies = [pltpu.make_async_copy(refs[i], refs[count + i], sem.at[i]) for i in range(count)]
    for copy in copies:
        copy.start()
    for copy in copies:
        copy.wait()


def solution(mesh):
    num_dev = mesh.shape['dp']

    def local_step(grad_row, master, mom_first, mom_second, decay_mask, learn_rate):
        shard_len = master.shape[0]
        rows = shard_len // LANES
        part = parts_of(rows, REDUCE_TILES)
        dma = pltpu.SemaphoreType.DMA
        hbm = pl.BlockSpec(memory_space=pltpu.HBM)
        vmem = pl.BlockSpec(memory_space=pltpu.VMEM)
        flat = (rows, LANES)
        whole = (num_dev * rows // 2, 2, LANES)
        n = len(REDUCE)
        longest = max(sum(part[i] for i in range(n) if SPAN_OF[i] == lead) for lead in range(2))
        k = len(GATHER)
        results = pl.pallas_call(
            functools.partial(kernel, rows),
            out_shape=(pltpu.VMEM(whole, BF16), pltpu.VMEM(flat, F32), pltpu.VMEM(flat, F32), pltpu.VMEM(flat, F32),
                       pltpu.VMEM((1, LANES), F32)),
            in_specs=[hbm] * 5 + [pl.BlockSpec(memory_space=pltpu.SMEM)],
            out_specs=(vmem,) * 5,
            scratch_shapes=[pltpu.VMEM((1, longest * LANES), BF16)] * STAGES
            + [pltpu.VMEM((4, 2, 3, padded(p, TILE), LANES), BF16) for p in part]
            + [pltpu.VMEM((groups, padded(p, 8), LANES), F32) for groups in (4, 4, 4, 3) for p in part]
            + [
                pltpu.VMEM((num_dev, padded(rows, TILE), LANES), BF16), pltpu.VMEM(flat, F32),
                pltpu.VMEM(flat, jnp.int32), pltpu.VMEM((num_dev, 8, LANES), F32),
                dma((STAGES,)), dma((4,)),
                dma((n, 4, 2, 3)), dma((n, 4, 2, 3)), dma((n, 4)), dma((n, 4)), dma((n, 3)), dma((n, 3)),
                dma((num_dev - 1,)), dma((num_dev - 1,)),
                dma((k, 3)), dma((k, 3)), dma((k, 4)), dma((k, 4)), dma((k, 4, 2)), dma((k, 4, 2)),
                dma((k, 4, 2, 2)), dma((k, 4, 2, 2)),
            ],
            compiler_params=pltpu.CompilerParams(
                collective_id=0, has_side_effects=True, vmem_limit_bytes=VMEM_LIMIT),
        )(grad_row, master.reshape(flat), mom_first.reshape(flat), mom_second.reshape(flat), decay_mask.reshape(flat), learn_rate)
        state = jax.ShapeDtypeStruct(flat, F32)
        params, new_master, new_first, new_second, norm = pl.pallas_call(
            write_out,
            out_shape=(jax.ShapeDtypeStruct(whole, BF16), state, state, state, jax.ShapeDtypeStruct((1, LANES), F32)),
            in_specs=[vmem] * 5,
            out_specs=(hbm,) * 5,
            scratch_shapes=[dma((5,))],
            compiler_params=pltpu.CompilerParams(vmem_limit_bytes=1024 * 1024),
        )(*results)
        return (params.reshape(num_dev * shard_len), new_master.reshape(shard_len), new_first.reshape(shard_len),
                new_second.reshape(shard_len), norm[0, :1])

    return jax.shard_map(local_step, mesh=mesh, in_specs=(P('dp', None), P('dp'), P('dp'), P('dp'), P('dp'), P()),
                         out_specs=(P(), P('dp'), P('dp'), P('dp'), P()), check_vma=False)
```

```python
import functools

import jax
import jax.numpy as jnp
from jax import lax
from jax.experimental import pallas as pl
from jax.experimental.pallas import tpu as pltpu
from jax.sharding import PartitionSpec as P

BETA_FIRST = 0.9
BETA_SECOND = 0.95
ADAM_EPS = 1e-8
CLIP_EPS = 1e-6
WEIGHT_DECAY = 0.1
ADAM_STEP = 10
LANES = 128
TILE = 16
STAGES = 4
VMEM_LIMIT = 46 * 1024 * 1024
MESH = pl.DeviceIdType.MESH
F32 = jnp.float32
BF16 = jnp.bfloat16

HIGH, LOW, Y, X, CORE = range(5)
REDUCE = (
    ((X, Y, LOW, HIGH), ((1, 1), (1, 0), (0, 1), (0, 0))),
    ((Y, X, LOW, HIGH), ((1, 1), (1, 0), (0, 1), (0, 0))),
    ((LOW, HIGH, X, Y), ((1, 1), (1, 0), (0, 1), (0, 0))),
)
REDUCE_TILES = (47, 47, 20)
SPAN_OF = (0, 0, 1)
GATHER = (
    ((X, Y, LOW, HIGH), ((1, 1), (0, 1), (1, 0), (0, 0))),
    ((Y, X, LOW, HIGH), ((1, 1), (0, 1), (1, 0), (0, 0))),
    ((LOW, HIGH, X, Y), ((1, 0), (1, 1), (0, 1), (0, 0))),
)
GATHER_TILES = (48, 48, 18)
REDUCE_ORDER = (
    (0, 1, 0, 1, 1, 1), (0, 0, 0, 1, 1, 1), (1, 0, 0, 1, 2), (1, 1, 0, 1, 2), (0, 1, 0, 1, 1, 0), (1, 2, 0, 1, 2),
    (0, 0, 0, 1, 1, 0), (1, 0, 0, 1, 1), (0, 1, 0, 1, 0, 1), (0, 0, 0, 1, 0, 1), (0, 1, 0, 1, 0, 0),
    (0, 0, 0, 1, 0, 0), (1, 1, 0, 0, 1), (1, 2, 0, 1, 1), (0, 1, 0, 0, 1, 1), (0, 0, 0, 0, 1, 1),
    (0, 1, 0, 0, 1, 0), (0, 0, 0, 0, 1, 0), (1, 2, 0, 0, 1), (0, 1, 0, 0, 0, 1), (0, 0, 0, 0, 0, 1),
    (0, 1, 0, 0, 0, 0), (0, 0, 0, 0, 0, 0), (0, 1, 1, 1, 1, 1), (0, 0, 1, 1, 1, 1), (1, 1, 0, 1, 1),
    (1, 1, 0, 1, 0), (1, 0, 0, 0, 2), (0, 1, 1, 1, 1, 0), (1, 2, 1, 1, 1), (0, 0, 1, 1, 1, 0), (1, 2, 0, 0, 2),
    (1, 0, 0, 1, 0), (1, 2, 0, 0, 0), (0, 1, 1, 1, 0, 1), (1, 0, 0, 0, 1), (1, 2, 1, 1, 0), (1, 2, 0, 1, 0),
    (1, 1, 0, 0, 2), (0, 0, 1, 1, 0, 1), (0, 1, 1, 1, 0, 0), (1, 1, 0, 0, 0), (0, 0, 1, 1, 0, 0), (1, 1, 1, 1, 1),
    (0, 1, 1, 0, 1, 1), (0, 0, 1, 0, 1, 1), (0, 1, 1, 0, 1, 0), (0, 0, 1, 0, 1, 0), (0, 1, 1, 0, 0, 1),
    (0, 0, 1, 0, 0, 1), (0, 1, 1, 0, 0, 0), (2, 2, 0), (0, 0, 1, 0, 0, 0), (1, 2, 1, 0, 2), (0, 1, 2, 1, 1, 1),
    (0, 0, 2, 1, 1, 1), (1, 2, 1, 1, 2), (1, 1, 2, 1, 2), (1, 0, 1, 1, 0), (0, 1, 2, 1, 1, 0), (3, 2, 0),
    (1, 2, 1, 0, 0), (0, 0, 2, 1, 1, 0), (0, 1, 2, 1, 0, 1), (0, 0, 2, 1, 0, 1), (4, 2, 0), (2, 1, 0), (3, 1, 0),
    (0, 1, 2, 1, 0, 0), (0, 0, 2, 1, 0, 0), (2, 0, 0), (1, 1, 1, 0, 1), (0, 1, 2, 0, 1, 1), (1, 0, 1, 1, 2),
    (1, 2, 2, 1, 2), (0, 0, 2, 0, 1, 1), (1, 2, 2, 1, 0), (0, 1, 2, 0, 1, 0), (0, 0, 2, 0, 1, 0),
    (0, 1, 2, 0, 0, 1), (1, 0, 2, 0, 1), (3, 0, 0), (0, 0, 2, 0, 0, 1), (1, 2, 2, 1, 1), (1, 0, 0, 0, 0),
    (1, 1, 2, 0, 0), (1, 0, 2, 1, 0), (1, 2, 1, 0, 1), (0, 1, 2, 0, 0, 0), (0, 0, 2, 0, 0, 0), (0, 1, 3, 1, 1, 1),
    (1, 0, 1, 1, 1), (0, 0, 3, 1, 1, 1), (0, 1, 3, 1, 1, 0), (2, 2, 1), (3, 2, 1), (4, 0, 0), (1, 0, 2, 0, 2),
    (1, 0, 1, 0, 2), (5, 2, 0), (1, 1, 1, 1, 2), (0, 0, 3, 1, 1, 0), (0, 1, 3, 1, 0, 1), (0, 0, 3, 1, 0, 1),
    (1, 1, 3, 0, 2), (2, 2, 2), (1, 2, 2, 0, 1), (0, 1, 3, 1, 0, 0), (0, 0, 3, 1, 0, 0), (4, 1, 0), (5, 1, 0),
    (1, 2, 2, 0, 2), (0, 1, 3, 0, 1, 1), (0, 0, 3, 0, 1, 1), (1, 1, 1, 0, 0), (0, 1, 3, 0, 1, 0), (1, 2, 3, 0, 1),
    (1, 2, 3, 1, 1), (6, 1, 0), (0, 0, 3, 0, 1, 0), (0, 1, 3, 0, 0, 1), (2, 0, 1), (1, 2, 3, 1, 0), (1, 1, 2, 1, 1),
    (4, 2, 1), (5, 0, 0), (1, 0, 3, 0, 2), (1, 2, 2, 0, 0), (0, 0, 3, 0, 0, 1), (0, 1, 3, 0, 0, 0), (5, 2, 1),
    (4, 2, 2), (1, 2, 3, 1, 2), (1, 2, 3, 0, 2), (6, 0, 0), (1, 0, 1, 0, 1), (1, 1, 1, 1, 0), (3, 2, 2),
    (1, 1, 2, 1, 0), (1, 2, 3, 0, 0), (1, 1, 2, 0, 1), (1, 0, 2, 1, 2), (0, 0, 3, 0, 0, 0), (1, 0, 2, 0, 0),
    (1, 1, 1, 0, 2), (1, 0, 1, 0, 0), (1, 1, 3, 1, 0), (1, 1, 3, 1, 1), (2, 1, 2), (2, 1, 1), (3, 1, 1),
    (1, 0, 3, 1, 0), (4, 1, 1), (1, 0, 2, 1, 1), (3, 0, 1), (5, 1, 1), (1, 0, 3, 0, 0), (6, 1, 1), (4, 0, 1),
    (2, 2, 3), (3, 2, 3), (1, 1, 2, 0, 2), (3, 1, 2), (5, 0, 1), (1, 1, 3, 0, 1), (6, 2, 1), (2, 0, 2), (3, 0, 2),
    (4, 1, 2), (4, 0, 2), (1, 0, 3, 1, 1), (5, 2, 2), (5, 1, 2), (6, 1, 2), (6, 0, 1), (6, 2, 0), (1, 1, 3, 0, 0),
    (1, 0, 3, 0, 1), (5, 0, 2), (4, 2, 3), (6, 0, 2), (6, 2, 2), (1, 1, 3, 1, 2), (1, 0, 3, 1, 2), (2, 1, 3),
    (2, 0, 3), (3, 0, 3), (3, 1, 3), (4, 1, 3), (4, 0, 3), (5, 0, 3), (5, 2, 3), (7, 2, 0), (5, 1, 3), (7, 1, 0),
    (7, 0, 0),
)
GATHER_ORDER = (
    (0, 2, 0), (1, 2, 1), (0, 0, 0), (1, 0, 2), (3, 0, 3, 0), (4, 2, 3, 0, 0), (1, 0, 0), (0, 1, 0), (2, 1, 3),
    (2, 0, 3), (3, 1, 3, 0), (3, 0, 3, 1), (1, 1, 1), (1, 2, 2), (3, 1, 3, 1), (1, 1, 2), (3, 0, 2, 0),
    (3, 0, 0, 0), (4, 0, 3, 0, 1), (1, 0, 1), (2, 0, 0), (2, 2, 2), (3, 1, 1, 0), (2, 1, 1), (2, 0, 2),
    (3, 1, 2, 0), (3, 2, 3, 0), (2, 1, 2), (4, 0, 1, 0, 0), (3, 2, 1, 0), (4, 1, 3, 0, 1), (1, 1, 0), (3, 0, 1, 0),
    (1, 2, 0), (4, 0, 0, 0, 1), (2, 0, 1), (4, 0, 0, 0, 0), (4, 2, 3, 0, 1), (3, 2, 2, 1), (4, 0, 3, 1, 0),
    (4, 1, 1, 1, 0), (3, 1, 1, 1), (3, 0, 0, 1), (4, 0, 3, 0, 0), (4, 0, 2, 0, 1), (4, 2, 1, 0, 1), (4, 1, 3, 0, 0),
    (4, 0, 1, 1, 0), (4, 2, 0, 0, 0), (4, 2, 2, 0, 0), (2, 2, 1), (4, 0, 2, 0, 0), (3, 2, 2, 0), (4, 2, 1, 0, 0),
    (2, 2, 3), (3, 0, 1, 1), (2, 1, 0), (3, 1, 2, 1), (3, 2, 1, 1), (4, 1, 1, 0, 1), (4, 2, 2, 1, 1), (3, 0, 2, 1),
    (4, 0, 1, 0, 1), (4, 1, 1, 1, 1), (2, 2, 0), (4, 1, 2, 1, 0), (3, 2, 0, 0), (4, 0, 0, 1, 0), (3, 1, 0, 0),
    (4, 0, 2, 1, 0), (4, 1, 3, 1, 1), (4, 1, 2, 1, 1), (4, 1, 3, 1, 0), (4, 2, 1, 1, 1), (4, 0, 1, 1, 1),
    (3, 1, 0, 1), (4, 0, 0, 1, 1), (4, 2, 2, 0, 1), (4, 2, 1, 1, 0), (4, 1, 2, 0, 1), (4, 1, 0, 0, 1),
    (4, 1, 2, 0, 0), (3, 2, 3, 1), (3, 2, 0, 1), (4, 2, 2, 1, 0), (4, 1, 0, 1, 0), (4, 2, 3, 1, 0), (4, 1, 0, 0, 0),
    (4, 0, 2, 1, 1), (4, 0, 3, 1, 1), (4, 1, 1, 0, 0), (4, 2, 0, 1, 0), (4, 2, 3, 1, 1), (4, 1, 0, 1, 1),
    (4, 2, 0, 0, 1), (4, 2, 0, 1, 1),
)
HALF = ((1, 1), (1, 0), (0, 1), (0, 0))


def parts_of(rows, tiles):
    full = rows // TILE
    part = [max(1, full * n // sum(tiles)) * TILE for n in tiles[:-1]]
    return part + [rows - sum(part)]


def padded(n, unit):
    return -(-n // unit) * unit


def over_rows(rows, group, body):
    size = group * TILE
    whole = rows // size

    def step(i, carry):
        body(pl.multiple_of(i * size, size), size)
        return carry

    if whole:
        lax.fori_loop(0, whole, step, 0)
    at = whole * size
    if rows - at >= TILE:
        body(at, (rows - at) // TILE * TILE)
        at += (rows - at) // TILE * TILE
    if rows > at:
        body(at, rows - at)


def half_of(at):
    return at // 2 if isinstance(at, int) else lax.div(at, 2)


def kernel(rows, grad_hbm, w_hbm, m_hbm, v_hbm, d_hbm, lr_ref, full, w, m, v, norm_ref, *scratch):
    count = len(REDUCE)
    stages = scratch[:STAGES]
    scratch = scratch[STAGES:]
    got1, kept, sent2, got2, got3 = (scratch[count * i:count * i + count] for i in range(5))
    (row, mean, d, partial, stage_sem, state_sem, s1, r1, s2, r2, s3, r3, ns, nr,
     gs1, gr1, gs2, gr2, gs3, gr3, gs4, gr4) = scratch[5 * count:]
    part = parts_of(rows, REDUCE_TILES)
    first = [sum(part[:i]) for i in range(count)]
    units = rows // 2
    gather_part = parts_of(rows, GATHER_TILES)
    gather_first = [sum(gather_part[:i]) for i in range(len(gather_part))]

    me = lax.axis_index('dp')
    bits = (lax.div(me, 16), lax.rem(lax.div(me, 8), 2), lax.rem(lax.div(me, 4), 2), lax.rem(lax.div(me, 2), 2),
            lax.rem(me, 2))

    def across(*flips):
        total = 0
        for bit in range(5):
            value = 1 - bits[bit] if bit in flips else bits[bit]
            total = total * 2 + value
        return total

    def pick(axes, values):
        return tuple(a for a, val in zip(axes, values) if val)

    def where(colour, g, j2, j1, jc):
        axes, groups = colour
        return pick(axes + (CORE,), (j1, j2) + groups[g] + (jc,))

    def send(src, dst, send_sem, recv_sem, flips):
        return pltpu.make_async_remote_copy(
            src_ref=src, dst_ref=dst, send_sem=send_sem, recv_sem=recv_sem,
            device_id=(across(*flips),), device_id_type=MESH)

    waited = set()

    def need(copy_of, *key):
        if (copy_of.__name__,) + key not in waited:
            waited.add((copy_of.__name__,) + key)
            copy_of(*key).wait_recv()

    def state_copy(i):
        return pltpu.make_async_copy((w_hbm, m_hbm, v_hbm, d_hbm)[i], (w, m, v, d)[i], state_sem.at[i])

    work = [task[1:] for task in REDUCE_ORDER if task[0] == 0]
    spans = []
    for lead in range(2):
        inside = [i for i in range(count) if SPAN_OF[i] == lead]
        spans.append((inside[0], first[inside[0]], sum(part[i] for i in inside)))

    def stage_copy(i):
        span, g, j2, j1, jc = work[i]
        c, begin, length = spans[span]
        k = across(*where(REDUCE[c], g, j2, j1, jc))
        at = pl.multiple_of((k * rows + begin) * LANES, LANES)
        return pltpu.make_async_copy(grad_hbm.at[:, pl.ds(at, length * LANES)],
                                     stages[i % STAGES].at[:, pl.ds(0, length * LANES)], stage_sem.at[i % STAGES])

    def first_copy(c, g, j2, slot):
        j1 = 1 if slot else 0
        jc = 0 if slot == 1 else 1
        k = across(*where(REDUCE[c], g, j2, j1, jc))
        return send(row.at[k, pl.ds(first[c], padded(part[c], TILE))], got1[c].at[g, j2, slot],
                    s1.at[c, g, j2, slot], r1.at[c, g, j2, slot], pick((REDUCE[c][0][0], CORE), (j1, jc)))

    def second_copy(c, g):
        return send(sent2[c].at[g], got2[c].at[g], s2.at[c, g], r2.at[c, g], (REDUCE[c][0][1],))

    def third_copy(c, g):
        return send(kept[c].at[g], got3[c].at[g], s3.at[c, g], r3.at[c, g], pick(REDUCE[c][0][2:], REDUCE[c][1][g]))

    def pack(i):
        span, g, j2, j1, jc = work[i]
        c, begin, length = spans[span]
        k = across(*where(REDUCE[c], g, j2, j1, jc))
        source = stages[i % STAGES]
        stage_copy(i).wait()

        def body(at, size):
            lane = at * LANES
            if not isinstance(at, int):
                lane = pl.multiple_of(lane, TILE * LANES)
            val = source[:, pl.ds(lane, size * LANES)].astype(F32).reshape(size, LANES)
            row[k, pl.ds(begin + at, size), :] = val.astype(BF16)

        over_rows(length, 4, body)
        if i + STAGES < len(work):
            stage_copy(i + STAGES).start()

    def four_sum(c, g, j2, target):
        for slot in (0, 1, 2):
            need(first_copy, c, g, j2, slot)
        k = across(*where(REDUCE[c], g, j2, 0, 0))

        def body(at, size):
            near = pl.ds(at, size)
            mine = row[k, pl.ds(first[c] + at, size), :].astype(F32) + got1[c][g, j2, 0, near, :].astype(F32)
            other = got1[c][g, j2, 1, near, :].astype(F32) + got1[c][g, j2, 2, near, :].astype(F32)
            target[g, near, :] = mine + other

        over_rows(part[c], 4, body)

    def plane_sum(c, g):
        need(second_copy, c, g)

        def body(at, size):
            near = pl.ds(at, size)
            kept[c][g, near, :] = kept[c][g, near, :] + got2[c][g, near, :]

        if g < 3:
            over_rows(part[c], 4, body)

    def final(c, acc):
        for g in range(3):
            need(third_copy, c, g)

        def mean_of(at, size):
            near = pl.ds(at, size)
            total = (kept[c][3, near, :] + got2[c][3, near, :]) + (got3[c][0, near, :] + got3[c][1, near, :])
            total = (total + got3[c][2, near, :]) * (1.0 / 32.0)
            mean[pl.ds(first[c] + at, size), :] = total
            return total * total

        def fold(val):
            return jnp.sum(val.reshape(val.shape[0] // 8, 8, LANES), axis=0)

        whole = part[c] // 64
        if whole:
            acc = lax.fori_loop(0, whole, lambda i, a: a + fold(mean_of(pl.multiple_of(i * 64, 64), 64)), acc)
        at = whole * 64
        if part[c] - at >= 8:
            size = (part[c] - at) // 8 * 8
            acc = acc + fold(mean_of(at, size))
            at += size
        if part[c] > at:
            tail = mean_of(at, part[c] - at)
            acc = acc + jnp.concatenate([tail, jnp.zeros((8 - tail.shape[0], LANES), F32)], axis=0)
        return acc

    everyone = [pick((HIGH, LOW, Y, X, CORE), [(n >> b) & 1 for b in (4, 3, 2, 1, 0)]) for n in range(1, 32)]

    for i in range(STAGES):
        stage_copy(i).start()
    barrier = pltpu.get_barrier_semaphore()
    for flips in everyone:
        pl.semaphore_signal(barrier, inc=1, device_id=(across(*flips),), device_id_type=MESH)

    acc = jnp.zeros((8, LANES), F32)
    packed = 0
    entered = False
    for task in REDUCE_ORDER:
        kind, c, g = task[:3]
        if kind == 0:
            pack(packed)
            packed += 1
            if packed == len(work):
                for i in range(4):
                    state_copy(i).start()
        elif kind == 1:
            if not entered:
                pl.semaphore_wait(barrier, 31)
                entered = True
            first_copy(c, g, *task[3:]).start()
        elif kind == 2:
            four_sum(c, g, 1, sent2[c])
        elif kind == 3:
            second_copy(c, g).start()
        elif kind == 4:
            four_sum(c, g, 0, kept[c])
        elif kind == 5:
            plane_sum(c, g)
        elif kind == 6:
            third_copy(c, g).start()
        else:
            acc = final(c, acc)

    partial[me] = acc

    def norm_copy(j, owner):
        return send(partial.at[owner], partial.at[owner], ns.at[j], nr.at[j], everyone[j])

    for j in range(31):
        norm_copy(j, me).start()
    for i in range(4):
        state_copy(i).wait()
    for j in range(31):
        norm_copy(j, across(*everyone[j])).wait_recv()
    norm = jnp.sqrt(jnp.full((1, LANES), jnp.sum(jnp.sum(partial[...], axis=0)), F32))
    norm_ref[...] = norm
    coef = jnp.minimum(1.0, 1.0 / (norm + CLIP_EPS))
    lr = lr_ref[0]

    def update(c):
        def body(at, size):
            near = pl.ds(gather_first[c] + at, size)
            h = mean[near, :] * coef
            nm = BETA_FIRST * m[near, :] + (1.0 - BETA_FIRST) * h
            nv = BETA_SECOND * v[near, :] + (1.0 - BETA_SECOND) * h * h
            step = (nm * (1.0 / (1.0 - BETA_FIRST ** ADAM_STEP))) / (
                jnp.sqrt(nv * (1.0 / (1.0 - BETA_SECOND ** ADAM_STEP))) + ADAM_EPS)
            old = w[near, :]
            nw = old - lr * (step + WEIGHT_DECAY * d[near, :].astype(F32) * old)
            m[near, :] = nm
            v[near, :] = nv
            w[near, :] = nw
            full[pl.ds(me * units + gather_first[c] // 2 + half_of(at), size // 2)] = nw.astype(BF16).reshape(
                size // 2, 2, LANES)

        over_rows(gather_part[c], 2, body)

    def piece(c, g, j2, j1):
        k = across(*where(GATHER[c], g, j2, j1, 0))
        return full.at[pl.ds(k * units + gather_first[c] // 2, gather_part[c] // 2)]

    def gather1(c, g):
        spot = piece(c, 3, 0, 0)
        return send(spot, spot, gs1.at[c, g], gr1.at[c, g], pick(GATHER[c][0][2:], GATHER[c][1][g]))

    def gather1_in(c, g):
        spot = piece(c, g, 0, 0)
        return send(spot, spot, gs1.at[c, g], gr1.at[c, g], pick(GATHER[c][0][2:], GATHER[c][1][g]))

    def gather2(c, g):
        spot = piece(c, g, 0, 0)
        return send(spot, spot, gs2.at[c, g], gr2.at[c, g], (GATHER[c][0][1],))

    def gather3(c, g, j2):
        spot = piece(c, g, j2, 0)
        return send(spot, spot, gs3.at[c, g, j2], gr3.at[c, g, j2], (GATHER[c][0][0],))

    def gather4(c, g, j2, j1):
        spot = piece(c, g, j2, j1)
        return send(spot, spot, gs4.at[c, g, j2, j1], gr4.at[c, g, j2, j1], (CORE,))

    for kind, c, *key in GATHER_ORDER:
        if kind == 0:
            update(c)
        elif kind == 1:
            gather1(c, *key).start()
        else:
            if kind == 4 and key[2]:
                need(gather3, c, *key[:2])
            elif kind > 2 and key[1]:
                need(gather2, c, key[0])
            elif key[0] < 3:
                need(gather1_in, c, key[0])
            (gather2, gather3, gather4)[kind - 2](c, *key).start()

    for c in range(count):
        for g in range(4):
            for j2 in (0, 1):
                for slot in range(3):
                    first_copy(c, g, j2, slot).wait_send()
            second_copy(c, g).wait_send()
        for g in range(3):
            third_copy(c, g).wait_send()
    for j in range(31):
        norm_copy(j, me).wait_send()
    for c in range(len(GATHER)):
        for g in range(3):
            gather1(c, g).wait_send()
        for g in range(4):
            gather2(c, g).wait_send()
            for j2 in (0, 1):
                gather3(c, g, j2).wait_send()
                for j1 in (0, 1):
                    gather4(c, g, j2, j1).wait()


def write_out(*refs):
    sem = refs[-1]
    count = len(refs) // 2
    copies = [pltpu.make_async_copy(refs[i], refs[count + i], sem.at[i]) for i in range(count)]
    for copy in copies:
        copy.start()
    for copy in copies:
        copy.wait()


def solution(mesh):
    num_dev = mesh.shape['dp']

    def local_step(grad_row, master, mom_first, mom_second, decay_mask, learn_rate):
        shard_len = master.shape[0]
        rows = shard_len // LANES
        part = parts_of(rows, REDUCE_TILES)
        dma = pltpu.SemaphoreType.DMA
        hbm = pl.BlockSpec(memory_space=pltpu.HBM)
        vmem = pl.BlockSpec(memory_space=pltpu.VMEM)
        flat = (rows, LANES)
        whole = (num_dev * rows // 2, 2, LANES)
        n = len(REDUCE)
        longest = max(sum(part[i] for i in range(n) if SPAN_OF[i] == lead) for lead in range(2))
        k = len(GATHER)
        results = pl.pallas_call(
            functools.partial(kernel, rows),
            out_shape=(pltpu.VMEM(whole, BF16), pltpu.VMEM(flat, F32), pltpu.VMEM(flat, F32), pltpu.VMEM(flat, F32),
                       pltpu.VMEM((1, LANES), F32)),
            in_specs=[hbm] * 5 + [pl.BlockSpec(memory_space=pltpu.SMEM)],
            out_specs=(vmem,) * 5,
            scratch_shapes=[pltpu.VMEM((1, longest * LANES), BF16)] * STAGES
            + [pltpu.VMEM((4, 2, 3, padded(p, TILE), LANES), BF16) for p in part]
            + [pltpu.VMEM((groups, padded(p, 8), LANES), F32) for groups in (4, 4, 4, 3) for p in part]
            + [
                pltpu.VMEM((num_dev, padded(rows, TILE), LANES), BF16), pltpu.VMEM(flat, F32),
                pltpu.VMEM(flat, jnp.int32), pltpu.VMEM((num_dev, 8, LANES), F32),
                dma((STAGES,)), dma((4,)),
                dma((n, 4, 2, 3)), dma((n, 4, 2, 3)), dma((n, 4)), dma((n, 4)), dma((n, 3)), dma((n, 3)),
                dma((num_dev - 1,)), dma((num_dev - 1,)),
                dma((k, 3)), dma((k, 3)), dma((k, 4)), dma((k, 4)), dma((k, 4, 2)), dma((k, 4, 2)),
                dma((k, 4, 2, 2)), dma((k, 4, 2, 2)),
            ],
            compiler_params=pltpu.CompilerParams(
                collective_id=0, has_side_effects=True, vmem_limit_bytes=VMEM_LIMIT),
        )(grad_row, master.reshape(flat), mom_first.reshape(flat), mom_second.reshape(flat), decay_mask.reshape(flat), learn_rate)
        state = jax.ShapeDtypeStruct(flat, F32)
        params, new_master, new_first, new_second, norm = pl.pallas_call(
            write_out,
            out_shape=(jax.ShapeDtypeStruct(whole, BF16), state, state, state, jax.ShapeDtypeStruct((1, LANES), F32)),
            in_specs=[vmem] * 5,
            out_specs=(hbm,) * 5,
            scratch_shapes=[dma((5,))],
            compiler_params=pltpu.CompilerParams(vmem_limit_bytes=1024 * 1024),
        )(*results)
        return (params.reshape(num_dev * shard_len), new_master.reshape(shard_len), new_first.reshape(shard_len),
                new_second.reshape(shard_len), norm[0, :1])

    return jax.shard_map(local_step, mesh=mesh, in_specs=(P('dp', None), P('dp'), P('dp'), P('dp'), P('dp'), P()),
                         out_specs=(P(), P('dp'), P('dp'), P('dp'), P()), check_vma=False)
```

```python
import functools

import jax
import jax.numpy as jnp
from jax import lax
from jax.experimental import pallas as pl
from jax.experimental.pallas import tpu as pltpu
from jax.sharding import PartitionSpec as P

BETA_FIRST = 0.9
BETA_SECOND = 0.95
ADAM_EPS = 1e-8
CLIP_EPS = 1e-6
WEIGHT_DECAY = 0.1
ADAM_STEP = 10
LANES = 128
TILE = 16
STAGES = 4
CHUNKS = 8
VMEM_LIMIT = 46 * 1024 * 1024
MESH = pl.DeviceIdType.MESH
F32 = jnp.float32
BF16 = jnp.bfloat16

HIGH, LOW, Y, X, CORE = range(5)
REDUCE = (
    ((X, Y, LOW, HIGH), ((1, 1), (1, 0), (0, 1), (0, 0))),
    ((Y, X, LOW, HIGH), ((1, 1), (1, 0), (0, 1), (0, 0))),
    ((LOW, HIGH, X, Y), ((1, 1), (1, 0), (0, 1), (0, 0))),
)
REDUCE_TILES = (47, 47, 20)
SPAN_OF = (0, 0, 1)
GATHER = (
    ((X, Y, LOW, HIGH), ((1, 1), (0, 1), (1, 0), (0, 0))),
    ((Y, X, LOW, HIGH), ((1, 1), (0, 1), (1, 0), (0, 0))),
    ((LOW, HIGH, X, Y), ((1, 0), (1, 1), (0, 1), (0, 0))),
)
GATHER_TILES = (48, 48, 18)
REDUCE_ORDER = (
    (0, 1, 0, 1, 1, 1), (0, 0, 0, 1, 1, 1), (1, 1, 0, 1, 2), (1, 0, 0, 1, 2), (0, 1, 0, 1, 1, 0), (1, 2, 0, 1, 1),
    (0, 0, 0, 1, 1, 0), (0, 1, 0, 1, 0, 1), (1, 2, 0, 1, 2), (1, 1, 0, 1, 1), (1, 2, 0, 1, 0), (0, 0, 0, 1, 0, 1),
    (0, 1, 0, 1, 0, 0), (0, 0, 0, 1, 0, 0), (0, 1, 0, 0, 1, 1), (0, 0, 0, 0, 1, 1), (0, 1, 0, 0, 1, 0),
    (0, 0, 0, 0, 1, 0), (1, 0, 0, 0, 1), (0, 1, 0, 0, 0, 1), (0, 0, 0, 0, 0, 1), (0, 1, 0, 0, 0, 0),
    (0, 0, 0, 0, 0, 0), (0, 1, 1, 1, 1, 1), (0, 0, 1, 1, 1, 1), (1, 2, 1, 1, 2), (0, 1, 1, 1, 1, 0),
    (1, 2, 1, 1, 1), (0, 0, 1, 1, 1, 0), (0, 1, 1, 1, 0, 1), (0, 0, 1, 1, 0, 1), (0, 1, 1, 1, 0, 0),
    (1, 0, 0, 1, 0), (0, 0, 1, 1, 0, 0), (0, 1, 1, 0, 1, 1), (2, 2, 0), (0, 0, 1, 0, 1, 1), (0, 1, 1, 0, 1, 0),
    (1, 2, 0, 0, 2), (1, 1, 0, 0, 2), (0, 0, 1, 0, 1, 0), (0, 1, 1, 0, 0, 1), (0, 0, 1, 0, 0, 1), (1, 1, 0, 1, 0),
    (1, 0, 0, 1, 1), (0, 1, 1, 0, 0, 0), (1, 1, 1, 1, 0), (0, 0, 1, 0, 0, 0), (0, 1, 2, 1, 1, 1),
    (0, 0, 2, 1, 1, 1), (2, 1, 0), (3, 2, 0), (1, 2, 1, 1, 0), (1, 0, 0, 0, 2), (3, 1, 0), (0, 1, 2, 1, 1, 0),
    (0, 0, 2, 1, 1, 0), (0, 1, 2, 1, 0, 1), (1, 2, 2, 1, 1), (1, 1, 0, 0, 1), (1, 2, 2, 1, 2), (0, 0, 2, 1, 0, 1),
    (0, 1, 2, 1, 0, 0), (0, 0, 2, 1, 0, 0), (1, 1, 2, 0, 1), (1, 1, 1, 0, 0), (0, 1, 2, 0, 1, 1),
    (0, 0, 2, 0, 1, 1), (0, 1, 2, 0, 1, 0), (2, 0, 0), (3, 0, 0), (1, 1, 2, 1, 0), (2, 2, 1), (1, 0, 0, 0, 0),
    (1, 1, 1, 0, 2), (1, 2, 0, 0, 0), (1, 0, 2, 0, 2), (1, 1, 0, 0, 0), (0, 0, 2, 0, 1, 0), (1, 1, 2, 0, 2),
    (0, 1, 2, 0, 0, 1), (0, 0, 2, 0, 0, 1), (0, 1, 2, 0, 0, 0), (0, 0, 2, 0, 0, 0), (1, 0, 1, 0, 0),
    (0, 1, 3, 1, 1, 1), (3, 2, 1), (0, 0, 3, 1, 1, 1), (1, 0, 1, 1, 0), (1, 2, 2, 0, 0), (0, 1, 3, 1, 1, 0),
    (1, 2, 3, 1, 1), (0, 0, 3, 1, 1, 0), (0, 1, 3, 1, 0, 1), (1, 0, 2, 0, 1), (1, 1, 1, 1, 1), (1, 2, 2, 1, 0),
    (1, 1, 1, 1, 2), (1, 1, 2, 1, 1), (1, 1, 1, 0, 1), (2, 2, 2), (1, 0, 1, 1, 1), (1, 2, 2, 0, 2),
    (0, 0, 3, 1, 0, 1), (1, 2, 3, 1, 0), (1, 1, 2, 0, 0), (0, 1, 3, 1, 0, 0), (1, 2, 1, 0, 2), (0, 0, 3, 1, 0, 0),
    (1, 0, 1, 1, 2), (1, 2, 3, 1, 2), (1, 0, 2, 0, 0), (0, 1, 3, 0, 1, 1), (1, 0, 1, 0, 1), (0, 0, 3, 0, 1, 1),
    (1, 2, 3, 0, 2), (1, 0, 1, 0, 2), (1, 1, 3, 1, 0), (0, 1, 3, 0, 1, 0), (1, 2, 3, 0, 1), (0, 0, 3, 0, 1, 0),
    (0, 1, 3, 0, 0, 1), (1, 1, 2, 1, 2), (1, 2, 2, 0, 1), (1, 2, 0, 0, 1), (1, 0, 2, 1, 0), (1, 2, 1, 0, 0),
    (1, 2, 1, 0, 1), (0, 0, 3, 0, 0, 1), (1, 1, 3, 0, 0), (1, 1, 3, 0, 1), (1, 0, 3, 0, 0), (1, 0, 2, 1, 1),
    (4, 0, 0), (1, 1, 3, 0, 2), (4, 1, 0), (5, 1, 0), (6, 1, 0), (5, 0, 0), (6, 0, 0), (4, 2, 1), (5, 2, 1),
    (1, 2, 3, 0, 0), (4, 2, 0), (2, 1, 1), (3, 1, 1), (1, 1, 3, 1, 1), (0, 1, 3, 0, 0, 0), (4, 2, 3),
    (1, 0, 2, 1, 2), (2, 2, 3), (2, 1, 2), (3, 2, 2), (0, 0, 3, 0, 0, 0), (4, 0, 2), (1, 0, 3, 1, 0), (3, 1, 2),
    (2, 0, 1), (5, 2, 0), (4, 2, 2), (1, 0, 3, 1, 1), (3, 2, 3), (1, 0, 3, 1, 2), (3, 0, 1), (1, 0, 3, 0, 1),
    (4, 1, 1), (6, 2, 1), (5, 1, 1), (6, 1, 1), (4, 1, 2), (6, 2, 0), (2, 0, 2), (3, 0, 2), (5, 1, 2), (4, 1, 3),
    (6, 1, 2), (4, 0, 1), (5, 0, 1), (6, 0, 1), (1, 1, 3, 1, 2), (5, 2, 2), (5, 0, 2), (6, 0, 2), (2, 0, 3),
    (3, 0, 3), (1, 0, 3, 0, 2), (2, 1, 3), (3, 1, 3), (4, 0, 3), (5, 0, 3), (6, 2, 2), (5, 2, 3), (7, 2, 0),
    (5, 1, 3), (7, 1, 0), (7, 0, 0),
)
GATHER_ORDER = (
    (0, 2, 0), (1, 2, 1), (0, 0, 0), (3, 0, 3, 0), (1, 0, 2), (4, 2, 3, 0, 0), (1, 0, 0), (0, 1, 0), (2, 1, 3),
    (2, 0, 3), (3, 1, 3, 0), (3, 0, 3, 1), (1, 1, 1), (1, 2, 2), (3, 1, 3, 1), (1, 1, 2), (3, 0, 2, 0),
    (3, 0, 0, 0), (4, 0, 3, 0, 1), (1, 0, 1), (2, 0, 0), (2, 2, 2), (3, 1, 1, 0), (2, 1, 1), (2, 0, 2), (1, 2, 0),
    (3, 1, 2, 0), (3, 2, 3, 0), (2, 1, 2), (4, 0, 1, 0, 0), (3, 2, 1, 0), (4, 1, 3, 0, 1), (1, 1, 0), (3, 0, 1, 0),
    (4, 0, 0, 0, 1), (2, 0, 1), (4, 0, 0, 0, 0), (4, 2, 3, 0, 1), (3, 2, 2, 1), (4, 0, 3, 1, 0), (4, 1, 1, 1, 0),
    (3, 1, 1, 1), (4, 0, 3, 0, 0), (3, 0, 0, 1), (4, 0, 2, 0, 1), (4, 2, 1, 0, 1), (4, 1, 3, 0, 0), (4, 0, 1, 1, 0),
    (4, 2, 0, 0, 0), (4, 2, 2, 0, 0), (2, 2, 1), (4, 0, 2, 0, 0), (3, 2, 2, 0), (4, 2, 1, 0, 0), (2, 2, 3),
    (3, 0, 1, 1), (2, 1, 0), (3, 1, 2, 1), (3, 2, 1, 1), (4, 1, 1, 0, 1), (4, 2, 2, 1, 1), (3, 0, 2, 1),
    (4, 0, 1, 0, 1), (4, 1, 1, 1, 1), (2, 2, 0), (4, 0, 3, 1, 1), (4, 1, 2, 1, 0), (3, 2, 0, 0), (4, 0, 0, 1, 0),
    (3, 1, 0, 0), (4, 0, 2, 1, 0), (4, 1, 3, 1, 1), (4, 1, 2, 1, 1), (4, 1, 3, 1, 0), (4, 2, 1, 1, 1),
    (4, 0, 1, 1, 1), (3, 1, 0, 1), (4, 0, 0, 1, 1), (4, 2, 2, 0, 1), (4, 2, 1, 1, 0), (4, 1, 2, 0, 1),
    (4, 1, 0, 0, 1), (4, 1, 2, 0, 0), (3, 2, 3, 1), (3, 2, 0, 1), (4, 2, 2, 1, 0), (4, 1, 0, 1, 0), (4, 2, 3, 1, 0),
    (4, 1, 0, 0, 0), (4, 0, 2, 1, 1), (4, 1, 1, 0, 0), (4, 2, 0, 1, 0), (4, 2, 3, 1, 1), (4, 1, 0, 1, 1),
    (4, 2, 0, 0, 1), (4, 2, 0, 1, 1),
)
HALF = ((1, 1), (1, 0), (0, 1), (0, 0))


def parts_of(rows, tiles):
    full = rows // TILE
    part = [max(1, full * n // sum(tiles)) * TILE for n in tiles[:-1]]
    return part + [rows - sum(part)]


def padded(n, unit):
    return -(-n // unit) * unit


def over_rows(rows, group, body):
    size = group * TILE
    whole = rows // size

    def step(i, carry):
        body(pl.multiple_of(i * size, size), size)
        return carry

    if whole:
        lax.fori_loop(0, whole, step, 0)
    at = whole * size
    if rows - at >= TILE:
        body(at, (rows - at) // TILE * TILE)
        at += (rows - at) // TILE * TILE
    if rows > at:
        body(at, rows - at)


def half_of(at):
    return at // 2 if isinstance(at, int) else lax.div(at, 2)


def kernel(rows, grad_hbm, w_hbm, m_hbm, v_hbm, d_hbm, lr_ref, full, w, m, v, norm_ref, *scratch):
    count = len(REDUCE)
    stages = scratch[:STAGES]
    scratch = scratch[STAGES:]
    got1, kept, sent2, got2, got3 = (scratch[count * i:count * i + count] for i in range(5))
    (row, mean, d, partial, stage_sem, state_sem, s1, r1, s2, r2, s3, r3, ns, nr,
     gs1, gr1, gs2, gr2, gs3, gr3, gs4, gr4) = scratch[5 * count:]
    part = parts_of(rows, REDUCE_TILES)
    first = [sum(part[:i]) for i in range(count)]
    units = rows // 2
    gather_part = parts_of(rows, GATHER_TILES)
    gather_first = [sum(gather_part[:i]) for i in range(len(gather_part))]

    me = lax.axis_index('dp')
    bits = (lax.div(me, 16), lax.rem(lax.div(me, 8), 2), lax.rem(lax.div(me, 4), 2), lax.rem(lax.div(me, 2), 2),
            lax.rem(me, 2))

    def across(*flips):
        total = 0
        for bit in range(5):
            value = 1 - bits[bit] if bit in flips else bits[bit]
            total = total * 2 + value
        return total

    def pick(axes, values):
        return tuple(a for a, val in zip(axes, values) if val)

    def where(colour, g, j2, j1, jc):
        axes, groups = colour
        return pick(axes + (CORE,), (j1, j2) + groups[g] + (jc,))

    def send(src, dst, send_sem, recv_sem, flips):
        return pltpu.make_async_remote_copy(
            src_ref=src, dst_ref=dst, send_sem=send_sem, recv_sem=recv_sem,
            device_id=(across(*flips),), device_id_type=MESH)

    waited = set()

    def need(copy_of, *key):
        if (copy_of.__name__,) + key not in waited:
            waited.add((copy_of.__name__,) + key)
            copy_of(*key).wait_recv()

    def state_copy(i):
        return pltpu.make_async_copy((w_hbm, m_hbm, v_hbm, d_hbm)[i], (w, m, v, d)[i], state_sem.at[i])

    work = [task[1:] for task in REDUCE_ORDER if task[0] == 0]
    spans = []
    for lead in range(2):
        inside = [i for i in range(count) if SPAN_OF[i] == lead]
        spans.append((inside[0], first[inside[0]], sum(part[i] for i in inside)))

    def stage_copy(i):
        span, g, j2, j1, jc = work[i]
        c, begin, length = spans[span]
        k = across(*where(REDUCE[c], g, j2, j1, jc))
        at = pl.multiple_of((k * rows + begin) * LANES, LANES)
        return pltpu.make_async_copy(grad_hbm.at[:, pl.ds(at, length * LANES)],
                                     stages[i % STAGES].at[:, pl.ds(0, length * LANES)], stage_sem.at[i % STAGES])

    def first_copy(c, g, j2, slot):
        j1 = 1 if slot else 0
        jc = 0 if slot == 1 else 1
        k = across(*where(REDUCE[c], g, j2, j1, jc))
        return send(row.at[k, pl.ds(first[c], padded(part[c], TILE))], got1[c].at[g, j2, slot],
                    s1.at[c, g, j2, slot], r1.at[c, g, j2, slot], pick((REDUCE[c][0][0], CORE), (j1, jc)))

    def second_copy(c, g):
        return send(sent2[c].at[g], got2[c].at[g], s2.at[c, g], r2.at[c, g], (REDUCE[c][0][1],))

    def third_copy(c, g):
        return send(kept[c].at[g], got3[c].at[g], s3.at[c, g], r3.at[c, g], pick(REDUCE[c][0][2:], REDUCE[c][1][g]))

    def pack(i):
        span, g, j2, j1, jc = work[i]
        c, begin, length = spans[span]
        k = across(*where(REDUCE[c], g, j2, j1, jc))
        source = stages[i % STAGES]
        stage_copy(i).wait()

        def body(at, size):
            lane = at * LANES
            if not isinstance(at, int):
                lane = pl.multiple_of(lane, TILE * LANES)
            val = source[:, pl.ds(lane, size * LANES)].astype(F32).reshape(size, LANES)
            row[k, pl.ds(begin + at, size), :] = val.astype(BF16)

        over_rows(length, 4, body)
        if i + STAGES < len(work):
            stage_copy(i + STAGES).start()

    def four_sum(c, g, j2, target):
        for slot in (0, 1, 2):
            need(first_copy, c, g, j2, slot)
        k = across(*where(REDUCE[c], g, j2, 0, 0))

        def body(at, size):
            near = pl.ds(at, size)
            mine = row[k, pl.ds(first[c] + at, size), :].astype(F32) + got1[c][g, j2, 0, near, :].astype(F32)
            other = got1[c][g, j2, 1, near, :].astype(F32) + got1[c][g, j2, 2, near, :].astype(F32)
            target[g, near, :] = mine + other

        over_rows(part[c], 4, body)

    def plane_sum(c, g):
        need(second_copy, c, g)

        def body(at, size):
            near = pl.ds(at, size)
            kept[c][g, near, :] = kept[c][g, near, :] + got2[c][g, near, :]

        if g < 3:
            over_rows(part[c], 4, body)

    def final(c, acc):
        for g in range(3):
            need(third_copy, c, g)

        def mean_of(at, size):
            near = pl.ds(at, size)
            total = (kept[c][3, near, :] + got2[c][3, near, :]) + (got3[c][0, near, :] + got3[c][1, near, :])
            total = (total + got3[c][2, near, :]) * (1.0 / 32.0)
            mean[pl.ds(first[c] + at, size), :] = total
            return total * total

        def fold(val):
            return jnp.sum(val.reshape(val.shape[0] // 8, 8, LANES), axis=0)

        whole = part[c] // 64
        if whole:
            acc = lax.fori_loop(0, whole, lambda i, a: a + fold(mean_of(pl.multiple_of(i * 64, 64), 64)), acc)
        at = whole * 64
        if part[c] - at >= 8:
            size = (part[c] - at) // 8 * 8
            acc = acc + fold(mean_of(at, size))
            at += size
        if part[c] > at:
            tail = mean_of(at, part[c] - at)
            acc = acc + jnp.concatenate([tail, jnp.zeros((8 - tail.shape[0], LANES), F32)], axis=0)
        return acc

    everyone = [pick((HIGH, LOW, Y, X, CORE), [(n >> b) & 1 for b in (4, 3, 2, 1, 0)]) for n in range(1, 32)]

    for i in range(STAGES):
        stage_copy(i).start()
    barrier = pltpu.get_barrier_semaphore()
    for flips in everyone:
        pl.semaphore_signal(barrier, inc=1, device_id=(across(*flips),), device_id_type=MESH)

    acc = jnp.zeros((8, LANES), F32)
    packed = 0
    entered = False
    for task in REDUCE_ORDER:
        kind, c, g = task[:3]
        if kind == 0:
            pack(packed)
            packed += 1
            if packed == len(work):
                for i in range(4):
                    state_copy(i).start()
        elif kind == 1:
            if not entered:
                pl.semaphore_wait(barrier, 31)
                entered = True
            first_copy(c, g, *task[3:]).start()
        elif kind == 2:
            four_sum(c, g, 1, sent2[c])
        elif kind == 3:
            second_copy(c, g).start()
        elif kind == 4:
            four_sum(c, g, 0, kept[c])
        elif kind == 5:
            plane_sum(c, g)
        elif kind == 6:
            third_copy(c, g).start()
        else:
            acc = final(c, acc)

    partial[me] = jnp.sum(acc, axis=0, keepdims=True)

    def norm_copy(j, owner):
        return send(partial.at[owner], partial.at[owner], ns.at[j], nr.at[j], everyone[j])

    for j in range(31):
        norm_copy(j, me).start()
    for i in range(4):
        state_copy(i).wait()
    for j in range(31):
        norm_copy(j, across(*everyone[j])).wait_recv()
    norm = jnp.sqrt(jnp.full((1, LANES), jnp.sum(jnp.sum(partial[...], axis=0)), F32))
    norm_ref[...] = norm
    coef = jnp.minimum(1.0, 1.0 / (norm + CLIP_EPS))
    lr = lr_ref[0]

    def update(c):
        def body(at, size):
            near = pl.ds(gather_first[c] + at, size)
            h = mean[near, :] * coef
            nm = BETA_FIRST * m[near, :] + (1.0 - BETA_FIRST) * h
            nv = BETA_SECOND * v[near, :] + (1.0 - BETA_SECOND) * h * h
            step = (nm * (1.0 / (1.0 - BETA_FIRST ** ADAM_STEP))) / (
                jnp.sqrt(nv * (1.0 / (1.0 - BETA_SECOND ** ADAM_STEP))) + ADAM_EPS)
            old = w[near, :]
            nw = old - lr * (step + WEIGHT_DECAY * d[near, :].astype(F32) * old)
            m[near, :] = nm
            v[near, :] = nv
            w[near, :] = nw
            full[pl.ds(me * units + gather_first[c] // 2 + half_of(at), size // 2)] = nw.astype(BF16).reshape(
                size // 2, 2, LANES)

        over_rows(gather_part[c], 2, body)

    def piece(c, g, j2, j1):
        k = across(*where(GATHER[c], g, j2, j1, 0))
        return full.at[pl.ds(k * units + gather_first[c] // 2, gather_part[c] // 2)]

    def gather1(c, g):
        spot = piece(c, 3, 0, 0)
        return send(spot, spot, gs1.at[c, g], gr1.at[c, g], pick(GATHER[c][0][2:], GATHER[c][1][g]))

    def gather1_in(c, g):
        spot = piece(c, g, 0, 0)
        return send(spot, spot, gs1.at[c, g], gr1.at[c, g], pick(GATHER[c][0][2:], GATHER[c][1][g]))

    def gather2(c, g):
        spot = piece(c, g, 0, 0)
        return send(spot, spot, gs2.at[c, g], gr2.at[c, g], (GATHER[c][0][1],))

    def gather3(c, g, j2):
        spot = piece(c, g, j2, 0)
        return send(spot, spot, gs3.at[c, g, j2], gr3.at[c, g, j2], (GATHER[c][0][0],))

    def gather4(c, g, j2, j1):
        spot = piece(c, g, j2, j1)
        return send(spot, spot, gs4.at[c, g, j2, j1], gr4.at[c, g, j2, j1], (CORE,))

    for kind, c, *key in GATHER_ORDER:
        if kind == 0:
            update(c)
        elif kind == 1:
            gather1(c, *key).start()
        else:
            if kind == 4 and key[2]:
                need(gather3, c, *key[:2])
            elif kind > 2 and key[1]:
                need(gather2, c, key[0])
            elif key[0] < 3:
                need(gather1_in, c, key[0])
            (gather2, gather3, gather4)[kind - 2](c, *key).start()

    for c in range(count):
        for g in range(4):
            for j2 in (0, 1):
                for slot in range(3):
                    first_copy(c, g, j2, slot).wait_send()
            second_copy(c, g).wait_send()
        for g in range(3):
            third_copy(c, g).wait_send()
    for j in range(31):
        norm_copy(j, me).wait_send()
    for c in range(len(GATHER)):
        for g in range(3):
            gather1(c, g).wait_send()
        for g in range(4):
            gather2(c, g).wait_send()
            for j2 in (0, 1):
                gather3(c, g, j2).wait_send()
                for j1 in (0, 1):
                    gather4(c, g, j2, j1).wait()


def write_out(*refs):
    sem = refs[-1]
    count = len(refs) // 2
    length = refs[0].shape[0] // CHUNKS
    copies = []
    for i in range(CHUNKS):
        near = pl.ds(i * length, length)
        copies.append(pltpu.make_async_copy(refs[0].at[near], refs[count].at[near], sem.at[i]))
    for i in range(1, count):
        copies.append(pltpu.make_async_copy(refs[i], refs[count + i], sem.at[CHUNKS + i - 1]))
    for copy in copies:
        copy.start()
    for copy in copies:
        copy.wait()


def solution(mesh):
    num_dev = mesh.shape['dp']

    def local_step(grad_row, master, mom_first, mom_second, decay_mask, learn_rate):
        shard_len = master.shape[0]
        rows = shard_len // LANES
        part = parts_of(rows, REDUCE_TILES)
        dma = pltpu.SemaphoreType.DMA
        hbm = pl.BlockSpec(memory_space=pltpu.HBM)
        vmem = pl.BlockSpec(memory_space=pltpu.VMEM)
        flat = (rows, LANES)
        whole = (num_dev * rows // 2, 2, LANES)
        n = len(REDUCE)
        longest = max(sum(part[i] for i in range(n) if SPAN_OF[i] == lead) for lead in range(2))
        k = len(GATHER)
        results = pl.pallas_call(
            functools.partial(kernel, rows),
            out_shape=(pltpu.VMEM(whole, BF16), pltpu.VMEM(flat, F32), pltpu.VMEM(flat, F32), pltpu.VMEM(flat, F32),
                       pltpu.VMEM((1, LANES), F32)),
            in_specs=[hbm] * 5 + [pl.BlockSpec(memory_space=pltpu.SMEM)],
            out_specs=(vmem,) * 5,
            scratch_shapes=[pltpu.VMEM((1, longest * LANES), BF16)] * STAGES
            + [pltpu.VMEM((4, 2, 3, padded(p, TILE), LANES), BF16) for p in part]
            + [pltpu.VMEM((groups, padded(p, 8), LANES), F32) for groups in (4, 4, 4, 3) for p in part]
            + [
                pltpu.VMEM((num_dev, padded(rows, TILE), LANES), BF16), pltpu.VMEM(flat, F32),
                pltpu.VMEM(flat, jnp.int32), pltpu.VMEM((num_dev, 1, LANES), F32),
                dma((STAGES,)), dma((4,)),
                dma((n, 4, 2, 3)), dma((n, 4, 2, 3)), dma((n, 4)), dma((n, 4)), dma((n, 3)), dma((n, 3)),
                dma((num_dev - 1,)), dma((num_dev - 1,)),
                dma((k, 3)), dma((k, 3)), dma((k, 4)), dma((k, 4)), dma((k, 4, 2)), dma((k, 4, 2)),
                dma((k, 4, 2, 2)), dma((k, 4, 2, 2)),
            ],
            compiler_params=pltpu.CompilerParams(
                collective_id=0, has_side_effects=True, vmem_limit_bytes=VMEM_LIMIT),
        )(grad_row, master.reshape(flat), mom_first.reshape(flat), mom_second.reshape(flat), decay_mask.reshape(flat), learn_rate)
        state = jax.ShapeDtypeStruct(flat, F32)
        params, new_master, new_first, new_second, norm = pl.pallas_call(
            write_out,
            out_shape=(jax.ShapeDtypeStruct(whole, BF16), state, state, state, jax.ShapeDtypeStruct((1, LANES), F32)),
            in_specs=[vmem] * 5,
            out_specs=(hbm,) * 5,
            scratch_shapes=[dma((CHUNKS + 4,))],
            compiler_params=pltpu.CompilerParams(vmem_limit_bytes=1024 * 1024),
        )(*results)
        return (params.reshape(num_dev * shard_len), new_master.reshape(shard_len), new_first.reshape(shard_len),
                new_second.reshape(shard_len), norm[0, :1])

    return jax.shard_map(local_step, mesh=mesh, in_specs=(P('dp', None), P('dp'), P('dp'), P('dp'), P('dp'), P()),
                         out_specs=(P(), P('dp'), P('dp'), P('dp'), P()), check_vma=False)
```

```python
import functools

import jax
import jax.numpy as jnp
from jax import lax
from jax.experimental import pallas as pl
from jax.experimental.pallas import tpu as pltpu
from jax.sharding import PartitionSpec as P

BETA_FIRST = 0.9
BETA_SECOND = 0.95
ADAM_EPS = 1e-8
CLIP_EPS = 1e-6
WEIGHT_DECAY = 0.1
ADAM_STEP = 10
LANES = 128
TILE = 16
STAGES = 4
CHUNKS = 8
VMEM_LIMIT = 46 * 1024 * 1024
MESH = pl.DeviceIdType.MESH
F32 = jnp.float32
BF16 = jnp.bfloat16

HIGH, LOW, Y, X, CORE = range(5)
REDUCE = (
    ((X, Y, LOW, HIGH), ((1, 1), (1, 0), (0, 1), (0, 0))),
    ((Y, X, LOW, HIGH), ((1, 1), (1, 0), (0, 1), (0, 0))),
    ((LOW, HIGH, X, Y), ((1, 1), (0, 1), (1, 0), (0, 0))),
)
REDUCE_TILES = (46, 46, 22)
SPAN_OF = (0, 0, 1)
GATHER = (
    ((X, Y, LOW, HIGH), ((1, 1), (0, 1), (1, 0), (0, 0))),
    ((Y, X, LOW, HIGH), ((1, 1), (0, 1), (1, 0), (0, 0))),
    ((LOW, HIGH, X, Y), ((0, 1), (1, 1), (1, 0), (0, 0))),
)
GATHER_TILES = (49, 49, 16)
REDUCE_ORDER = (
    (0, 1, 0, 1, 1, 1), (1, 2, 0, 1, 2), (0, 0, 0, 1, 1, 1), (0, 1, 0, 1, 1, 0), (0, 0, 0, 1, 1, 0),
    (1, 1, 0, 1, 1), (1, 0, 0, 1, 1), (1, 2, 0, 1, 1), (0, 1, 0, 1, 0, 1), (0, 0, 0, 1, 0, 1), (0, 1, 0, 1, 0, 0),
    (0, 0, 0, 1, 0, 0), (0, 1, 0, 0, 1, 1), (0, 0, 0, 0, 1, 1), (0, 1, 0, 0, 1, 0), (0, 0, 0, 0, 1, 0),
    (0, 1, 0, 0, 0, 1), (1, 2, 0, 0, 2), (0, 0, 0, 0, 0, 1), (0, 1, 0, 0, 0, 0), (0, 0, 0, 0, 0, 0),
    (0, 1, 1, 1, 1, 1), (1, 2, 1, 1, 2), (0, 0, 1, 1, 1, 1), (1, 1, 0, 1, 2), (0, 1, 1, 1, 1, 0), (1, 2, 1, 1, 1),
    (0, 0, 1, 1, 1, 0), (0, 1, 1, 1, 0, 1), (0, 0, 1, 1, 0, 1), (1, 0, 0, 1, 2), (1, 2, 0, 1, 0), (1, 1, 0, 1, 0),
    (0, 1, 1, 1, 0, 0), (0, 0, 1, 1, 0, 0), (1, 0, 0, 0, 0), (1, 1, 1, 1, 2), (0, 1, 1, 0, 1, 1),
    (0, 0, 1, 0, 1, 1), (2, 2, 0), (3, 2, 0), (0, 1, 1, 0, 1, 0), (1, 2, 1, 0, 1), (0, 0, 1, 0, 1, 0),
    (0, 1, 1, 0, 0, 1), (0, 0, 1, 0, 0, 1), (0, 1, 1, 0, 0, 0), (0, 0, 1, 0, 0, 0), (0, 1, 2, 1, 1, 1),
    (0, 0, 2, 1, 1, 1), (0, 1, 2, 1, 1, 0), (1, 2, 2, 1, 1), (1, 0, 0, 0, 1), (0, 0, 2, 1, 1, 0), (1, 2, 2, 1, 2),
    (0, 1, 2, 1, 0, 1), (1, 1, 0, 0, 1), (1, 1, 0, 0, 2), (0, 0, 2, 1, 0, 1), (0, 1, 2, 1, 0, 0), (2, 1, 0),
    (0, 0, 2, 1, 0, 0), (1, 1, 2, 0, 1), (1, 2, 2, 1, 0), (0, 1, 2, 0, 1, 1), (1, 1, 0, 0, 0), (0, 0, 2, 0, 1, 1),
    (0, 1, 2, 0, 1, 0), (0, 0, 2, 0, 1, 0), (0, 1, 2, 0, 0, 1), (1, 2, 1, 1, 0), (3, 1, 0), (2, 2, 1),
    (0, 0, 2, 0, 0, 1), (1, 0, 0, 1, 0), (2, 0, 0), (0, 1, 2, 0, 0, 0), (0, 0, 2, 0, 0, 0), (3, 0, 0),
    (1, 0, 0, 0, 2), (1, 0, 1, 1, 2), (1, 2, 0, 0, 0), (3, 2, 1), (1, 0, 2, 1, 0), (1, 2, 1, 0, 0), (1, 2, 2, 0, 1),
    (1, 2, 0, 0, 1), (0, 1, 3, 1, 1, 1), (0, 0, 3, 1, 1, 1), (1, 2, 3, 1, 2), (1, 1, 2, 0, 0), (1, 2, 2, 0, 2),
    (1, 1, 1, 1, 0), (0, 1, 3, 1, 1, 0), (0, 0, 3, 1, 1, 0), (0, 1, 3, 1, 0, 1), (0, 0, 3, 1, 0, 1),
    (0, 1, 3, 1, 0, 0), (2, 2, 2), (1, 0, 2, 0, 2), (0, 0, 3, 1, 0, 0), (1, 1, 1, 0, 1), (0, 1, 3, 0, 1, 1),
    (0, 0, 3, 0, 1, 1), (1, 0, 1, 1, 0), (1, 1, 1, 1, 1), (1, 2, 1, 0, 2), (1, 2, 3, 1, 0), (1, 1, 2, 0, 2),
    (0, 1, 3, 0, 1, 0), (4, 1, 0), (0, 0, 3, 0, 1, 0), (1, 1, 1, 0, 2), (1, 1, 2, 1, 2), (1, 1, 2, 1, 1),
    (1, 0, 2, 0, 1), (5, 1, 0), (1, 2, 3, 1, 1), (1, 0, 2, 0, 0), (1, 2, 3, 0, 2), (1, 2, 2, 0, 0), (1, 1, 2, 1, 0),
    (1, 1, 3, 0, 2), (1, 2, 3, 0, 1), (1, 0, 1, 1, 1), (4, 0, 0), (6, 1, 0), (1, 1, 1, 0, 0), (1, 0, 1, 0, 1),
    (5, 0, 0), (6, 0, 0), (0, 1, 3, 0, 0, 1), (0, 0, 3, 0, 0, 1), (1, 1, 3, 0, 0), (1, 0, 1, 0, 2), (4, 2, 1),
    (1, 1, 3, 1, 0), (4, 2, 0), (5, 2, 0), (4, 1, 2), (2, 1, 1), (3, 1, 1), (0, 1, 3, 0, 0, 0), (0, 0, 3, 0, 0, 0),
    (2, 1, 2), (3, 1, 2), (1, 0, 2, 1, 1), (3, 2, 2), (1, 0, 3, 0, 0), (6, 2, 0), (1, 0, 1, 0, 0), (1, 0, 3, 1, 0),
    (2, 0, 1), (1, 0, 2, 1, 2), (1, 1, 3, 0, 1), (2, 2, 3), (3, 2, 3), (3, 0, 1), (4, 1, 1), (5, 1, 1), (6, 1, 1),
    (5, 1, 2), (6, 1, 2), (1, 0, 3, 0, 1), (1, 0, 3, 0, 2), (4, 0, 1), (2, 0, 2), (3, 0, 2), (5, 0, 1), (4, 0, 2),
    (5, 2, 1), (6, 0, 1), (1, 0, 3, 1, 1), (1, 1, 3, 1, 1), (1, 2, 3, 0, 0), (1, 0, 3, 1, 2), (4, 2, 2), (5, 2, 2),
    (5, 0, 2), (4, 0, 3), (6, 0, 2), (1, 1, 3, 1, 2), (6, 2, 2), (2, 0, 3), (3, 0, 3), (4, 2, 3), (5, 2, 3),
    (4, 1, 3), (2, 1, 3), (3, 1, 3), (6, 2, 1), (5, 1, 3), (7, 1, 0), (5, 0, 3), (7, 0, 0), (7, 2, 0),
)
GATHER_ORDER = (
    (0, 2, 0), (1, 2, 1), (3, 2, 3, 0), (0, 0, 0), (1, 0, 2), (4, 2, 3, 0, 0), (1, 2, 0), (1, 0, 0), (2, 0, 3),
    (0, 1, 0), (2, 1, 3), (3, 1, 3, 0), (3, 0, 2, 0), (2, 0, 2), (4, 0, 3, 1, 0), (3, 0, 3, 1), (1, 1, 2),
    (1, 1, 0), (1, 2, 2), (3, 1, 3, 1), (4, 0, 2, 0, 0), (2, 2, 0), (3, 0, 0, 0), (2, 0, 0), (2, 1, 2),
    (3, 1, 2, 0), (3, 2, 0, 1), (1, 1, 1), (2, 1, 0), (4, 0, 0, 0, 0), (4, 1, 3, 1, 0), (2, 2, 2), (3, 0, 2, 1),
    (4, 1, 2, 1, 0), (3, 1, 0, 0), (3, 1, 2, 1), (4, 0, 0, 0, 1), (4, 1, 2, 0, 0), (3, 2, 0, 0), (1, 0, 1),
    (3, 0, 0, 1), (3, 1, 1, 0), (4, 0, 3, 0, 0), (3, 2, 2, 1), (2, 1, 1), (3, 2, 1, 0), (4, 0, 2, 0, 1),
    (3, 1, 0, 1), (4, 1, 1, 0, 0), (3, 0, 3, 0), (4, 0, 0, 1, 0), (4, 1, 1, 1, 0), (4, 2, 0, 1, 1), (2, 2, 3),
    (4, 2, 1, 0, 0), (2, 0, 1), (4, 1, 3, 0, 1), (4, 0, 0, 1, 1), (4, 2, 0, 1, 0), (4, 2, 3, 0, 1), (4, 0, 1, 0, 0),
    (2, 2, 1), (4, 2, 2, 1, 1), (4, 2, 2, 1, 0), (4, 1, 0, 0, 1), (4, 2, 2, 0, 0), (4, 0, 3, 1, 1), (4, 1, 3, 0, 0),
    (4, 1, 0, 1, 0), (4, 1, 2, 0, 1), (4, 1, 1, 0, 1), (3, 1, 1, 1), (4, 1, 2, 1, 1), (4, 2, 0, 0, 1),
    (4, 1, 0, 0, 0), (3, 0, 1, 0), (4, 1, 3, 1, 1), (4, 0, 2, 1, 0), (3, 2, 2, 0), (3, 0, 1, 1), (3, 2, 3, 1),
    (4, 1, 0, 1, 1), (4, 0, 1, 0, 1), (4, 0, 2, 1, 1), (4, 0, 3, 0, 1), (3, 2, 1, 1), (4, 0, 1, 1, 0),
    (4, 2, 3, 1, 1), (4, 1, 1, 1, 1), (4, 2, 1, 0, 1), (4, 2, 3, 1, 0), (4, 2, 1, 1, 0), (4, 2, 1, 1, 1),
    (4, 2, 0, 0, 0), (4, 0, 1, 1, 1), (4, 2, 2, 0, 1),
)
HALF = ((1, 1), (1, 0), (0, 1), (0, 0))


def parts_of(rows, tiles):
    full = rows // TILE
    part = [max(1, full * n // sum(tiles)) * TILE for n in tiles[:-1]]
    return part + [rows - sum(part)]


def padded(n, unit):
    return -(-n // unit) * unit


def over_rows(rows, group, body):
    size = group * TILE
    whole = rows // size

    def step(i, carry):
        body(pl.multiple_of(i * size, size), size)
        return carry

    if whole:
        lax.fori_loop(0, whole, step, 0)
    at = whole * size
    if rows - at >= TILE:
        body(at, (rows - at) // TILE * TILE)
        at += (rows - at) // TILE * TILE
    if rows > at:
        body(at, rows - at)


def half_of(at):
    return at // 2 if isinstance(at, int) else lax.div(at, 2)


def kernel(rows, grad_hbm, w_hbm, m_hbm, v_hbm, d_hbm, lr_ref, full, w, m, v, norm_ref, *scratch):
    count = len(REDUCE)
    stages = scratch[:STAGES]
    scratch = scratch[STAGES:]
    got1, kept, sent2, got2, got3 = (scratch[count * i:count * i + count] for i in range(5))
    (row, mean, d, partial, stage_sem, state_sem, s1, r1, s2, r2, s3, r3, ns, nr,
     gs1, gr1, gs2, gr2, gs3, gr3, gs4, gr4) = scratch[5 * count:]
    part = parts_of(rows, REDUCE_TILES)
    first = [sum(part[:i]) for i in range(count)]
    units = rows // 2
    gather_part = parts_of(rows, GATHER_TILES)
    gather_first = [sum(gather_part[:i]) for i in range(len(gather_part))]

    me = lax.axis_index('dp')
    bits = (lax.div(me, 16), lax.rem(lax.div(me, 8), 2), lax.rem(lax.div(me, 4), 2), lax.rem(lax.div(me, 2), 2),
            lax.rem(me, 2))

    def across(*flips):
        total = 0
        for bit in range(5):
            value = 1 - bits[bit] if bit in flips else bits[bit]
            total = total * 2 + value
        return total

    def pick(axes, values):
        return tuple(a for a, val in zip(axes, values) if val)

    def where(colour, g, j2, j1, jc):
        axes, groups = colour
        return pick(axes + (CORE,), (j1, j2) + groups[g] + (jc,))

    def send(src, dst, send_sem, recv_sem, flips):
        return pltpu.make_async_remote_copy(
            src_ref=src, dst_ref=dst, send_sem=send_sem, recv_sem=recv_sem,
            device_id=(across(*flips),), device_id_type=MESH)

    waited = set()

    def need(copy_of, *key):
        if (copy_of.__name__,) + key not in waited:
            waited.add((copy_of.__name__,) + key)
            copy_of(*key).wait_recv()

    def state_copy(i):
        return pltpu.make_async_copy((w_hbm, m_hbm, v_hbm, d_hbm)[i], (w, m, v, d)[i], state_sem.at[i])

    work = [task[1:] for task in REDUCE_ORDER if task[0] == 0]
    spans = []
    for lead in range(2):
        inside = [i for i in range(count) if SPAN_OF[i] == lead]
        spans.append((inside[0], first[inside[0]], sum(part[i] for i in inside)))

    def stage_copy(i):
        span, g, j2, j1, jc = work[i]
        c, begin, length = spans[span]
        k = across(*where(REDUCE[c], g, j2, j1, jc))
        at = pl.multiple_of((k * rows + begin) * LANES, LANES)
        return pltpu.make_async_copy(grad_hbm.at[:, pl.ds(at, length * LANES)],
                                     stages[i % STAGES].at[:, pl.ds(0, length * LANES)], stage_sem.at[i % STAGES])

    def first_copy(c, g, j2, slot):
        j1 = 1 if slot else 0
        jc = 0 if slot == 1 else 1
        k = across(*where(REDUCE[c], g, j2, j1, jc))
        return send(row.at[k, pl.ds(first[c], padded(part[c], TILE))], got1[c].at[g, j2, slot],
                    s1.at[c, g, j2, slot], r1.at[c, g, j2, slot], pick((REDUCE[c][0][0], CORE), (j1, jc)))

    def second_copy(c, g):
        return send(sent2[c].at[g], got2[c].at[g], s2.at[c, g], r2.at[c, g], (REDUCE[c][0][1],))

    def third_copy(c, g):
        return send(kept[c].at[g], got3[c].at[g], s3.at[c, g], r3.at[c, g], pick(REDUCE[c][0][2:], REDUCE[c][1][g]))

    def pack(i):
        span, g, j2, j1, jc = work[i]
        c, begin, length = spans[span]
        k = across(*where(REDUCE[c], g, j2, j1, jc))
        source = stages[i % STAGES]
        stage_copy(i).wait()

        def body(at, size):
            lane = at * LANES
            if not isinstance(at, int):
                lane = pl.multiple_of(lane, TILE * LANES)
            val = source[:, pl.ds(lane, size * LANES)].astype(F32).reshape(size, LANES)
            row[k, pl.ds(begin + at, size), :] = val.astype(BF16)

        over_rows(length, 4, body)
        if i + STAGES < len(work):
            stage_copy(i + STAGES).start()

    def four_sum(c, g, j2, target):
        for slot in (0, 1, 2):
            need(first_copy, c, g, j2, slot)
        k = across(*where(REDUCE[c], g, j2, 0, 0))

        def body(at, size):
            near = pl.ds(at, size)
            mine = row[k, pl.ds(first[c] + at, size), :].astype(F32) + got1[c][g, j2, 0, near, :].astype(F32)
            other = got1[c][g, j2, 1, near, :].astype(F32) + got1[c][g, j2, 2, near, :].astype(F32)
            target[g, near, :] = mine + other

        over_rows(part[c], 4, body)

    def plane_sum(c, g):
        need(second_copy, c, g)

        def body(at, size):
            near = pl.ds(at, size)
            kept[c][g, near, :] = kept[c][g, near, :] + got2[c][g, near, :]

        if g < 3:
            over_rows(part[c], 4, body)

    def final(c, acc):
        for g in range(3):
            need(third_copy, c, g)

        def mean_of(at, size):
            near = pl.ds(at, size)
            total = (kept[c][3, near, :] + got2[c][3, near, :]) + (got3[c][0, near, :] + got3[c][1, near, :])
            total = (total + got3[c][2, near, :]) * (1.0 / 32.0)
            mean[pl.ds(first[c] + at, size), :] = total
            return total * total

        def fold(val):
            return jnp.sum(val.reshape(val.shape[0] // 8, 8, LANES), axis=0)

        whole = part[c] // 64
        if whole:
            acc = lax.fori_loop(0, whole, lambda i, a: a + fold(mean_of(pl.multiple_of(i * 64, 64), 64)), acc)
        at = whole * 64
        if part[c] - at >= 8:
            size = (part[c] - at) // 8 * 8
            acc = acc + fold(mean_of(at, size))
            at += size
        if part[c] > at:
            tail = mean_of(at, part[c] - at)
            acc = acc + jnp.concatenate([tail, jnp.zeros((8 - tail.shape[0], LANES), F32)], axis=0)
        return acc

    everyone = [pick((HIGH, LOW, Y, X, CORE), [(n >> b) & 1 for b in (4, 3, 2, 1, 0)]) for n in range(1, 32)]

    for i in range(STAGES):
        stage_copy(i).start()
    barrier = pltpu.get_barrier_semaphore()
    for flips in everyone:
        pl.semaphore_signal(barrier, inc=1, device_id=(across(*flips),), device_id_type=MESH)

    acc = jnp.zeros((8, LANES), F32)
    packed = 0
    entered = False
    for task in REDUCE_ORDER:
        kind, c, g = task[:3]
        if kind == 0:
            pack(packed)
            packed += 1
            if packed == len(work):
                for i in range(4):
                    state_copy(i).start()
        elif kind == 1:
            if not entered:
                pl.semaphore_wait(barrier, 31)
                entered = True
            first_copy(c, g, *task[3:]).start()
        elif kind == 2:
            four_sum(c, g, 1, sent2[c])
        elif kind == 3:
            second_copy(c, g).start()
        elif kind == 4:
            four_sum(c, g, 0, kept[c])
        elif kind == 5:
            plane_sum(c, g)
        elif kind == 6:
            third_copy(c, g).start()
        else:
            acc = final(c, acc)

    partial[me] = jnp.sum(acc, axis=0, keepdims=True)

    def norm_copy(j, owner):
        return send(partial.at[owner], partial.at[owner], ns.at[j], nr.at[j], everyone[j])

    for j in range(31):
        norm_copy(j, me).start()
    for i in range(4):
        state_copy(i).wait()
    for j in range(31):
        norm_copy(j, across(*everyone[j])).wait_recv()
    norm = jnp.sqrt(jnp.full((1, LANES), jnp.sum(jnp.sum(partial[...], axis=0)), F32))
    norm_ref[...] = norm
    coef = jnp.minimum(1.0, 1.0 / (norm + CLIP_EPS))
    lr = lr_ref[0]

    def update(c):
        def body(at, size):
            near = pl.ds(gather_first[c] + at, size)
            h = mean[near, :] * coef
            nm = BETA_FIRST * m[near, :] + (1.0 - BETA_FIRST) * h
            nv = BETA_SECOND * v[near, :] + (1.0 - BETA_SECOND) * h * h
            step = (nm * (1.0 / (1.0 - BETA_FIRST ** ADAM_STEP))) / (
                jnp.sqrt(nv * (1.0 / (1.0 - BETA_SECOND ** ADAM_STEP))) + ADAM_EPS)
            old = w[near, :]
            nw = old - lr * (step + WEIGHT_DECAY * d[near, :].astype(F32) * old)
            m[near, :] = nm
            v[near, :] = nv
            w[near, :] = nw
            full[pl.ds(me * units + gather_first[c] // 2 + half_of(at), size // 2)] = nw.astype(BF16).reshape(
                size // 2, 2, LANES)

        over_rows(gather_part[c], 2, body)

    def piece(c, g, j2, j1):
        k = across(*where(GATHER[c], g, j2, j1, 0))
        return full.at[pl.ds(k * units + gather_first[c] // 2, gather_part[c] // 2)]

    def gather1(c, g):
        spot = piece(c, 3, 0, 0)
        return send(spot, spot, gs1.at[c, g], gr1.at[c, g], pick(GATHER[c][0][2:], GATHER[c][1][g]))

    def gather1_in(c, g):
        spot = piece(c, g, 0, 0)
        return send(spot, spot, gs1.at[c, g], gr1.at[c, g], pick(GATHER[c][0][2:], GATHER[c][1][g]))

    def gather2(c, g):
        spot = piece(c, g, 0, 0)
        return send(spot, spot, gs2.at[c, g], gr2.at[c, g], (GATHER[c][0][1],))

    def gather3(c, g, j2):
        spot = piece(c, g, j2, 0)
        return send(spot, spot, gs3.at[c, g, j2], gr3.at[c, g, j2], (GATHER[c][0][0],))

    def gather4(c, g, j2, j1):
        spot = piece(c, g, j2, j1)
        return send(spot, spot, gs4.at[c, g, j2, j1], gr4.at[c, g, j2, j1], (CORE,))

    for kind, c, *key in GATHER_ORDER:
        if kind == 0:
            update(c)
        elif kind == 1:
            gather1(c, *key).start()
        else:
            if kind == 4 and key[2]:
                need(gather3, c, *key[:2])
            elif kind > 2 and key[1]:
                need(gather2, c, key[0])
            elif key[0] < 3:
                need(gather1_in, c, key[0])
            (gather2, gather3, gather4)[kind - 2](c, *key).start()

    for c in range(count):
        for g in range(4):
            for j2 in (0, 1):
                for slot in range(3):
                    first_copy(c, g, j2, slot).wait_send()
            second_copy(c, g).wait_send()
        for g in range(3):
            third_copy(c, g).wait_send()
    for j in range(31):
        norm_copy(j, me).wait_send()
    for c in range(len(GATHER)):
        for g in range(3):
            gather1(c, g).wait_send()
        for g in range(4):
            gather2(c, g).wait_send()
            for j2 in (0, 1):
                gather3(c, g, j2).wait_send()
                for j1 in (0, 1):
                    gather4(c, g, j2, j1).wait()


def write_out(*refs):
    sem = refs[-1]
    count = len(refs) // 2
    length = refs[0].shape[0] // CHUNKS
    copies = []
    for i in range(CHUNKS):
        near = pl.ds(i * length, length)
        copies.append(pltpu.make_async_copy(refs[0].at[near], refs[count].at[near], sem.at[i]))
    for i in range(1, count):
        copies.append(pltpu.make_async_copy(refs[i], refs[count + i], sem.at[CHUNKS + i - 1]))
    for copy in copies:
        copy.start()
    for copy in copies:
        copy.wait()


def solution(mesh):
    num_dev = mesh.shape['dp']

    def local_step(grad_row, master, mom_first, mom_second, decay_mask, learn_rate):
        shard_len = master.shape[0]
        rows = shard_len // LANES
        part = parts_of(rows, REDUCE_TILES)
        dma = pltpu.SemaphoreType.DMA
        hbm = pl.BlockSpec(memory_space=pltpu.HBM)
        vmem = pl.BlockSpec(memory_space=pltpu.VMEM)
        flat = (rows, LANES)
        whole = (num_dev * rows // 2, 2, LANES)
        n = len(REDUCE)
        longest = max(sum(part[i] for i in range(n) if SPAN_OF[i] == lead) for lead in range(2))
        k = len(GATHER)
        results = pl.pallas_call(
            functools.partial(kernel, rows),
            out_shape=(pltpu.VMEM(whole, BF16), pltpu.VMEM(flat, F32), pltpu.VMEM(flat, F32), pltpu.VMEM(flat, F32),
                       pltpu.VMEM((1, LANES), F32)),
            in_specs=[hbm] * 5 + [pl.BlockSpec(memory_space=pltpu.SMEM)],
            out_specs=(vmem,) * 5,
            scratch_shapes=[pltpu.VMEM((1, longest * LANES), BF16)] * STAGES
            + [pltpu.VMEM((4, 2, 3, padded(p, TILE), LANES), BF16) for p in part]
            + [pltpu.VMEM((groups, padded(p, 8), LANES), F32) for groups in (4, 4, 4, 3) for p in part]
            + [
                pltpu.VMEM((num_dev, padded(rows, TILE), LANES), BF16), pltpu.VMEM(flat, F32),
                pltpu.VMEM(flat, jnp.int32), pltpu.VMEM((num_dev, 1, LANES), F32),
                dma((STAGES,)), dma((4,)),
                dma((n, 4, 2, 3)), dma((n, 4, 2, 3)), dma((n, 4)), dma((n, 4)), dma((n, 3)), dma((n, 3)),
                dma((num_dev - 1,)), dma((num_dev - 1,)),
                dma((k, 3)), dma((k, 3)), dma((k, 4)), dma((k, 4)), dma((k, 4, 2)), dma((k, 4, 2)),
                dma((k, 4, 2, 2)), dma((k, 4, 2, 2)),
            ],
            compiler_params=pltpu.CompilerParams(
                collective_id=0, has_side_effects=True, vmem_limit_bytes=VMEM_LIMIT),
        )(grad_row, master.reshape(flat), mom_first.reshape(flat), mom_second.reshape(flat), decay_mask.reshape(flat), learn_rate)
        state = jax.ShapeDtypeStruct(flat, F32)
        params, new_master, new_first, new_second, norm = pl.pallas_call(
            write_out,
            out_shape=(jax.ShapeDtypeStruct(whole, BF16), state, state, state, jax.ShapeDtypeStruct((1, LANES), F32)),
            in_specs=[vmem] * 5,
            out_specs=(hbm,) * 5,
            scratch_shapes=[dma((CHUNKS + 4,))],
            compiler_params=pltpu.CompilerParams(vmem_limit_bytes=1024 * 1024),
        )(*results)
        return (params.reshape(num_dev * shard_len), new_master.reshape(shard_len), new_first.reshape(shard_len),
                new_second.reshape(shard_len), norm[0, :1])

    return jax.shard_map(local_step, mesh=mesh, in_specs=(P('dp', None), P('dp'), P('dp'), P('dp'), P('dp'), P()),
                         out_specs=(P(), P('dp'), P('dp'), P('dp'), P()), check_vma=False)
```

```python
import functools

import jax
import jax.numpy as jnp
from jax import lax
from jax.experimental import pallas as pl
from jax.experimental.pallas import tpu as pltpu
from jax.sharding import PartitionSpec as P

BETA_FIRST = 0.9
BETA_SECOND = 0.95
ADAM_EPS = 1e-8
CLIP_EPS = 1e-6
WEIGHT_DECAY = 0.1
ADAM_STEP = 10
LANES = 128
TILE = 16
STAGES = 4
CHUNKS = 8
VMEM_LIMIT = 46 * 1024 * 1024
MESH = pl.DeviceIdType.MESH
F32 = jnp.float32
BF16 = jnp.bfloat16

HIGH, LOW, Y, X, CORE = range(5)
REDUCE = (
    ((X, Y, LOW, HIGH), ((1, 1), (1, 0), (0, 1), (0, 0))),
    ((Y, X, LOW, HIGH), ((1, 1), (1, 0), (0, 1), (0, 0))),
    ((LOW, HIGH, X, Y), ((1, 1), (0, 1), (1, 0), (0, 0))),
)
REDUCE_TILES = (47, 47, 20)
SPAN_OF = (0, 0, 1)
GATHER = (
    ((X, Y, LOW, HIGH), ((1, 1), (0, 1), (1, 0), (0, 0))),
    ((Y, X, LOW, HIGH), ((1, 1), (0, 1), (1, 0), (0, 0))),
    ((LOW, HIGH, X, Y), ((0, 1), (1, 1), (1, 0), (0, 0))),
)
GATHER_TILES = (49, 49, 16)
REDUCE_ORDER = (
    (0, 1, 0, 1, 1, 1), (0, 0, 0, 1, 1, 1), (1, 0, 0, 1, 2), (0, 1, 0, 1, 1, 0), (1, 2, 0, 1, 1), (1, 1, 0, 1, 2),
    (0, 0, 0, 1, 1, 0), (1, 1, 0, 1, 1), (1, 0, 0, 1, 1), (0, 1, 0, 1, 0, 1), (1, 2, 0, 1, 0), (0, 0, 0, 1, 0, 1),
    (1, 0, 0, 1, 0), (0, 1, 0, 1, 0, 0), (0, 0, 0, 1, 0, 0), (0, 1, 0, 0, 1, 1), (0, 0, 0, 0, 1, 1),
    (0, 1, 0, 0, 1, 0), (0, 0, 0, 0, 1, 0), (0, 1, 0, 0, 0, 1), (0, 0, 0, 0, 0, 1), (0, 1, 0, 0, 0, 0),
    (1, 0, 0, 0, 2), (0, 0, 0, 0, 0, 0), (0, 1, 1, 1, 1, 1), (1, 2, 0, 1, 2), (1, 1, 0, 1, 0), (1, 0, 0, 0, 0),
    (0, 0, 1, 1, 1, 1), (1, 2, 1, 1, 2), (1, 1, 0, 0, 2), (0, 1, 1, 1, 1, 0), (0, 0, 1, 1, 1, 0),
    (0, 1, 1, 1, 0, 1), (0, 0, 1, 1, 0, 1), (0, 1, 1, 1, 0, 0), (0, 0, 1, 1, 0, 0), (0, 1, 1, 0, 1, 1),
    (1, 1, 1, 0, 1), (0, 0, 1, 0, 1, 1), (0, 1, 1, 0, 1, 0), (1, 1, 1, 1, 1), (0, 0, 1, 0, 1, 0),
    (0, 1, 1, 0, 0, 1), (0, 0, 1, 0, 0, 1), (1, 1, 1, 0, 0), (0, 1, 1, 0, 0, 0), (0, 0, 1, 0, 0, 0),
    (0, 1, 2, 1, 1, 1), (0, 0, 2, 1, 1, 1), (0, 1, 2, 1, 1, 0), (1, 2, 1, 1, 1), (1, 0, 0, 0, 1), (2, 2, 0),
    (3, 2, 0), (0, 0, 2, 1, 1, 0), (1, 2, 1, 1, 0), (1, 1, 0, 0, 1), (0, 1, 2, 1, 0, 1), (0, 0, 2, 1, 0, 1),
    (0, 1, 2, 1, 0, 0), (0, 0, 2, 1, 0, 0), (2, 0, 0), (3, 0, 0), (0, 1, 2, 0, 1, 1), (1, 2, 2, 1, 1),
    (1, 0, 1, 1, 0), (0, 0, 2, 0, 1, 1), (0, 1, 2, 0, 1, 0), (2, 1, 0), (2, 2, 1), (3, 1, 0), (1, 2, 2, 0, 1),
    (0, 0, 2, 0, 1, 0), (0, 1, 2, 0, 0, 1), (1, 2, 2, 0, 0), (0, 0, 2, 0, 0, 1), (1, 0, 2, 0, 0),
    (0, 1, 2, 0, 0, 0), (1, 1, 2, 0, 1), (1, 2, 0, 0, 2), (1, 1, 1, 0, 2), (0, 0, 2, 0, 0, 0), (0, 1, 3, 1, 1, 1),
    (1, 0, 2, 1, 1), (1, 0, 2, 0, 2), (1, 2, 2, 1, 0), (1, 2, 1, 0, 0), (0, 0, 3, 1, 1, 1), (0, 1, 3, 1, 1, 0),
    (1, 0, 2, 1, 2), (3, 2, 1), (1, 2, 2, 0, 2), (0, 0, 3, 1, 1, 0), (0, 1, 3, 1, 0, 1), (1, 1, 2, 0, 0),
    (1, 2, 3, 1, 2), (0, 0, 3, 1, 0, 1), (1, 1, 3, 0, 2), (1, 2, 2, 1, 2), (1, 0, 1, 1, 1), (0, 1, 3, 1, 0, 0),
    (0, 0, 3, 1, 0, 0), (4, 0, 0), (1, 2, 1, 0, 1), (1, 2, 1, 0, 2), (0, 1, 3, 0, 1, 1), (0, 0, 3, 0, 1, 1),
    (1, 2, 0, 0, 1), (0, 1, 3, 0, 1, 0), (0, 0, 3, 0, 1, 0), (1, 2, 3, 0, 1), (1, 2, 3, 1, 1), (1, 1, 0, 0, 0),
    (1, 0, 1, 0, 1), (0, 1, 3, 0, 0, 1), (1, 0, 3, 1, 0), (1, 1, 1, 1, 0), (4, 1, 0), (1, 2, 3, 0, 2),
    (0, 0, 3, 0, 0, 1), (1, 0, 3, 0, 0), (0, 1, 3, 0, 0, 0), (1, 1, 1, 1, 2), (5, 1, 0), (6, 1, 0), (5, 0, 0),
    (1, 0, 2, 1, 0), (1, 0, 1, 1, 2), (1, 1, 2, 1, 2), (1, 0, 2, 0, 1), (6, 0, 0), (1, 0, 1, 0, 2), (1, 1, 2, 1, 1),
    (2, 2, 2), (3, 2, 2), (1, 1, 2, 1, 0), (2, 1, 1), (3, 1, 1), (0, 0, 3, 0, 0, 0), (1, 2, 3, 1, 0),
    (1, 1, 3, 0, 1), (1, 1, 3, 1, 0), (1, 1, 3, 1, 1), (1, 1, 2, 0, 2), (2, 1, 2), (1, 0, 1, 0, 0), (3, 1, 2),
    (4, 2, 1), (5, 2, 1), (6, 2, 1), (2, 2, 3), (3, 2, 3), (4, 2, 2), (1, 2, 3, 0, 0), (2, 0, 1), (1, 0, 3, 1, 1),
    (3, 0, 1), (1, 1, 3, 0, 0), (4, 1, 1), (5, 1, 1), (6, 1, 1), (5, 2, 2), (6, 2, 2), (1, 2, 0, 0, 0), (4, 1, 2),
    (5, 1, 2), (6, 1, 2), (1, 0, 3, 0, 1), (4, 2, 0), (1, 0, 3, 1, 2), (2, 0, 2), (3, 0, 2), (1, 1, 3, 1, 2),
    (4, 0, 1), (5, 0, 1), (6, 0, 1), (5, 2, 0), (6, 2, 0), (1, 0, 3, 0, 2), (2, 0, 3), (4, 0, 2), (3, 0, 3),
    (5, 0, 2), (6, 0, 2), (4, 2, 3), (5, 2, 3), (2, 1, 3), (3, 1, 3), (4, 1, 3), (5, 1, 3), (7, 1, 0), (7, 2, 0),
    (4, 0, 3), (5, 0, 3), (7, 0, 0),
)
GATHER_ORDER = (
    (0, 2, 0), (1, 2, 1), (3, 2, 3, 0), (1, 2, 0), (0, 0, 0), (1, 0, 2), (2, 0, 3), (1, 2, 2), (1, 0, 0), (0, 1, 0),
    (4, 1, 3, 0, 0), (2, 1, 3), (2, 0, 2), (3, 0, 2, 0), (4, 0, 3, 1, 0), (2, 2, 2), (3, 1, 3, 1), (3, 0, 3, 1),
    (2, 0, 0), (4, 2, 3, 0, 1), (3, 1, 3, 0), (4, 0, 2, 1, 0), (1, 1, 2), (1, 1, 0), (2, 2, 0), (3, 0, 2, 1),
    (3, 0, 0, 0), (3, 1, 2, 0), (4, 1, 3, 1, 1), (4, 2, 2, 0, 0), (2, 1, 2), (3, 2, 0, 1), (1, 1, 1), (3, 1, 0, 0),
    (2, 1, 0), (4, 1, 0, 0, 0), (1, 0, 1), (4, 0, 3, 0, 0), (4, 0, 0, 0, 1), (4, 2, 1, 0, 0), (3, 1, 2, 1),
    (3, 2, 2, 0), (3, 2, 0, 0), (4, 0, 2, 1, 1), (4, 2, 0, 1, 0), (4, 1, 3, 1, 0), (2, 2, 1), (4, 1, 2, 1, 0),
    (4, 0, 0, 0, 0), (3, 0, 0, 1), (3, 1, 0, 1), (2, 2, 3), (3, 0, 3, 0), (3, 2, 2, 1), (4, 1, 2, 1, 1),
    (4, 1, 3, 0, 1), (2, 1, 1), (4, 0, 0, 1, 0), (4, 0, 0, 1, 1), (4, 0, 2, 0, 0), (3, 1, 1, 0), (3, 2, 1, 0),
    (4, 2, 2, 1, 0), (2, 0, 1), (4, 1, 1, 0, 0), (4, 0, 3, 0, 1), (3, 0, 1, 0), (4, 2, 0, 0, 0), (4, 1, 2, 0, 0),
    (4, 1, 1, 0, 1), (3, 1, 1, 1), (4, 1, 1, 1, 0), (4, 1, 0, 1, 1), (4, 2, 2, 0, 1), (4, 2, 3, 1, 0),
    (4, 1, 2, 0, 1), (4, 0, 3, 1, 1), (3, 0, 1, 1), (4, 0, 1, 1, 0), (4, 2, 0, 0, 1), (4, 0, 2, 0, 1),
    (4, 2, 0, 1, 1), (4, 2, 2, 1, 1), (4, 1, 0, 0, 1), (3, 2, 3, 1), (4, 2, 1, 0, 1), (4, 2, 1, 1, 0),
    (4, 1, 0, 1, 0), (3, 2, 1, 1), (4, 2, 3, 0, 0), (4, 0, 1, 0, 1), (4, 0, 1, 0, 0), (4, 1, 1, 1, 1),
    (4, 2, 3, 1, 1), (4, 2, 1, 1, 1), (4, 0, 1, 1, 1),
)
HALF = ((1, 1), (1, 0), (0, 1), (0, 0))


def parts_of(rows, tiles):
    full = rows // TILE
    part = [max(1, full * n // sum(tiles)) * TILE for n in tiles[:-1]]
    return part + [rows - sum(part)]


def padded(n, unit):
    return -(-n // unit) * unit


def over_rows(rows, group, body):
    size = group * TILE
    whole = rows // size

    def step(i, carry):
        body(pl.multiple_of(i * size, size), size)
        return carry

    if whole:
        lax.fori_loop(0, whole, step, 0)
    at = whole * size
    if rows - at >= TILE:
        body(at, (rows - at) // TILE * TILE)
        at += (rows - at) // TILE * TILE
    if rows > at:
        body(at, rows - at)


def half_of(at):
    return at // 2 if isinstance(at, int) else lax.div(at, 2)


def kernel(rows, grad_hbm, w_hbm, m_hbm, v_hbm, d_hbm, lr_ref, full, w, m, v, norm_ref, *scratch):
    count = len(REDUCE)
    stages = scratch[:STAGES]
    scratch = scratch[STAGES:]
    got1, kept, sent2, got2, got3 = (scratch[count * i:count * i + count] for i in range(5))
    (row, mean, d, partial, stage_sem, state_sem, s1, r1, s2, r2, s3, r3, ns, nr,
     gs1, gr1, gs2, gr2, gs3, gr3, gs4, gr4) = scratch[5 * count:]
    part = parts_of(rows, REDUCE_TILES)
    first = [sum(part[:i]) for i in range(count)]
    units = rows // 2
    gather_part = parts_of(rows, GATHER_TILES)
    gather_first = [sum(gather_part[:i]) for i in range(len(gather_part))]

    me = lax.axis_index('dp')
    bits = (lax.div(me, 16), lax.rem(lax.div(me, 8), 2), lax.rem(lax.div(me, 4), 2), lax.rem(lax.div(me, 2), 2),
            lax.rem(me, 2))

    def across(*flips):
        total = 0
        for bit in range(5):
            value = 1 - bits[bit] if bit in flips else bits[bit]
            total = total * 2 + value
        return total

    def pick(axes, values):
        return tuple(a for a, val in zip(axes, values) if val)

    def where(colour, g, j2, j1, jc):
        axes, groups = colour
        return pick(axes + (CORE,), (j1, j2) + groups[g] + (jc,))

    def send(src, dst, send_sem, recv_sem, flips):
        return pltpu.make_async_remote_copy(
            src_ref=src, dst_ref=dst, send_sem=send_sem, recv_sem=recv_sem,
            device_id=(across(*flips),), device_id_type=MESH)

    waited = set()

    def need(copy_of, *key):
        if (copy_of.__name__,) + key not in waited:
            waited.add((copy_of.__name__,) + key)
            copy_of(*key).wait_recv()

    def state_copy(i):
        return pltpu.make_async_copy((w_hbm, m_hbm, v_hbm, d_hbm)[i], (w, m, v, d)[i], state_sem.at[i])

    work = [task[1:] for task in REDUCE_ORDER if task[0] == 0]
    spans = []
    for lead in range(2):
        inside = [i for i in range(count) if SPAN_OF[i] == lead]
        spans.append((inside[0], first[inside[0]], sum(part[i] for i in inside)))

    def stage_copy(i):
        span, g, j2, j1, jc = work[i]
        c, begin, length = spans[span]
        k = across(*where(REDUCE[c], g, j2, j1, jc))
        at = pl.multiple_of((k * rows + begin) * LANES, LANES)
        return pltpu.make_async_copy(grad_hbm.at[:, pl.ds(at, length * LANES)],
                                     stages[i % STAGES].at[:, pl.ds(0, length * LANES)], stage_sem.at[i % STAGES])

    def first_copy(c, g, j2, slot):
        j1 = 1 if slot else 0
        jc = 0 if slot == 1 else 1
        k = across(*where(REDUCE[c], g, j2, j1, jc))
        return send(row.at[k, pl.ds(first[c], padded(part[c], TILE))], got1[c].at[g, j2, slot],
                    s1.at[c, g, j2, slot], r1.at[c, g, j2, slot], pick((REDUCE[c][0][0], CORE), (j1, jc)))

    def second_copy(c, g):
        return send(sent2[c].at[g], got2[c].at[g], s2.at[c, g], r2.at[c, g], (REDUCE[c][0][1],))

    def third_copy(c, g):
        return send(kept[c].at[g], got3[c].at[g], s3.at[c, g], r3.at[c, g], pick(REDUCE[c][0][2:], REDUCE[c][1][g]))

    def pack(i):
        span, g, j2, j1, jc = work[i]
        c, begin, length = spans[span]
        k = across(*where(REDUCE[c], g, j2, j1, jc))
        source = stages[i % STAGES]
        stage_copy(i).wait()

        def body(at, size):
            lane = at * LANES
            if not isinstance(at, int):
                lane = pl.multiple_of(lane, TILE * LANES)
            val = source[:, pl.ds(lane, size * LANES)].astype(F32).reshape(size, LANES)
            row[k, pl.ds(begin + at, size), :] = val.astype(BF16)

        over_rows(length, 4, body)
        if i + STAGES < len(work):
            stage_copy(i + STAGES).start()

    def four_sum(c, g, j2, target):
        for slot in (0, 1, 2):
            need(first_copy, c, g, j2, slot)
        k = across(*where(REDUCE[c], g, j2, 0, 0))

        def body(at, size):
            near = pl.ds(at, size)
            mine = row[k, pl.ds(first[c] + at, size), :].astype(F32) + got1[c][g, j2, 0, near, :].astype(F32)
            other = got1[c][g, j2, 1, near, :].astype(F32) + got1[c][g, j2, 2, near, :].astype(F32)
            target[g, near, :] = mine + other

        over_rows(part[c], 4, body)

    def plane_sum(c, g):
        need(second_copy, c, g)

        def body(at, size):
            near = pl.ds(at, size)
            kept[c][g, near, :] = kept[c][g, near, :] + got2[c][g, near, :]

        if g < 3:
            over_rows(part[c], 4, body)

    def final(c, acc):
        for g in range(3):
            need(third_copy, c, g)

        def mean_of(at, size):
            near = pl.ds(at, size)
            total = (kept[c][3, near, :] + got2[c][3, near, :]) + (got3[c][0, near, :] + got3[c][1, near, :])
            total = (total + got3[c][2, near, :]) * (1.0 / 32.0)
            mean[pl.ds(first[c] + at, size), :] = total
            return total * total

        def fold(val):
            return jnp.sum(val.reshape(val.shape[0] // 8, 8, LANES), axis=0)

        whole = part[c] // 64
        if whole:
            acc = lax.fori_loop(0, whole, lambda i, a: a + fold(mean_of(pl.multiple_of(i * 64, 64), 64)), acc)
        at = whole * 64
        if part[c] - at >= 8:
            size = (part[c] - at) // 8 * 8
            acc = acc + fold(mean_of(at, size))
            at += size
        if part[c] > at:
            tail = mean_of(at, part[c] - at)
            acc = acc + jnp.concatenate([tail, jnp.zeros((8 - tail.shape[0], LANES), F32)], axis=0)
        return acc

    everyone = [pick((HIGH, LOW, Y, X, CORE), [(n >> b) & 1 for b in (4, 3, 2, 1, 0)]) for n in range(1, 32)]

    for i in range(STAGES):
        stage_copy(i).start()
    barrier = pltpu.get_barrier_semaphore()
    for flips in everyone:
        pl.semaphore_signal(barrier, inc=1, device_id=(across(*flips),), device_id_type=MESH)

    acc = jnp.zeros((8, LANES), F32)
    packed = 0
    entered = False
    for task in REDUCE_ORDER:
        kind, c, g = task[:3]
        if kind == 0:
            pack(packed)
            packed += 1
            if packed == len(work):
                for i in range(4):
                    state_copy(i).start()
        elif kind == 1:
            if not entered:
                pl.semaphore_wait(barrier, 31)
                entered = True
            first_copy(c, g, *task[3:]).start()
        elif kind == 2:
            four_sum(c, g, 1, sent2[c])
        elif kind == 3:
            second_copy(c, g).start()
        elif kind == 4:
            four_sum(c, g, 0, kept[c])
        elif kind == 5:
            plane_sum(c, g)
        elif kind == 6:
            third_copy(c, g).start()
        else:
            acc = final(c, acc)

    partial[me] = jnp.sum(acc, axis=0, keepdims=True)

    def norm_copy(j, owner):
        return send(partial.at[owner], partial.at[owner], ns.at[j], nr.at[j], everyone[j])

    for j in range(31):
        norm_copy(j, me).start()
    for i in range(4):
        state_copy(i).wait()
    for j in range(31):
        norm_copy(j, across(*everyone[j])).wait_recv()
    norm = jnp.sqrt(jnp.full((1, LANES), jnp.sum(jnp.sum(partial[...], axis=0)), F32))
    norm_ref[...] = norm
    coef = jnp.minimum(1.0, 1.0 / (norm + CLIP_EPS))
    lr = lr_ref[0]

    def update(c):
        def body(at, size):
            near = pl.ds(gather_first[c] + at, size)
            h = mean[near, :] * coef
            nm = BETA_FIRST * m[near, :] + (1.0 - BETA_FIRST) * h
            nv = BETA_SECOND * v[near, :] + (1.0 - BETA_SECOND) * h * h
            step = (nm * (1.0 / (1.0 - BETA_FIRST ** ADAM_STEP))) / (
                jnp.sqrt(nv * (1.0 / (1.0 - BETA_SECOND ** ADAM_STEP))) + ADAM_EPS)
            old = w[near, :]
            nw = old - lr * (step + WEIGHT_DECAY * d[near, :].astype(F32) * old)
            m[near, :] = nm
            v[near, :] = nv
            w[near, :] = nw
            full[pl.ds(me * units + gather_first[c] // 2 + half_of(at), size // 2)] = nw.astype(BF16).reshape(
                size // 2, 2, LANES)

        over_rows(gather_part[c], 2, body)

    def piece(c, g, j2, j1):
        k = across(*where(GATHER[c], g, j2, j1, 0))
        return full.at[pl.ds(k * units + gather_first[c] // 2, gather_part[c] // 2)]

    def gather1(c, g):
        spot = piece(c, 3, 0, 0)
        return send(spot, spot, gs1.at[c, g], gr1.at[c, g], pick(GATHER[c][0][2:], GATHER[c][1][g]))

    def gather1_in(c, g):
        spot = piece(c, g, 0, 0)
        return send(spot, spot, gs1.at[c, g], gr1.at[c, g], pick(GATHER[c][0][2:], GATHER[c][1][g]))

    def gather2(c, g):
        spot = piece(c, g, 0, 0)
        return send(spot, spot, gs2.at[c, g], gr2.at[c, g], (GATHER[c][0][1],))

    def gather3(c, g, j2):
        spot = piece(c, g, j2, 0)
        return send(spot, spot, gs3.at[c, g, j2], gr3.at[c, g, j2], (GATHER[c][0][0],))

    def gather4(c, g, j2, j1):
        spot = piece(c, g, j2, j1)
        return send(spot, spot, gs4.at[c, g, j2, j1], gr4.at[c, g, j2, j1], (CORE,))

    for kind, c, *key in GATHER_ORDER:
        if kind == 0:
            update(c)
        elif kind == 1:
            gather1(c, *key).start()
        else:
            if kind == 4 and key[2]:
                need(gather3, c, *key[:2])
            elif kind > 2 and key[1]:
                need(gather2, c, key[0])
            elif key[0] < 3:
                need(gather1_in, c, key[0])
            (gather2, gather3, gather4)[kind - 2](c, *key).start()

    for c in range(count):
        for g in range(4):
            for j2 in (0, 1):
                for slot in range(3):
                    first_copy(c, g, j2, slot).wait_send()
            second_copy(c, g).wait_send()
        for g in range(3):
            third_copy(c, g).wait_send()
    for j in range(31):
        norm_copy(j, me).wait_send()
    for c in range(len(GATHER)):
        for g in range(3):
            gather1(c, g).wait_send()
        for g in range(4):
            gather2(c, g).wait_send()
            for j2 in (0, 1):
                gather3(c, g, j2).wait_send()
                for j1 in (0, 1):
                    gather4(c, g, j2, j1).wait()


def write_out(*refs):
    sem = refs[-1]
    count = len(refs) // 2
    length = refs[0].shape[0] // CHUNKS
    copies = []
    for i in range(CHUNKS):
        near = pl.ds(i * length, length)
        copies.append(pltpu.make_async_copy(refs[0].at[near], refs[count].at[near], sem.at[i]))
    for i in range(1, count):
        copies.append(pltpu.make_async_copy(refs[i], refs[count + i], sem.at[CHUNKS + i - 1]))
    for copy in copies:
        copy.start()
    for copy in copies:
        copy.wait()


def solution(mesh):
    num_dev = mesh.shape['dp']

    def local_step(grad_row, master, mom_first, mom_second, decay_mask, learn_rate):
        shard_len = master.shape[0]
        rows = shard_len // LANES
        part = parts_of(rows, REDUCE_TILES)
        dma = pltpu.SemaphoreType.DMA
        hbm = pl.BlockSpec(memory_space=pltpu.HBM)
        vmem = pl.BlockSpec(memory_space=pltpu.VMEM)
        flat = (rows, LANES)
        whole = (num_dev * rows // 2, 2, LANES)
        n = len(REDUCE)
        longest = max(sum(part[i] for i in range(n) if SPAN_OF[i] == lead) for lead in range(2))
        k = len(GATHER)
        results = pl.pallas_call(
            functools.partial(kernel, rows),
            out_shape=(pltpu.VMEM(whole, BF16), pltpu.VMEM(flat, F32), pltpu.VMEM(flat, F32), pltpu.VMEM(flat, F32),
                       pltpu.VMEM((1, LANES), F32)),
            in_specs=[hbm] * 5 + [pl.BlockSpec(memory_space=pltpu.SMEM)],
            out_specs=(vmem,) * 5,
            scratch_shapes=[pltpu.VMEM((1, longest * LANES), BF16)] * STAGES
            + [pltpu.VMEM((4, 2, 3, padded(p, TILE), LANES), BF16) for p in part]
            + [pltpu.VMEM((groups, padded(p, 8), LANES), F32) for groups in (4, 4, 4, 3) for p in part]
            + [
                pltpu.VMEM((num_dev, padded(rows, TILE), LANES), BF16), pltpu.VMEM(flat, F32),
                pltpu.VMEM(flat, jnp.int32), pltpu.VMEM((num_dev, 1, LANES), F32),
                dma((STAGES,)), dma((4,)),
                dma((n, 4, 2, 3)), dma((n, 4, 2, 3)), dma((n, 4)), dma((n, 4)), dma((n, 3)), dma((n, 3)),
                dma((num_dev - 1,)), dma((num_dev - 1,)),
                dma((k, 3)), dma((k, 3)), dma((k, 4)), dma((k, 4)), dma((k, 4, 2)), dma((k, 4, 2)),
                dma((k, 4, 2, 2)), dma((k, 4, 2, 2)),
            ],
            compiler_params=pltpu.CompilerParams(
                collective_id=0, has_side_effects=True, vmem_limit_bytes=VMEM_LIMIT),
        )(grad_row, master.reshape(flat), mom_first.reshape(flat), mom_second.reshape(flat), decay_mask.reshape(flat), learn_rate)
        state = jax.ShapeDtypeStruct(flat, F32)
        params, new_master, new_first, new_second, norm = pl.pallas_call(
            write_out,
            out_shape=(jax.ShapeDtypeStruct(whole, BF16), state, state, state, jax.ShapeDtypeStruct((1, LANES), F32)),
            in_specs=[vmem] * 5,
            out_specs=(hbm,) * 5,
            scratch_shapes=[dma((CHUNKS + 4,))],
            compiler_params=pltpu.CompilerParams(vmem_limit_bytes=1024 * 1024),
        )(*results)
        return (params.reshape(num_dev * shard_len), new_master.reshape(shard_len), new_first.reshape(shard_len),
                new_second.reshape(shard_len), norm[0, :1])

    return jax.shard_map(local_step, mesh=mesh, in_specs=(P('dp', None), P('dp'), P('dp'), P('dp'), P('dp'), P()),
                         out_specs=(P(), P('dp'), P('dp'), P('dp'), P()), check_vma=False)
```

```python
import functools

import jax
import jax.numpy as jnp
from jax import lax
from jax.experimental import pallas as pl
from jax.experimental.pallas import tpu as pltpu
from jax.sharding import PartitionSpec as P

BETA_FIRST = 0.9
BETA_SECOND = 0.95
ADAM_EPS = 1e-8
CLIP_EPS = 1e-6
WEIGHT_DECAY = 0.1
ADAM_STEP = 10
LANES = 128
TILE = 16
STAGES = 4
CHUNKS = 8
VMEM_LIMIT = 46 * 1024 * 1024
MESH = pl.DeviceIdType.MESH
F32 = jnp.float32
BF16 = jnp.bfloat16

HIGH, LOW, Y, X, CORE = range(5)
REDUCE = (
    ((X, Y, LOW, HIGH), ((1, 1), (1, 0), (0, 1), (0, 0))),
    ((Y, X, LOW, HIGH), ((1, 1), (1, 0), (0, 1), (0, 0))),
    ((LOW, HIGH, X, Y), ((1, 1), (0, 1), (1, 0), (0, 0))),
)
REDUCE_TILES = (47, 47, 20)
SPAN_OF = (0, 0, 1)
GATHER = (
    ((X, Y, LOW, HIGH), ((1, 1), (0, 1), (1, 0), (0, 0))),
    ((Y, X, LOW, HIGH), ((1, 1), (0, 1), (1, 0), (0, 0))),
    ((LOW, HIGH, X, Y), ((1, 0), (1, 1), (0, 1), (0, 0))),
)
GATHER_TILES = (48, 48, 18)
REDUCE_ORDER = (
    (0, 1, 0, 1, 1, 1), (0, 0, 0, 1, 1, 1), (1, 0, 0, 1, 2), (0, 1, 0, 1, 1, 0), (1, 2, 0, 1, 1), (1, 1, 0, 1, 2),
    (0, 0, 0, 1, 1, 0), (1, 0, 0, 1, 1), (1, 1, 0, 1, 1), (0, 1, 0, 1, 0, 1), (0, 0, 0, 1, 0, 1),
    (0, 1, 0, 1, 0, 0), (0, 0, 0, 1, 0, 0), (0, 1, 0, 0, 1, 1), (0, 0, 0, 0, 1, 1), (0, 1, 0, 0, 1, 0),
    (0, 0, 0, 0, 1, 0), (1, 0, 0, 1, 0), (0, 1, 0, 0, 0, 1), (0, 0, 0, 0, 0, 1), (0, 1, 0, 0, 0, 0),
    (0, 0, 0, 0, 0, 0), (1, 0, 0, 0, 2), (0, 1, 1, 1, 1, 1), (1, 2, 0, 1, 2), (1, 1, 0, 1, 0), (1, 0, 0, 0, 0),
    (0, 0, 1, 1, 1, 1), (0, 1, 1, 1, 1, 0), (1, 2, 1, 1, 2), (1, 1, 0, 0, 2), (0, 0, 1, 1, 1, 0), (1, 2, 1, 1, 1),
    (1, 1, 1, 1, 1), (0, 1, 1, 1, 0, 1), (0, 0, 1, 1, 0, 1), (0, 1, 1, 1, 0, 0), (0, 0, 1, 1, 0, 0),
    (1, 1, 1, 0, 1), (0, 1, 1, 0, 1, 1), (1, 2, 0, 1, 0), (0, 0, 1, 0, 1, 1), (0, 1, 1, 0, 1, 0),
    (0, 0, 1, 0, 1, 0), (0, 1, 1, 0, 0, 1), (0, 0, 1, 0, 0, 1), (1, 1, 1, 0, 0), (0, 1, 1, 0, 0, 0),
    (0, 0, 1, 0, 0, 0), (0, 1, 2, 1, 1, 1), (0, 0, 2, 1, 1, 1), (0, 1, 2, 1, 1, 0), (1, 0, 0, 0, 1),
    (0, 0, 2, 1, 1, 0), (1, 2, 1, 1, 0), (1, 1, 0, 0, 1), (2, 2, 0), (3, 2, 0), (0, 1, 2, 1, 0, 1),
    (0, 0, 2, 1, 0, 1), (0, 1, 2, 1, 0, 0), (2, 1, 0), (0, 0, 2, 1, 0, 0), (2, 0, 0), (3, 0, 0), (1, 0, 1, 1, 0),
    (1, 2, 2, 1, 1), (3, 1, 0), (0, 1, 2, 0, 1, 1), (0, 0, 2, 0, 1, 1), (0, 1, 2, 0, 1, 0), (1, 2, 2, 0, 1),
    (0, 0, 2, 0, 1, 0), (0, 1, 2, 0, 0, 1), (1, 2, 2, 0, 0), (0, 0, 2, 0, 0, 1), (1, 0, 2, 0, 0), (2, 2, 1),
    (0, 1, 2, 0, 0, 0), (1, 0, 2, 1, 1), (0, 0, 2, 0, 0, 0), (0, 1, 3, 1, 1, 1), (0, 0, 3, 1, 1, 1),
    (1, 0, 2, 0, 2), (1, 2, 2, 1, 0), (1, 0, 1, 0, 1), (0, 1, 3, 1, 1, 0), (0, 0, 3, 1, 1, 0), (0, 1, 3, 1, 0, 1),
    (0, 0, 3, 1, 0, 1), (1, 1, 3, 0, 2), (1, 0, 2, 1, 2), (3, 2, 1), (1, 2, 2, 0, 2), (1, 2, 1, 0, 1),
    (1, 2, 1, 0, 2), (1, 2, 2, 1, 2), (1, 0, 3, 1, 0), (0, 1, 3, 1, 0, 0), (0, 0, 3, 1, 0, 0), (1, 0, 1, 1, 1),
    (4, 0, 0), (0, 1, 3, 0, 1, 1), (0, 0, 3, 0, 1, 1), (0, 1, 3, 0, 1, 0), (1, 2, 0, 0, 1), (1, 1, 0, 0, 0),
    (1, 2, 3, 1, 2), (1, 1, 1, 1, 0), (0, 0, 3, 0, 1, 0), (1, 2, 3, 0, 1), (1, 2, 3, 1, 1), (0, 1, 3, 0, 0, 1),
    (1, 1, 1, 0, 2), (4, 1, 0), (5, 1, 0), (1, 2, 0, 0, 2), (1, 2, 3, 0, 2), (0, 0, 3, 0, 0, 1), (0, 1, 3, 0, 0, 0),
    (1, 0, 3, 0, 0), (1, 1, 1, 1, 2), (6, 1, 0), (1, 1, 2, 1, 2), (1, 0, 2, 0, 1), (5, 0, 0), (1, 0, 1, 1, 2),
    (1, 1, 2, 0, 0), (6, 0, 0), (1, 0, 1, 0, 2), (1, 1, 2, 0, 1), (1, 0, 2, 1, 0), (1, 1, 2, 1, 1), (2, 2, 2),
    (0, 0, 3, 0, 0, 0), (1, 2, 3, 1, 0), (1, 1, 3, 0, 1), (1, 1, 3, 1, 0), (3, 2, 2), (1, 2, 1, 0, 0),
    (1, 1, 2, 1, 0), (2, 1, 1), (3, 1, 1), (4, 1, 1), (1, 1, 2, 0, 2), (1, 0, 1, 0, 0), (2, 1, 2), (3, 1, 2),
    (2, 0, 1), (4, 2, 1), (5, 2, 1), (1, 1, 3, 1, 1), (2, 2, 3), (3, 2, 3), (1, 1, 3, 0, 0), (6, 2, 1),
    (1, 0, 3, 1, 1), (3, 0, 1), (4, 2, 2), (5, 1, 1), (6, 1, 1), (5, 2, 2), (6, 2, 2), (1, 2, 0, 0, 0), (4, 1, 2),
    (5, 1, 2), (6, 1, 2), (1, 0, 3, 1, 2), (4, 2, 0), (2, 0, 2), (3, 0, 2), (1, 1, 3, 1, 2), (4, 0, 1),
    (1, 2, 3, 0, 0), (5, 0, 1), (6, 0, 1), (5, 2, 0), (1, 0, 3, 0, 2), (2, 0, 3), (4, 0, 2), (3, 0, 3),
    (1, 0, 3, 0, 1), (5, 0, 2), (6, 0, 2), (4, 2, 3), (5, 2, 3), (2, 1, 3), (3, 1, 3), (6, 2, 0), (4, 1, 3),
    (5, 1, 3), (7, 1, 0), (7, 2, 0), (4, 0, 3), (5, 0, 3), (7, 0, 0),
)
GATHER_ORDER = (
    (0, 2, 0), (1, 2, 1), (0, 0, 0), (3, 0, 3, 0), (1, 0, 2), (4, 2, 3, 0, 0), (1, 0, 0), (0, 1, 0), (2, 1, 3),
    (2, 0, 3), (3, 1, 3, 0), (3, 0, 3, 1), (1, 1, 1), (1, 2, 2), (3, 1, 3, 1), (1, 1, 2), (3, 0, 2, 0),
    (3, 0, 0, 0), (4, 0, 3, 0, 1), (1, 0, 1), (2, 0, 0), (2, 2, 2), (3, 1, 1, 0), (2, 1, 1), (2, 0, 2), (1, 2, 0),
    (3, 1, 2, 0), (3, 2, 3, 0), (2, 1, 2), (4, 0, 1, 0, 0), (3, 2, 1, 0), (4, 1, 3, 0, 1), (1, 1, 0), (3, 0, 1, 0),
    (4, 0, 0, 0, 1), (2, 0, 1), (4, 0, 0, 0, 0), (4, 2, 3, 0, 1), (3, 2, 2, 1), (4, 0, 3, 1, 0), (4, 1, 1, 1, 0),
    (3, 1, 1, 1), (4, 0, 3, 0, 0), (3, 0, 0, 1), (4, 0, 2, 0, 1), (4, 2, 1, 0, 1), (4, 1, 3, 0, 0), (4, 0, 1, 1, 0),
    (4, 2, 0, 0, 0), (4, 2, 2, 0, 0), (2, 2, 1), (4, 0, 2, 0, 0), (3, 2, 2, 0), (4, 2, 1, 0, 0), (2, 2, 3),
    (3, 0, 1, 1), (2, 1, 0), (3, 1, 2, 1), (3, 2, 1, 1), (4, 1, 1, 0, 1), (4, 2, 2, 1, 1), (3, 0, 2, 1),
    (4, 0, 1, 0, 1), (4, 1, 1, 1, 1), (2, 2, 0), (4, 0, 3, 1, 1), (4, 1, 2, 1, 0), (3, 2, 0, 0), (4, 0, 0, 1, 0),
    (3, 1, 0, 0), (4, 0, 2, 1, 0), (4, 1, 3, 1, 1), (4, 1, 2, 1, 1), (4, 1, 3, 1, 0), (4, 2, 1, 1, 1),
    (4, 0, 1, 1, 1), (3, 1, 0, 1), (4, 0, 0, 1, 1), (4, 2, 2, 0, 1), (4, 2, 1, 1, 0), (4, 1, 2, 0, 1),
    (4, 1, 0, 0, 1), (4, 1, 2, 0, 0), (3, 2, 3, 1), (3, 2, 0, 1), (4, 2, 2, 1, 0), (4, 1, 0, 1, 0), (4, 2, 3, 1, 0),
    (4, 1, 0, 0, 0), (4, 0, 2, 1, 1), (4, 1, 1, 0, 0), (4, 2, 0, 1, 0), (4, 2, 3, 1, 1), (4, 1, 0, 1, 1),
    (4, 2, 0, 0, 1), (4, 2, 0, 1, 1),
)
HALF = ((1, 1), (1, 0), (0, 1), (0, 0))


def parts_of(rows, tiles):
    full = rows // TILE
    part = [max(1, full * n // sum(tiles)) * TILE for n in tiles[:-1]]
    return part + [rows - sum(part)]


def padded(n, unit):
    return -(-n // unit) * unit


def over_rows(rows, group, body):
    size = group * TILE
    whole = rows // size

    def step(i, carry):
        body(pl.multiple_of(i * size, size), size)
        return carry

    if whole:
        lax.fori_loop(0, whole, step, 0)
    at = whole * size
    if rows - at >= TILE:
        body(at, (rows - at) // TILE * TILE)
        at += (rows - at) // TILE * TILE
    if rows > at:
        body(at, rows - at)


def half_of(at):
    return at // 2 if isinstance(at, int) else lax.div(at, 2)


def kernel(rows, grad_hbm, w_hbm, m_hbm, v_hbm, d_hbm, lr_ref, full, w, m, v, norm_ref, *scratch):
    count = len(REDUCE)
    stages = scratch[:STAGES]
    scratch = scratch[STAGES:]
    got1, kept, sent2, got2, got3 = (scratch[count * i:count * i + count] for i in range(5))
    (row, mean, d, partial, stage_sem, state_sem, s1, r1, s2, r2, s3, r3, ns, nr,
     gs1, gr1, gs2, gr2, gs3, gr3, gs4, gr4) = scratch[5 * count:]
    part = parts_of(rows, REDUCE_TILES)
    first = [sum(part[:i]) for i in range(count)]
    units = rows // 2
    gather_part = parts_of(rows, GATHER_TILES)
    gather_first = [sum(gather_part[:i]) for i in range(len(gather_part))]

    me = lax.axis_index('dp')
    bits = (lax.div(me, 16), lax.rem(lax.div(me, 8), 2), lax.rem(lax.div(me, 4), 2), lax.rem(lax.div(me, 2), 2),
            lax.rem(me, 2))

    def across(*flips):
        total = 0
        for bit in range(5):
            value = 1 - bits[bit] if bit in flips else bits[bit]
            total = total * 2 + value
        return total

    def pick(axes, values):
        return tuple(a for a, val in zip(axes, values) if val)

    def where(colour, g, j2, j1, jc):
        axes, groups = colour
        return pick(axes + (CORE,), (j1, j2) + groups[g] + (jc,))

    def send(src, dst, send_sem, recv_sem, flips):
        return pltpu.make_async_remote_copy(
            src_ref=src, dst_ref=dst, send_sem=send_sem, recv_sem=recv_sem,
            device_id=(across(*flips),), device_id_type=MESH)

    waited = set()

    def need(copy_of, *key):
        if (copy_of.__name__,) + key not in waited:
            waited.add((copy_of.__name__,) + key)
            copy_of(*key).wait_recv()

    def state_copy(i):
        return pltpu.make_async_copy((w_hbm, m_hbm, v_hbm, d_hbm)[i], (w, m, v, d)[i], state_sem.at[i])

    work = [task[1:] for task in REDUCE_ORDER if task[0] == 0]
    spans = []
    for lead in range(2):
        inside = [i for i in range(count) if SPAN_OF[i] == lead]
        spans.append((inside[0], first[inside[0]], sum(part[i] for i in inside)))

    def stage_copy(i):
        span, g, j2, j1, jc = work[i]
        c, begin, length = spans[span]
        k = across(*where(REDUCE[c], g, j2, j1, jc))
        at = pl.multiple_of((k * rows + begin) * LANES, LANES)
        return pltpu.make_async_copy(grad_hbm.at[:, pl.ds(at, length * LANES)],
                                     stages[i % STAGES].at[:, pl.ds(0, length * LANES)], stage_sem.at[i % STAGES])

    def first_copy(c, g, j2, slot):
        j1 = 1 if slot else 0
        jc = 0 if slot == 1 else 1
        k = across(*where(REDUCE[c], g, j2, j1, jc))
        return send(row.at[k, pl.ds(first[c], padded(part[c], TILE))], got1[c].at[g, j2, slot],
                    s1.at[c, g, j2, slot], r1.at[c, g, j2, slot], pick((REDUCE[c][0][0], CORE), (j1, jc)))

    def second_copy(c, g):
        return send(sent2[c].at[g], got2[c].at[g], s2.at[c, g], r2.at[c, g], (REDUCE[c][0][1],))

    def third_copy(c, g):
        return send(kept[c].at[g], got3[c].at[g], s3.at[c, g], r3.at[c, g], pick(REDUCE[c][0][2:], REDUCE[c][1][g]))

    def pack(i):
        span, g, j2, j1, jc = work[i]
        c, begin, length = spans[span]
        k = across(*where(REDUCE[c], g, j2, j1, jc))
        source = stages[i % STAGES]
        stage_copy(i).wait()

        def body(at, size):
            lane = at * LANES
            if not isinstance(at, int):
                lane = pl.multiple_of(lane, TILE * LANES)
            val = source[:, pl.ds(lane, size * LANES)].astype(F32).reshape(size, LANES)
            row[k, pl.ds(begin + at, size), :] = val.astype(BF16)

        over_rows(length, 4, body)
        if i + STAGES < len(work):
            stage_copy(i + STAGES).start()

    def four_sum(c, g, j2, target):
        for slot in (0, 1, 2):
            need(first_copy, c, g, j2, slot)
        k = across(*where(REDUCE[c], g, j2, 0, 0))

        def body(at, size):
            near = pl.ds(at, size)
            mine = row[k, pl.ds(first[c] + at, size), :].astype(F32) + got1[c][g, j2, 0, near, :].astype(F32)
            other = got1[c][g, j2, 1, near, :].astype(F32) + got1[c][g, j2, 2, near, :].astype(F32)
            target[g, near, :] = mine + other

        over_rows(part[c], 4, body)

    def plane_sum(c, g):
        need(second_copy, c, g)

        def body(at, size):
            near = pl.ds(at, size)
            kept[c][g, near, :] = kept[c][g, near, :] + got2[c][g, near, :]

        if g < 3:
            over_rows(part[c], 4, body)

    def final(c, acc):
        for g in range(3):
            need(third_copy, c, g)

        def mean_of(at, size):
            near = pl.ds(at, size)
            total = (kept[c][3, near, :] + got2[c][3, near, :]) + (got3[c][0, near, :] + got3[c][1, near, :])
            total = (total + got3[c][2, near, :]) * (1.0 / 32.0)
            mean[pl.ds(first[c] + at, size), :] = total
            return total * total

        def fold(val):
            return jnp.sum(val.reshape(val.shape[0] // 8, 8, LANES), axis=0)

        whole = part[c] // 64
        if whole:
            acc = lax.fori_loop(0, whole, lambda i, a: a + fold(mean_of(pl.multiple_of(i * 64, 64), 64)), acc)
        at = whole * 64
        if part[c] - at >= 8:
            size = (part[c] - at) // 8 * 8
            acc = acc + fold(mean_of(at, size))
            at += size
        if part[c] > at:
            tail = mean_of(at, part[c] - at)
            acc = acc + jnp.concatenate([tail, jnp.zeros((8 - tail.shape[0], LANES), F32)], axis=0)
        return acc

    everyone = [pick((HIGH, LOW, Y, X, CORE), [(n >> b) & 1 for b in (4, 3, 2, 1, 0)]) for n in range(1, 32)]

    for i in range(STAGES):
        stage_copy(i).start()
    barrier = pltpu.get_barrier_semaphore()
    for flips in everyone:
        pl.semaphore_signal(barrier, inc=1, device_id=(across(*flips),), device_id_type=MESH)

    acc = jnp.zeros((8, LANES), F32)
    packed = 0
    entered = False
    for task in REDUCE_ORDER:
        kind, c, g = task[:3]
        if kind == 0:
            pack(packed)
            packed += 1
            if packed == len(work):
                for i in range(4):
                    state_copy(i).start()
        elif kind == 1:
            if not entered:
                pl.semaphore_wait(barrier, 31)
                entered = True
            first_copy(c, g, *task[3:]).start()
        elif kind == 2:
            four_sum(c, g, 1, sent2[c])
        elif kind == 3:
            second_copy(c, g).start()
        elif kind == 4:
            four_sum(c, g, 0, kept[c])
        elif kind == 5:
            plane_sum(c, g)
        elif kind == 6:
            third_copy(c, g).start()
        else:
            acc = final(c, acc)

    partial[me] = jnp.sum(acc, axis=0, keepdims=True)

    def norm_copy(j, owner):
        return send(partial.at[owner], partial.at[owner], ns.at[j], nr.at[j], everyone[j])

    for j in range(31):
        norm_copy(j, me).start()
    for i in range(4):
        state_copy(i).wait()
    for j in range(31):
        norm_copy(j, across(*everyone[j])).wait_recv()
    norm = jnp.sqrt(jnp.full((1, LANES), jnp.sum(jnp.sum(partial[...], axis=0)), F32))
    norm_ref[...] = norm
    coef = jnp.minimum(1.0, 1.0 / (norm + CLIP_EPS))
    lr = lr_ref[0]

    def update(c):
        def body(at, size):
            near = pl.ds(gather_first[c] + at, size)
            h = mean[near, :] * coef
            nm = BETA_FIRST * m[near, :] + (1.0 - BETA_FIRST) * h
            nv = BETA_SECOND * v[near, :] + (1.0 - BETA_SECOND) * h * h
            step = (nm * (1.0 / (1.0 - BETA_FIRST ** ADAM_STEP))) / (
                jnp.sqrt(nv * (1.0 / (1.0 - BETA_SECOND ** ADAM_STEP))) + ADAM_EPS)
            old = w[near, :]
            nw = old - lr * (step + WEIGHT_DECAY * d[near, :].astype(F32) * old)
            m[near, :] = nm
            v[near, :] = nv
            w[near, :] = nw
            full[pl.ds(me * units + gather_first[c] // 2 + half_of(at), size // 2)] = nw.astype(BF16).reshape(
                size // 2, 2, LANES)

        over_rows(gather_part[c], 2, body)

    def piece(c, g, j2, j1):
        k = across(*where(GATHER[c], g, j2, j1, 0))
        return full.at[pl.ds(k * units + gather_first[c] // 2, gather_part[c] // 2)]

    def gather1(c, g):
        spot = piece(c, 3, 0, 0)
        return send(spot, spot, gs1.at[c, g], gr1.at[c, g], pick(GATHER[c][0][2:], GATHER[c][1][g]))

    def gather1_in(c, g):
        spot = piece(c, g, 0, 0)
        return send(spot, spot, gs1.at[c, g], gr1.at[c, g], pick(GATHER[c][0][2:], GATHER[c][1][g]))

    def gather2(c, g):
        spot = piece(c, g, 0, 0)
        return send(spot, spot, gs2.at[c, g], gr2.at[c, g], (GATHER[c][0][1],))

    def gather3(c, g, j2):
        spot = piece(c, g, j2, 0)
        return send(spot, spot, gs3.at[c, g, j2], gr3.at[c, g, j2], (GATHER[c][0][0],))

    def gather4(c, g, j2, j1):
        spot = piece(c, g, j2, j1)
        return send(spot, spot, gs4.at[c, g, j2, j1], gr4.at[c, g, j2, j1], (CORE,))

    for kind, c, *key in GATHER_ORDER:
        if kind == 0:
            update(c)
        elif kind == 1:
            gather1(c, *key).start()
        else:
            if kind == 4 and key[2]:
                need(gather3, c, *key[:2])
            elif kind > 2 and key[1]:
                need(gather2, c, key[0])
            elif key[0] < 3:
                need(gather1_in, c, key[0])
            (gather2, gather3, gather4)[kind - 2](c, *key).start()

    for c in range(count):
        for g in range(4):
            for j2 in (0, 1):
                for slot in range(3):
                    first_copy(c, g, j2, slot).wait_send()
            second_copy(c, g).wait_send()
        for g in range(3):
            third_copy(c, g).wait_send()
    for j in range(31):
        norm_copy(j, me).wait_send()
    for c in range(len(GATHER)):
        for g in range(3):
            gather1(c, g).wait_send()
        for g in range(4):
            gather2(c, g).wait_send()
            for j2 in (0, 1):
                gather3(c, g, j2).wait_send()
                for j1 in (0, 1):
                    gather4(c, g, j2, j1).wait()


def write_out(*refs):
    sem = refs[-1]
    count = len(refs) // 2
    length = refs[0].shape[0] // CHUNKS
    copies = []
    for i in range(CHUNKS):
        near = pl.ds(i * length, length)
        copies.append(pltpu.make_async_copy(refs[0].at[near], refs[count].at[near], sem.at[i]))
    for i in range(1, count):
        copies.append(pltpu.make_async_copy(refs[i], refs[count + i], sem.at[CHUNKS + i - 1]))
    for copy in copies:
        copy.start()
    for copy in copies:
        copy.wait()


def solution(mesh):
    num_dev = mesh.shape['dp']

    def local_step(grad_row, master, mom_first, mom_second, decay_mask, learn_rate):
        shard_len = master.shape[0]
        rows = shard_len // LANES
        part = parts_of(rows, REDUCE_TILES)
        dma = pltpu.SemaphoreType.DMA
        hbm = pl.BlockSpec(memory_space=pltpu.HBM)
        vmem = pl.BlockSpec(memory_space=pltpu.VMEM)
        flat = (rows, LANES)
        whole = (num_dev * rows // 2, 2, LANES)
        n = len(REDUCE)
        longest = max(sum(part[i] for i in range(n) if SPAN_OF[i] == lead) for lead in range(2))
        k = len(GATHER)
        results = pl.pallas_call(
            functools.partial(kernel, rows),
            out_shape=(pltpu.VMEM(whole, BF16), pltpu.VMEM(flat, F32), pltpu.VMEM(flat, F32), pltpu.VMEM(flat, F32),
                       pltpu.VMEM((1, LANES), F32)),
            in_specs=[hbm] * 5 + [pl.BlockSpec(memory_space=pltpu.SMEM)],
            out_specs=(vmem,) * 5,
            scratch_shapes=[pltpu.VMEM((1, longest * LANES), BF16)] * STAGES
            + [pltpu.VMEM((4, 2, 3, padded(p, TILE), LANES), BF16) for p in part]
            + [pltpu.VMEM((groups, padded(p, 8), LANES), F32) for groups in (4, 4, 4, 3) for p in part]
            + [
                pltpu.VMEM((num_dev, padded(rows, TILE), LANES), BF16), pltpu.VMEM(flat, F32),
                pltpu.VMEM(flat, jnp.int32), pltpu.VMEM((num_dev, 1, LANES), F32),
                dma((STAGES,)), dma((4,)),
                dma((n, 4, 2, 3)), dma((n, 4, 2, 3)), dma((n, 4)), dma((n, 4)), dma((n, 3)), dma((n, 3)),
                dma((num_dev - 1,)), dma((num_dev - 1,)),
                dma((k, 3)), dma((k, 3)), dma((k, 4)), dma((k, 4)), dma((k, 4, 2)), dma((k, 4, 2)),
                dma((k, 4, 2, 2)), dma((k, 4, 2, 2)),
            ],
            compiler_params=pltpu.CompilerParams(
                collective_id=0, has_side_effects=True, vmem_limit_bytes=VMEM_LIMIT),
        )(grad_row, master.reshape(flat), mom_first.reshape(flat), mom_second.reshape(flat), decay_mask.reshape(flat), learn_rate)
        state = jax.ShapeDtypeStruct(flat, F32)
        params, new_master, new_first, new_second, norm = pl.pallas_call(
            write_out,
            out_shape=(jax.ShapeDtypeStruct(whole, BF16), state, state, state, jax.ShapeDtypeStruct((1, LANES), F32)),
            in_specs=[vmem] * 5,
            out_specs=(hbm,) * 5,
            scratch_shapes=[dma((CHUNKS + 4,))],
            compiler_params=pltpu.CompilerParams(vmem_limit_bytes=1024 * 1024),
        )(*results)
        return (params.reshape(num_dev * shard_len), new_master.reshape(shard_len), new_first.reshape(shard_len),
                new_second.reshape(shard_len), norm[0, :1])

    return jax.shard_map(local_step, mesh=mesh, in_specs=(P('dp', None), P('dp'), P('dp'), P('dp'), P('dp'), P()),
                         out_specs=(P(), P('dp'), P('dp'), P('dp'), P()), check_vma=False)
```
